128 devices in a mesh: right: 64 (over z, y, x), left: 2 (over core).
Axes of the slice: x: 4, y: 4, z: 4, core: 2. Of those that a mesh axis runs over, the one named last changes fastest.
Arguments:
- psi_init: float32 [1536, 2, 2, 1536], P('left', None, None, 'right')
- env_left: float32 [1536, 8, 1536], P('left')
- env_right: float32 [1536, 8, 1536], P('right')
- mpo_pair: float32 [8, 8, 2, 2, 2, 2], replicated
Outputs:
- output 1: float32 [5], replicated
- output 2: float32 [5], replicated
- output 3: float32 [1536, 2, 2, 1536], P('left', None, None, 'right')
All inputs are finite; a program needn't handle non-finite values.
Results may differ from the reference program's by a relative error of at most 0.001.
Values sent between devices are 32-bit elements.
A program may use at most 1 GiB of HBM per device.

```python
import math
import jax
import jax.numpy as jnp
from jax import lax

PHYS_DIM = 2
MPO_DIM = 8
BOND_DIM = 1536
KRYLOV_STEPS = 5
PREC_MODE = lax.Precision.HIGHEST


def sym_env(env_key, bond_dim, mpo_dim):
    key_mat, key_shift = jax.random.split(env_key)
    gauss_mat = jax.random.normal(key_mat, (bond_dim, mpo_dim, bond_dim), jnp.float32)
    sym_part = (gauss_mat + jnp.transpose(gauss_mat, (2, 1, 0))) / math.sqrt(2.0 * bond_dim)
    diag_shift = jax.random.normal(key_shift, (mpo_dim,), jnp.float32)
    eye_mat = jnp.eye(bond_dim, dtype=jnp.float32)
    return sym_part + eye_mat[:, None, :] * diag_shift[None, :, None]


def sym_mpo(mpo_key, mpo_dim, phys_dim):
    key_mat, key_diag = jax.random.split(mpo_key)
    gauss_mat = jax.random.normal(key_mat, (mpo_dim, mpo_dim, phys_dim, phys_dim, phys_dim, phys_dim), jnp.float32)
    sym_part = (gauss_mat + jnp.transpose(gauss_mat, (0, 1, 4, 5, 2, 3))) / (math.sqrt(2.0) * mpo_dim * phys_dim)
    diag_coef = jax.random.normal(key_diag, (mpo_dim, mpo_dim), jnp.float32) / mpo_dim
    eye_phys = jnp.eye(phys_dim * phys_dim, dtype=jnp.float32).reshape(phys_dim, phys_dim, phys_dim, phys_dim)
    return sym_part + diag_coef[:, :, None, None, None, None] * eye_phys[None, None]


def setup_inputs(seed: int = 0) -> dict:
    base_key = jax.random.key(seed)
    key_psi, key_left, key_right, key_mpo = jax.random.split(base_key, 4)
    psi_init = jax.random.normal(key_psi, (BOND_DIM, PHYS_DIM, PHYS_DIM, BOND_DIM), jnp.float32)
    return {
        "psi_init": psi_init,
        "env_left": sym_env(key_left, BOND_DIM, MPO_DIM),
        "env_right": sym_env(key_right, BOND_DIM, MPO_DIM),
        "mpo_pair": sym_mpo(key_mpo, MPO_DIM, PHYS_DIM),
    }


def apply_ham(in_vec, env_left, env_right, mpo_pair):
    stage_one = jnp.einsum("alc,asub->lcsub", env_left, in_vec, precision=PREC_MODE)
    stage_two = jnp.einsum("lrsutv,lcsub->rtvcb", mpo_pair, stage_one, precision=PREC_MODE)
    return jnp.einsum("rtvcb,bre->ctve", stage_two, env_right, precision=PREC_MODE)


def project_out(krylov_basis, residual, coeffs):
    for vec_idx, basis_vec in enumerate(krylov_basis):
        residual = residual - coeffs[vec_idx] * basis_vec
    return residual


def reference(psi_init, env_left, env_right, mpo_pair):
    init_norm = jnp.sqrt(jnp.sum(psi_init * psi_init))
    krylov_basis = [psi_init / init_norm]
    alpha_list = []
    beta_list = []
    for step_idx in range(KRYLOV_STEPS):
        residual = apply_ham(krylov_basis[-1], env_left, env_right, mpo_pair)
        first_pass = jnp.stack([jnp.sum(basis_vec * residual) for basis_vec in krylov_basis])
        alpha_list.append(first_pass[-1])
        residual = project_out(krylov_basis, residual, first_pass)
        second_pass = jnp.stack([jnp.sum(basis_vec * residual) for basis_vec in krylov_basis])
        residual = project_out(krylov_basis, residual, second_pass)
        beta_val = jnp.sqrt(jnp.sum(residual * residual))
        beta_list.append(beta_val)
        krylov_basis.append(residual / beta_val)
    out_scale = math.sqrt(float(psi_init.size))
    return jnp.stack(alpha_list), jnp.stack(beta_list), krylov_basis[-1] * out_scale
```

```python
import math
import jax
import jax.numpy as jnp
from jax import lax
from jax.sharding import Mesh
from jax.sharding import PartitionSpec as P

KRYLOV_STEPS = 5
PREC_MODE = lax.Precision.HIGHEST
ALL_AXES = ("z", "yb", "ya", "x", "core")
ROW_AXES = ("core", "ya", "x")
COL_AXES = ("z", "yb")


def solution(mesh):
    grid = Mesh(mesh.devices.reshape(4, 2, 2, 4, 2), ALL_AXES)
    n_devices = grid.devices.size
    psi_spec = P("core", None, None, ("z", "yb", "ya", "x"))

    def local_fn(psi_loc, env_left, env_right, mpo_pair):
        n_total = float(psi_loc.size * n_devices)
        rows_loc = psi_loc.shape[0] // 8
        row_idx = lax.axis_index(("ya", "x"))
        left_blk = lax.dynamic_slice_in_dim(env_left, row_idx * rows_loc, rows_loc, 0)
        right_blk = lax.all_gather(env_right, ("ya", "x"), axis=0, tiled=True)
        psi = lax.all_to_all(psi_loc, ("ya", "x"), 0, 3, tiled=True)
        psi = psi.reshape(psi.shape[0], 4, psi.shape[3])
        n_mpo = mpo_pair.shape[0]
        mix = mpo_pair.reshape(n_mpo, n_mpo, 4, 4)

        def apply_ham(vec):
            full = lax.all_gather(vec, ROW_AXES, axis=0, tiled=True)
            t1 = jnp.einsum("cla,asb->lcsb", left_blk, full, precision=PREC_MODE, preferred_element_type=jnp.float32)
            t2 = jnp.einsum("lrst,lcsb->ctrb", mix, t1, precision=PREC_MODE, preferred_element_type=jnp.float32)
            part = jnp.einsum("ctrb,bre->cte", t2, right_blk, precision=PREC_MODE, preferred_element_type=jnp.float32)
            return lax.psum_scatter(part, COL_AXES, scatter_dimension=2, tiled=True)

        def dots(basis, vec, extra=()):
            loc = [jnp.sum(b * vec) for b in basis] + [jnp.sum(p * q) for p, q in extra]
            return lax.psum(jnp.stack(loc), ALL_AXES)

        raw = apply_ham(psi)
        inv0 = 1.0 / jnp.sqrt(dots([psi], psi)[0])
        basis = [psi * inv0]
        images = [raw * inv0]
        gram = {}
        alphas, betas = [], []
        for step in range(KRYLOV_STEPS):
            cur = images[-1]
            if step + 1 < KRYLOV_STEPS:
                nxt = apply_ham(cur)
            k = step + 1
            red = dots(basis, cur, [(b, basis[-1]) for b in basis])
            c1 = red[:k]
            for i in range(k):
                gram[i, step] = gram[step, i] = red[k + i]
            alphas.append(c1[-1])
            res = cur
            for i in range(k):
                res = res - c1[i] * basis[i]
            red2 = dots(basis, res, [(res, res)])
            c2 = red2[:k]
            sq = red2[k]
            for i in range(k):
                sq = sq - 2.0 * c2[i] * c2[i]
            for i in range(k):
                for m in range(k):
                    sq = sq + c2[i] * c2[m] * gram[i, m]
                res = res - c2[i] * basis[i]
            beta = jnp.sqrt(sq)
            betas.append(beta)
            inv = 1.0 / beta
            basis.append(res * inv)
            if step + 1 < KRYLOV_STEPS:
                for i in range(k):
                    nxt = nxt - (c1[i] + c2[i]) * images[i]
                images.append(nxt * inv)
        out = basis[-1] * math.sqrt(n_total)
        out = out.reshape(out.shape[0], 2, 2, out.shape[2])
        out = lax.all_to_all(out, ("ya", "x"), 3, 0, tiled=True)
        return jnp.stack(alphas), jnp.stack(betas), out

    return jax.shard_map(
        local_fn,
        mesh=grid,
        in_specs=(psi_spec, P("core", None, None), P(("z", "yb", "ya", "x"), None, None), P()),
        out_specs=(P(), P(), psi_spec),
        check_vma=False,
    )
```

```python
import functools
import math

import jax
import jax.numpy as jnp
from jax import lax
from jax.experimental import pallas as pl
from jax.experimental.pallas import tpu as pltpu
from jax.sharding import Mesh
from jax.sharding import PartitionSpec as P

STEPS = 5
AXES = ("z", "yb", "ya", "x", "core")
F32, BF16 = jnp.float32, jnp.bfloat16
MESH = pl.DeviceIdType.MESH
D = 1536
HALF = 48
NCH = 6
LANE = 128
WIDE = 256
MROWS = 768


def split3(val):
    hi = val.astype(BF16)
    rest = val - hi.astype(F32)
    mid = rest.astype(BF16)
    low = (rest - mid.astype(F32)).astype(BF16)
    return hi, mid, low


def swap(val):
    return pltpu.roll(val, 64, axis=val.ndim - 1)


def low_half(shape):
    return lax.broadcasted_iota(jnp.int32, shape, len(shape) - 1) < 64


def dot(a, b):
    return jnp.dot(a, b, preferred_element_type=F32)


def dot6(a, b, k):
    return dot(a[...], b[...]) + dot(a[:, : 2 * k], b[k:, :]) + dot(a[:, :k], b[2 * k :, :])


def mult(val, n):
    return pl.multiple_of(val, n)


def seg(i, size):
    return slice(i * size, (i + 1) * size)


def row1(i):
    return slice(i, i + 1)


def wide(val):
    return jnp.concatenate([val, val], axis=1)


def pair_halves(e, o):
    lo = low_half(e.shape)
    return jnp.where(lo, e, swap(o)), jnp.where(lo, swap(e), o)


def fold(val):
    return jnp.sum(val.reshape(-1, 8, LANE), axis=0)


def kernel(
    psi_ref, mix_ref, el_ref, rg_ref, v_out, a_out, b_out,
    l3, r3, w3, gb, v3, t1, tq, t2, o3, sb, rsb, xs, vs, u1, stage, dots, ra, rb, cg, gam, gram,
    rs_recv, rs_send, ag_recv, ag_send, fw_recv, fw_send, ra_recv, ra_send, rb_recv, rb_send, st_sem,
):
    z, yb, ya, x, core = (lax.axis_index(name) for name in AXES)
    row = lax.rem(ya + yb, 2)
    ia8 = row * 4 + x
    ia = core * 8 + ia8
    ib = z * 2 + yb

    def a_peer(d, other):
        to_row = lax.rem(row + d // 4, 2)
        return {"z": z, "yb": yb, "ya": lax.rem(to_row + yb, 2), "x": lax.rem(x + d % 4, 4), "core": 1 - core if other else core}

    def b_peer(d):
        to_yb = lax.rem(yb + d // 4, 2)
        return {"z": lax.rem(z + d % 4, 4), "yb": to_yb, "ya": lax.rem(row + to_yb, 2), "x": x, "core": core}

    def b_index(d):
        return lax.rem(z + d % 4, 4) * 2 + lax.rem(yb + d // 4, 2)

    partner = a_peer(0, True)
    a_peers = [a_peer(d, False) for d in range(1, 8)] + [a_peer(d, True) for d in range(8)]
    b_peers = [b_peer(d) for d in range(1, 8)]

    barrier = pltpu.get_barrier_semaphore()
    for peer in a_peers + b_peers:
        pl.semaphore_signal(barrier, inc=1, device_id=peer, device_id_type=MESH)
    pl.semaphore_wait(barrier, len(a_peers) + len(b_peers))

    def remote(src, dst, send, recv, peer):
        return pltpu.make_async_remote_copy(src_ref=src, dst_ref=dst, send_sem=send, recv_sem=recv, device_id=peer, device_id_type=MESH)

    def wait_bytes(ref, sem):
        pltpu.make_async_copy(ref, ref, sem).wait()

    def ag_start(par, k):
        mine = gb.at[par, k, ia]
        for d in range(1, 8):
            remote(mine, mine, ag_send.at[k], ag_recv.at[par, k], a_peer(d, False)).start()

    def ag_forward(par, k, m):
        wait_bytes(rsb.at[0, k], ag_recv.at[par, k])

        @pl.when(m > 0)
        def _():
            wait_bytes(gb.at[0, k, pl.ds(0, 8)], fw_send.at[k])

        part = gb.at[par, k, pl.ds(core * 8, 8)]
        remote(part, part, fw_send.at[k], fw_recv.at[par, k], partner).start()

    def rs_start(par, k):
        for d in range(1, 8):
            remote(sb.at[k, b_index(d)], rsb.at[par, k, d - 1], rs_send.at[k], rs_recv.at[par, k], b_peers[d - 1]).start()

    def publish(m, k, first):
        par = lax.rem(m, 2)
        if not first:
            wait_bytes(rsb.at[0, k], ag_send.at[k])
        gb[par, k, ia] = xs[m, k]
        ag_start(par, k)

    def combine(m, k):
        prev = lax.rem(m + 1, 2)
        wait_bytes(rsb.at[prev, k], rs_recv.at[prev, k])
        w = sb[k, ib]
        for d in range(7):
            w = w + rsb[prev, k, d]
        for i in range(STEPS):
            w = w - wide(gam[row1(i), :]) * xs[i + 1, k]
        xs[m, k] = w * wide(gam[row1(STEPS), :])

    def local_dots(m, k):
        last = jnp.maximum(m - 1, 0)
        cur = xs[m, k]
        new = vs[last, k]
        for i in range(STEPS):
            vec = vs[i, k]
            dots[i] = dots[i] + fold(vec * cur)
            dots[5 + i] = dots[5 + i] + fold(vec * new)

    def red_rows(which, pairs):
        ra[which, ia] = jnp.zeros((16, LANE), F32)
        for src, dst in pairs:
            ra[which, ia, row1(dst), :] = jnp.sum(dots[src], axis=0, keepdims=True)
        mine = ra.at[which, ia]
        for peer in a_peers:
            remote(mine, mine, ra_send.at[which], ra_recv.at[which], peer).start()

    def red_mid(which):
        wait_bytes(ra.at[which, pl.ds(0, 15)], ra_recv.at[which])
        wait_bytes(ra.at[which, pl.ds(0, 15)], ra_send.at[which])
        total = ra[which, 0]
        for i in range(1, 16):
            total = total + ra[which, i]
        rb[which, ib] = total
        mine = rb.at[which, ib]
        for peer in b_peers:
            remote(mine, mine, rb_send.at[which], rb_recv.at[which], peer).start()

    def red_end(which):
        wait_bytes(rb.at[which, pl.ds(0, 7)], rb_recv.at[which])
        wait_bytes(rb.at[which, pl.ds(0, 7)], rb_send.at[which])
        total = rb[which, 0]
        for i in range(1, 8):
            total = total + rb[which, i]
        return jnp.broadcast_to(jnp.sum(total, axis=1, keepdims=True), (16, LANE))

    def red1_start():
        red_rows(0, [(i, i) for i in range(5)] + [(5 + i, 8 + i) for i in range(5)])
        dots[...] = jnp.zeros_like(dots)

    def red1_end(m):
        total = red_end(0)
        cg[...] = total[0:8]
        gram[jnp.maximum(m - 1, 0)] = total[8:16]
        a_out[m] = total[0:8]

        def piece(k, _):
            cur = xs[m, k]
            for i in range(STEPS):
                cur = cur - wide(cg[row1(i), :]) * vs[i, k]
            u1[k] = cur
            for i in range(STEPS):
                dots[i] = dots[i] + fold(vs[i, k] * cur)
            dots[5] = dots[5] + fold(cur * cur)
            return 0

        lax.fori_loop(0, NCH, piece, 0)
        red_rows(1, [(i, i) for i in range(5)] + [(5, 8)])
        dots[...] = jnp.zeros_like(dots)

    def red2_end(m, last):
        total = red_end(1)
        d8 = total[0:8]
        sq = total[8:9]
        for i in range(STEPS):
            di = d8[row1(i)]
            inner = jnp.sum(d8 * gram[i], axis=0, keepdims=True)
            sq = sq - 2.0 * di * di + di * (2.0 * inner - di * gram[i, row1(i), :])
        beta = jnp.sqrt(sq)
        inv = 1.0 / beta
        b_out[m] = jnp.broadcast_to(beta, (8, LANE))
        gam[...] = cg[...] + d8
        gam[row1(STEPS), :] = inv
        scale = inv * math.sqrt(float(4 * D * D)) if last else inv
        scale = wide(scale)

        def piece(k, _):
            cur = u1[k]
            for i in range(STEPS):
                cur = cur - wide(d8[row1(i)]) * vs[i, k]
            if last:
                v_out[k] = cur * scale
            else:
                vs[m, k] = cur * scale
            return 0

        lax.fori_loop(0, NCH, piece, 0)

    def split_chunk(par, n):
        def piece(i, _):
            for h in range(2):
                r = mult(i * 96 + h * HALF, 16)
                for part, val in enumerate(reversed(split3(gb[par, 2 * n + h, i]))):
                    v3[pl.ds(part * D + r, HALF), :] = val
            return 0

        lax.fori_loop(0, 16, piece, 0)

    def mix_chunk(n):
        def quad(q, _):
            r0 = mult(q * 256, 256)
            xg = [t1[pl.ds(r0 + 64 * i, 64), :] for i in range(4)]
            for p in range(2):
                for sp in range(2):
                    e, o = (xg[2 * p + i][:, seg(sp, LANE)] for i in range(2))
                    for s, val in enumerate(pair_halves(e, o)):
                        for part, piece in enumerate(reversed(split3(val))):
                            tq[seg(4 * part + 2 * sp + s, 64), seg(p, LANE)] = piece
            out = dot6(w3, tq, WIDE)
            for p in range(2):
                pp = 2 * q + p
                h = pp // 3
                base = h * 192 + (pp - 3 * h) * 16
                for t in range(4):
                    r = mult(base + t * HALF, 16)
                    for rp in range(4):
                        e, f = (out[seg(8 * t + 2 * rp + i, 8), seg(p, LANE)] for i in range(2))
                        g = jnp.concatenate(pair_halves(e, f), axis=0)
                        for part, val in enumerate(split3(g)):
                            t2[pl.ds(r, 16), pl.ds(mult(part * D + n * 512 + rp * LANE, LANE), LANE)] = val
            return 0

        lax.fori_loop(0, 3, quad, 0)

    def out_chunk(m, k):
        n = k // 2
        h = k - 2 * n
        o3[...] = dot6(t2.at[pl.ds(mult(h * 192, 192), 192)], r3.at[:, pl.ds(mult(n * 512, 512), 512)], D)

        @pl.when(m > 0)
        def _():
            wait_bytes(rsb.at[0, k], rs_send.at[k])

        for j in range(4):
            y = [o3[seg(t, HALF), seg(j, LANE)] for t in range(4)]
            for sp in range(2):
                for i, val in enumerate(pair_halves(y[2 * sp], y[2 * sp + 1])):
                    sb[k, 2 * j + i, :, seg(sp, LANE)] = val
        rs_start(lax.rem(m, 2), k)

    def init(k, _):
        for i in range(STEPS):
            xs[i + 1, k] = jnp.zeros((HALF, WIDE), F32)
            vs[i, k] = jnp.zeros((HALF, WIDE), F32)
        xs[0, k] = psi_ref[k]
        return 0

    lax.fori_loop(0, NCH, init, 0)
    dots[...] = jnp.zeros_like(dots)
    gram[...] = jnp.zeros_like(gram)
    gam[...] = jnp.zeros_like(gam)
    for k in range(4):
        publish(0, k, True)
        local_dots(0, k)
    for part, val in enumerate(split3(mix_ref[...])):
        w3[:, seg(part, WIDE)] = val

    def el_copy(i, slot):
        return pltpu.make_async_copy(el_ref.at[pl.ds(mult(ia8 * 768 + i * HALF, HALF), HALF)], stage.at[slot], st_sem.at[slot, 0])

    el_copy(0, 0).start()

    def el_piece(i, _):
        slot = lax.rem(i, 2)

        @pl.when(i < 15)
        def _():
            el_copy(i + 1, 1 - slot).start()

        el_copy(i, slot).wait()
        for c in range(6):
            for part, val in enumerate(split3(stage[slot, :, seg(c, WIDE)])):
                l3[pl.ds(mult(i * HALF, 16), HALF), seg(6 * part + c, WIDE)] = val
        return 0

    lax.fori_loop(0, 16, el_piece, 0)

    def rg_copy(i, slot, half):
        mp = i // 8
        r = i - 8 * mp
        return pltpu.make_async_copy(
            rg_ref.at[pl.ds(mult(((2 * mp + half) * 8 + r) * 24, 24), 24)],
            stage.at[slot, pl.ds(half * 24, 24)],
            st_sem.at[slot, half],
        )

    for half in range(2):
        rg_copy(0, 0, half).start()

    def rg_piece(i, _):
        slot = lax.rem(i, 2)

        @pl.when(i < 31)
        def _():
            for half in range(2):
                rg_copy(i + 1, 1 - slot, half).start()

        for half in range(2):
            rg_copy(i, slot, half).wait()
        mp = i // 8
        r = i - 8 * mp
        lo = low_half((16, LANE))
        for g in range(3):
            bg = 3 * mp + g
            n = bg // 4
            dst = mult(n * 512 + r * 64 + (bg - 4 * n) * 16, 16)
            for j in range(4):
                tl = [stage[slot, seg(g, 16), seg(3 * j + c, LANE)] for c in range(3)]
                new = (jnp.where(lo, tl[0], tl[1]), swap(jnp.where(lo, tl[2], tl[0])), jnp.where(lo, tl[1], tl[2]))
                for c in range(3):
                    for part, val in enumerate(reversed(split3(new[c]))):
                        r3[pl.ds(part * D + dst, 16), seg(4 * c + j, LANE)] = val
        return 0

    lax.fori_loop(0, 32, rg_piece, 0)

    def step(m, _):
        par = lax.rem(m, 2)

        def chunk(n, _):
            ag_forward(par, 2 * n, m)
            ag_forward(par, 2 * n + 1, m)

            @pl.when(n < 2)
            def _():
                k = 4 + n

                @pl.when(m > 0)
                def _():
                    combine(m, k)
                    wait_bytes(rsb.at[0, k], ag_send.at[k])

                gb[par, k, ia] = xs[m, k]
                ag_start(par, k)
                local_dots(m, k)

            @pl.when(n == 1)
            def _():
                red1_start()

            for h in range(2):
                wait_bytes(gb.at[par, 2 * n + h, pl.ds((1 - core) * 8, 8)], fw_recv.at[par, 2 * n + h])
            split_chunk(par, n)
            t1[...] = dot6(l3, v3, D)
            mix_chunk(n)

            @pl.when(n == 1)
            def _():
                red_mid(0)

            return 0

        lax.fori_loop(0, 3, chunk, 0)
        red1_end(m)

        def outs(k, _):
            out_chunk(m, k)

            @pl.when(k == 2)
            def _():
                red_mid(1)

            return 0

        lax.fori_loop(0, NCH, outs, 0)
        red2_end(m, False)

        def head(k, _):
            combine(m + 1, k)
            local_dots(m + 1, k)

            @pl.when(m < STEPS - 1)
            def _():
                publish(m + 1, k, False)

            return 0

        lax.fori_loop(0, 4, head, 0)
        return 0

    lax.fori_loop(0, STEPS, step, 0)

    def tail(k, _):
        combine(STEPS, k)
        local_dots(STEPS, k)
        return 0

    lax.fori_loop(4, NCH, tail, 0)
    red1_start()
    red_mid(0)
    red1_end(STEPS)
    red_mid(1)
    red2_end(STEPS, True)
    for k in range(NCH):
        wait_bytes(rsb.at[0, k], ag_send.at[k])
        wait_bytes(rsb.at[0, k], rs_send.at[k])
        wait_bytes(gb.at[0, k, pl.ds(0, 8)], fw_send.at[k])


def run_kernel(psi, mix, el, rg):
    vmem = pl.BlockSpec(memory_space=pltpu.VMEM)
    hbm = pl.BlockSpec(memory_space=pl.ANY)
    dma = pltpu.SemaphoreType.DMA
    return pl.pallas_call(
        kernel,
        out_shape=(
            jax.ShapeDtypeStruct((NCH, HALF, WIDE), F32),
            jax.ShapeDtypeStruct((STEPS + 1, 8, LANE), F32),
            jax.ShapeDtypeStruct((STEPS + 1, 8, LANE), F32),
        ),
        in_specs=[vmem, vmem, hbm, hbm],
        out_specs=(vmem, vmem, vmem),
        scratch_shapes=[
            pltpu.VMEM((MROWS, 3 * D), BF16),
            pltpu.VMEM((3 * D, D), BF16),
            pltpu.VMEM((WIDE, MROWS), BF16),
            pltpu.VMEM((2, NCH, 16, HALF, WIDE), F32),
            pltpu.VMEM((3 * D, WIDE), BF16),
            pltpu.VMEM((MROWS, WIDE), F32),
            pltpu.VMEM((MROWS, WIDE), BF16),
            pltpu.VMEM((384, 3 * D), BF16),
            pltpu.VMEM((192, 512), F32),
            pltpu.VMEM((NCH, 8, HALF, WIDE), F32),
            pltpu.VMEM((2, NCH, 7, HALF, WIDE), F32),
            pltpu.VMEM((STEPS + 1, NCH, HALF, WIDE), F32),
            pltpu.VMEM((STEPS, NCH, HALF, WIDE), F32),
            pltpu.VMEM((NCH, HALF, WIDE), F32),
            pltpu.VMEM((2, HALF, D), F32),
            pltpu.VMEM((10, 8, LANE), F32),
            pltpu.VMEM((2, 16, 16, LANE), F32),
            pltpu.VMEM((2, 8, 16, LANE), F32),
            pltpu.VMEM((8, LANE), F32),
            pltpu.VMEM((8, LANE), F32),
            pltpu.VMEM((STEPS, 8, LANE), F32),
            dma((2, NCH)), dma((NCH,)), dma((2, NCH)), dma((NCH,)), dma((2, NCH)), dma((NCH,)),
            dma((2,)), dma((2,)), dma((2,)), dma((2,)), dma((2, 2)),
        ],
        compiler_params=pltpu.CompilerParams(collective_id=0, has_side_effects=True, vmem_limit_bytes=67043328),
        name="lanczos",
    )(psi, mix, el, rg)


def solution(mesh):
    grid = Mesh(mesh.devices.reshape(4, 2, 2, 4, 2), AXES)
    psi_spec = P("core", None, None, ("z", "yb", "ya", "x"))

    def local_fn(psi_loc, env_left, env_right, mpo_pair):
        odd = lax.axis_index("yb") == 1

        def swap_rows(val):
            return jnp.where(odd, jnp.roll(val, 384, axis=0), val)

        rg = lax.all_gather(jnp.transpose(env_right, (1, 0, 2)), ("ya", "x"), axis=0, tiled=True).reshape(D, D)
        psi = lax.all_to_all(swap_rows(psi_loc.reshape(768, 4, 24)), ("ya", "x"), 0, 2, tiled=True)
        psi = psi.reshape(2, HALF, 4, 3, 64).transpose(3, 0, 1, 2, 4).reshape(NCH, HALF, WIDE)
        w = mpo_pair.reshape(8, 8, 4, 4)
        mix = jnp.einsum("lrst,ab->trasbl", w, jnp.eye(8, dtype=F32), precision=lax.Precision.HIGHEST).reshape(256, 256)
        vec, aa, bb = run_kernel(psi, mix, env_left.reshape(6144, D), rg)
        out = vec.reshape(3, 2, HALF, 4, 64).transpose(1, 2, 3, 0, 4).reshape(96, 4, 192)
        out = swap_rows(lax.all_to_all(out, ("ya", "x"), 2, 0, tiled=True)).reshape(768, 2, 2, 24)
        alpha = jnp.stack([aa[i + 1, i, 0] for i in range(STEPS)])
        return alpha, bb[1:, 0, 0], out

    return jax.shard_map(
        local_fn,
        mesh=grid,
        in_specs=(psi_spec, P("core", None, None), P(("z", "yb", "ya", "x"), None, None), P()),
        out_specs=(P(), P(), psi_spec),
        check_vma=False,
    )
```

```python
import functools
import math

import jax
import jax.numpy as jnp
from jax import lax
from jax.experimental import pallas as pl
from jax.experimental.pallas import tpu as pltpu
from jax.sharding import Mesh
from jax.sharding import PartitionSpec as P

STEPS = 5
AXES = ("z", "yb", "ya", "x", "core")
F32, BF16 = jnp.float32, jnp.bfloat16
MESH = pl.DeviceIdType.MESH
D = 1536
HALF = 48
NCH = 6
LANE = 128
WIDE = 256
MROWS = 768


def split3(val):
    hi = val.astype(BF16)
    rest = val - hi.astype(F32)
    mid = rest.astype(BF16)
    low = (rest - mid.astype(F32)).astype(BF16)
    return hi, mid, low


def swap(val):
    return pltpu.roll(val, 64, axis=val.ndim - 1)


def low_half(shape):
    return lax.broadcasted_iota(jnp.int32, shape, len(shape) - 1) < 64


def dot(a, b):
    return jnp.dot(a, b, preferred_element_type=F32)


def dot6(a, b, k):
    return dot(a[...], b[...]) + dot(a[:, : 2 * k], b[k:, :]) + dot(a[:, :k], b[2 * k :, :])


BOTH, TRIO, QUAD = range(2), range(3), range(4)


def loop(n, body):
    def run(i, carry):
        body(i)
        return carry

    lax.fori_loop(0, n, run, 0)


def top(n):
    return pl.ds(0, n)


def mult(val, n):
    return pl.multiple_of(val, n)


def seg(i, size):
    return slice(i * size, (i + 1) * size)


def row1(i):
    return slice(i, i + 1)


def wide(val):
    return jnp.concatenate([val, val], axis=1)


def pair_halves(e, o):
    lo = low_half(e.shape)
    return jnp.where(lo, e, swap(o)), jnp.where(lo, swap(e), o)


def fold(val):
    return jnp.sum(val.reshape(-1, 8, LANE), axis=0)


def kernel(
    psi_ref, wsm_ref, el_ref, rt_ref, v_out, a_out, b_out,
    l3, r3, w3, gb, v3, t1, tq, t2, o3, sb, rsb, xs, vs, u1, stage, rbuf, pbuf, obuf, obr, dots, ra, rb, cg, gam, gram,
    rs_recv, rs_last, rs_send, ag_recv, ag_last, ag_send, fw_recv, fw_send, ra_recv, ra_send, rb_recv, rb_send,
    st_sem, rl_sem, rr_recv, rr_last, rr_send, rf_recv, rf_send, ps_recv, ps_send, ou_recv, ou_send,
):
    z, yb, ya, x, core = (lax.axis_index(name) for name in AXES)
    row = lax.rem(ya + yb, 2)
    ia8 = row * 4 + x
    ia = core * 8 + ia8
    ib = z * 2 + yb
    mem = ya * 4 + x

    def a_peer(d, other=False):
        to_row = lax.rem(row + d // 4, 2)
        return {"z": z, "yb": yb, "ya": lax.rem(to_row + yb, 2), "x": lax.rem(x + d % 4, 4), "core": 1 - core if other else core}

    def b_peer(d):
        to_yb = lax.rem(yb + d // 4, 2)
        return {"z": lax.rem(z + d % 4, 4), "yb": to_yb, "ya": lax.rem(row + to_yb, 2), "x": x, "core": core}

    partner = a_peer(0, True)
    a_peers = [a_peer(d) for d in range(1, 8)] + [a_peer(d, True) for d in range(8)]
    b_peers = [b_peer(d) for d in range(1, 8)]
    x_peers, ya_peer = a_peers[:3], a_peers[3]
    z_peers, yb_peer = b_peers[:3], b_peers[3]

    barrier = pltpu.get_barrier_semaphore()
    for peer in a_peers + b_peers:
        pl.semaphore_signal(barrier, inc=1, device_id=peer, device_id_type=MESH)
    pl.semaphore_wait(barrier, len(a_peers) + len(b_peers))

    def remote(src, dst, send, recv, peer):
        pltpu.make_async_remote_copy(src_ref=src, dst_ref=dst, send_sem=send, recv_sem=recv, device_id=peer, device_id_type=MESH).start()

    def wait_bytes(ref, sem):
        pltpu.make_async_copy(ref, ref, sem).wait()

    def blocks(k, n):
        return rsb.at[0, k, top(n)]

    def ag_first(par, k, h):
        mine = gb.at[par, k, ia]
        for peer in x_peers:
            remote(mine, mine, ag_send.at[k], (ag_recv if h else ag_last).at[par, k], peer)
        if not h:
            remote(mine, mine, ag_send.at[k], ag_recv.at[par, k], ya_peer)

    def ag_second(par, k, h):
        wait_bytes(blocks(k, 3 if h else 1), ag_recv.at[par, k])
        if h:
            part = gb.at[par, k, pl.ds(core * 8 + row * 4, 4)]
            remote(part, part, ag_send.at[k], ag_last.at[par, k], ya_peer)
        else:
            part = gb.at[par, k, core * 8 + (1 - row) * 4 + x]
            for peer in x_peers:
                remote(part, part, ag_send.at[k], ag_last.at[par, k], peer)

    def ag_forward(par, k, h, m):
        wait_bytes(blocks(k, 4 if h else 6), ag_last.at[par, k])

        @pl.when(m > 0)
        def _():
            wait_bytes(gb.at[0, k, top(8)], fw_send.at[k])

        part = gb.at[par, k, pl.ds(core * 8, 8)]
        remote(part, part, fw_send.at[k], fw_recv.at[par, k], partner)

    def rs_first(par, k, h):
        if h:
            remote(sb.at[k, pl.ds((1 - yb) * 4, 4)], rsb.at[par, k, top(4)], rs_send.at[k], rs_recv.at[par, k], yb_peer)
        else:
            for d, peer in enumerate(z_peers):
                src = sb.at[k, pl.ds(lax.rem(z + d + 1, 4) * 2, 2)]
                remote(src, rsb.at[par, k, pl.ds(2 * d, 2)], rs_send.at[k], rs_recv.at[par, k], peer)

    def rs_second(par, k, h):
        wait_bytes(blocks(k, 4 if h else 6), rs_recv.at[par, k])
        if h:
            for j in QUAD:
                sb[k, yb * 4 + j] = sb[k, yb * 4 + j] + rsb[par, k, j]
            for d, peer in enumerate(z_peers):
                src = sb.at[k, yb * 4 + lax.rem(z + d + 1, 4)]
                remote(src, rsb.at[par, k, 4 + d], rs_send.at[k], rs_last.at[par, k], peer)
        else:
            for j in BOTH:
                sb[k, z * 2 + j] = sb[k, z * 2 + j] + rsb[par, k, j] + rsb[par, k, 2 + j] + rsb[par, k, 4 + j]
            remote(sb.at[k, z * 2 + 1 - yb], rsb.at[par, k, 6], rs_send.at[k], rs_last.at[par, k], yb_peer)

    def combine(m, k, h):
        prev = lax.rem(m + 1, 2)
        wait_bytes(blocks(k, 3 if h else 1), rs_last.at[prev, k])
        if h:
            w = sb[k, yb * 4 + z] + rsb[prev, k, 4] + rsb[prev, k, 5] + rsb[prev, k, 6]
        else:
            w = sb[k, ib] + rsb[prev, k, 6]
        for i in range(STEPS):
            w = w - wide(gam[row1(i), :]) * xs[i + 1, k]
        w = w * wide(gam[row1(STEPS), :])
        xs[m, k] = w
        local_dots(m, k, w)

    def publish(m, k, h, first):
        par = lax.rem(m, 2)
        if not first:
            wait_bytes(blocks(k, 7), ag_send.at[k])
        gb[par, k, ia] = xs[m, k]
        ag_first(par, k, h)

    def local_dots(m, k, cur):
        new = vs[jnp.maximum(m - 1, 0), k]
        for i in range(STEPS):
            vec = vs[i, k]
            dots[i] = dots[i] + fold(vec * cur)
            dots[5 + i] = dots[5 + i] + fold(vec * new)

    def red_rows(which, pairs):
        ra[which, ia] = jnp.zeros((16, LANE), F32)
        for src, dst in pairs:
            ra[which, ia, row1(dst), :] = jnp.sum(dots[src], axis=0, keepdims=True)
        mine = ra.at[which, ia]
        for peer in a_peers:
            remote(mine, mine, ra_send.at[which], ra_recv.at[which], peer)
        dots[...] = jnp.zeros_like(dots)

    def red_mid(which):
        wait_bytes(ra.at[which, top(15)], ra_recv.at[which])
        wait_bytes(ra.at[which, top(15)], ra_send.at[which])
        total = ra[which, 0]
        for i in range(1, 16):
            total = total + ra[which, i]
        rb[which, ib] = total
        mine = rb.at[which, ib]
        for peer in b_peers:
            remote(mine, mine, rb_send.at[which], rb_recv.at[which], peer)

    def red_end(which):
        wait_bytes(rb.at[which, top(7)], rb_recv.at[which])
        wait_bytes(rb.at[which, top(7)], rb_send.at[which])
        total = rb[which, 0]
        for i in range(1, 8):
            total = total + rb[which, i]
        return jnp.broadcast_to(jnp.sum(total, axis=1, keepdims=True), (16, LANE))

    def red1_start():
        red_rows(0, [(i, i) for i in range(5)] + [(5 + i, 8 + i) for i in range(5)])

    def red1_end(m):
        total = red_end(0)
        cg[...] = total[0:8]
        gram[jnp.maximum(m - 1, 0)] = total[8:16]
        a_out[m] = total[0:8]

        def piece(k):
            cur = xs[m, k]
            for i in range(STEPS):
                cur = cur - wide(cg[row1(i), :]) * vs[i, k]
            u1[k] = cur
            for i in range(STEPS):
                dots[i] = dots[i] + fold(vs[i, k] * cur)
            dots[5] = dots[5] + fold(cur * cur)

        loop(NCH, piece)
        red_rows(1, [(i, i) for i in range(5)] + [(5, 8)])

    def red2_end(m, last):
        total = red_end(1)
        d8 = total[0:8]
        sq = total[8:9]
        for i in range(STEPS):
            di = d8[row1(i)]
            inner = jnp.sum(d8 * gram[i], axis=0, keepdims=True)
            sq = sq - 2.0 * di * di + di * (2.0 * inner - di * gram[i, row1(i), :])
        beta = jnp.sqrt(sq)
        inv = 1.0 / beta
        b_out[m] = jnp.broadcast_to(beta, (8, LANE))
        gam[...] = cg[...] + d8
        gam[row1(STEPS), :] = inv
        scale = wide(inv * math.sqrt(float(4 * D * D)) if last else inv)

        def piece(k):
            cur = u1[k]
            for i in range(STEPS):
                cur = cur - wide(d8[row1(i)]) * vs[i, k]
            if last:
                u1[k] = cur * scale
            else:
                vs[m, k] = cur * scale

        loop(NCH, piece)

    def split_chunk(par, n):
        def piece(i):
            for h in BOTH:
                r = mult(i * 96 + h * HALF, 16)
                for part, val in enumerate(reversed(split3(gb[par, 2 * n + h, i]))):
                    v3[pl.ds(part * D + r, HALF), :] = val

        loop(16, piece)

    def mix_chunk(n):
        def quad(q):
            r0 = mult(q * 256, 256)
            xg = [t1[pl.ds(r0 + 64 * i, 64), :] for i in QUAD]
            for p in BOTH:
                for sp in BOTH:
                    e, o = (xg[2 * p + i][:, seg(sp, LANE)] for i in BOTH)
                    for s, val in enumerate(pair_halves(e, o)):
                        for part, piece in enumerate(reversed(split3(val))):
                            tq[seg(4 * part + 2 * sp + s, 64), seg(p, LANE)] = piece
            out = dot6(w3, tq, WIDE)
            for p in BOTH:
                pp = 2 * q + p
                h = pp // 3
                base = h * 192 + (pp - 3 * h) * 16
                for t in QUAD:
                    r = mult(base + t * HALF, 16)
                    for rp in QUAD:
                        e, f = (out[seg(8 * t + 2 * rp + i, 8), seg(p, LANE)] for i in BOTH)
                        g = jnp.concatenate(pair_halves(e, f), axis=0)
                        for part, val in enumerate(split3(g)):
                            t2[pl.ds(r, 16), pl.ds(mult(part * D + n * 512 + rp * LANE, LANE), LANE)] = val

        loop(3, quad)

    def out_chunk(m, n, h):
        k = 2 * n + h
        o3[...] = dot6(t2.at[seg(h, 192)], r3.at[:, pl.ds(mult(n * 512, 512), 512)], D)

        @pl.when(m > 0)
        def _():
            wait_bytes(blocks(k, 7), rs_send.at[k])

        for j in QUAD:
            y = [o3[seg(t, HALF), seg(j, LANE)] for t in QUAD]
            for sp in BOTH:
                for i, val in enumerate(pair_halves(y[2 * sp], y[2 * sp + 1])):
                    sb[k, 4 * i + j if h else 2 * j + i, :, seg(sp, LANE)] = val
        rs_first(lax.rem(m, 2), k, h)

    def rg_first(p):
        r = core * 4 + p
        mine = rbuf.at[r, mem]
        for peer in x_peers:
            remote(mine, mine, rr_send.at[p], (rr_recv if p % 2 else rr_last).at[p], peer)
        if p % 2 == 0:
            remote(mine, mine, rr_send.at[p], rr_recv.at[p], ya_peer)

    def rg_second(p):
        r = core * 4 + p
        wait_bytes(rbuf.at[0, top(3 if p % 2 else 1)], rr_recv.at[p])
        if p % 2:
            part = rbuf.at[r, pl.ds(ya * 4, 4)]
            remote(part, part, rr_send.at[p], rr_last.at[p], ya_peer)
        else:
            part = rbuf.at[r, (1 - ya) * 4 + x]
            for peer in x_peers:
                remote(part, part, rr_send.at[p], rr_last.at[p], peer)

    def rg_forward(p):
        wait_bytes(rbuf.at[0, top(4 if p % 2 else 6)], rr_last.at[p])
        part = rbuf.at[core * 4 + p]
        remote(part, part, rf_send.at[p], rf_recv.at[p], partner)

    def rg_split(r):
        def piece(mp):
            for g in TRIO:
                bg = 3 * mp + g
                n = bg // 4
                dst = mult(n * 512 + r * 64 + (bg - 4 * n) * 16, 16)
                for j in QUAD:
                    tl = []
                    for c in TRIO:
                        eights = [rbuf[r, 2 * mp + (2 * g + e) // 3, seg((2 * g + e) % 3, 8), seg(3 * j + c, LANE)] for e in BOTH]
                        tl.append(jnp.concatenate(eights, axis=0))
                    lo = low_half(tl[0].shape)
                    new = (jnp.where(lo, tl[0], tl[1]), swap(jnp.where(lo, tl[2], tl[0])), jnp.where(lo, tl[1], tl[2]))
                    for c in TRIO:
                        for part, val in enumerate(reversed(split3(new[c]))):
                            r3[pl.ds(part * D + dst, 16), seg(4 * c + j, LANE)] = val

        loop(4, piece)

    for d, peer in enumerate(a_peers[:7]):
        to = lax.rem(row + (d + 1) // 4, 2) * 4 + lax.rem(x + (d + 1) % 4, 4)
        remote(psi_ref.at[to], pbuf.at[mem], ps_send, ps_recv, peer)
    pbuf[mem] = psi_ref[ia8]

    def rt_copy(p):
        r = core * 4 + p
        return pltpu.make_async_copy(rt_ref.at[pl.ds(mult(r * 24, 24), 24)], rbuf.at[r, mem], rl_sem.at[p])

    for p in QUAD:
        rt_copy(p).start()

    def el_copy(i, slot):
        return pltpu.make_async_copy(el_ref.at[pl.ds(mult(ia8 * 768 + i * HALF, HALF), HALF)], stage.at[slot], st_sem.at[slot])

    el_copy(0, 0).start()

    def init(k):
        for i in range(STEPS):
            xs[i + 1, k] = jnp.zeros((HALF, WIDE), F32)
            vs[i, k] = jnp.zeros((HALF, WIDE), F32)

    loop(NCH, init)
    dots[...] = jnp.zeros_like(dots)
    gram[...] = jnp.zeros_like(gram)
    gam[...] = jnp.zeros_like(gam)

    i0 = lax.broadcasted_iota(jnp.int32, (WIDE, WIDE), 0)
    i1 = lax.broadcasted_iota(jnp.int32, (WIDE, WIDE), 1)
    same = (i0 & 7) == ((i1 >> 3) & 7)
    left = ((lax.broadcasted_iota(jnp.int32, (WIDE, 32), 0) >> 3) == lax.broadcasted_iota(jnp.int32, (WIDE, 32), 1)).astype(BF16)
    c1 = lax.broadcasted_iota(jnp.int32, (32, WIDE), 1)
    right = (((c1 >> 6) * 8 + (c1 & 7)) == lax.broadcasted_iota(jnp.int32, (32, WIDE), 0)).astype(BF16)
    for part, val in enumerate(split3(wsm_ref[...])):
        full = dot(dot(left, val).astype(BF16), right)
        w3[:, seg(part, WIDE)] = jnp.where(same, full, 0.0).astype(BF16)

    wait_bytes(pbuf.at[top(7)], ps_recv)
    for i in range(8):
        for s in QUAD:
            t1[s * 192 + i * 24 : s * 192 + i * 24 + 24, 0:LANE] = pbuf[i, seg(s, 24), :]
    for n in TRIO:
        for sp in BOTH:
            tile = jnp.concatenate([t1[seg(6 * sp + 3 * i + n, 64), 0:LANE] for i in BOTH], axis=0).T
            for h in BOTH:
                xs[0, 2 * n + h, :, seg(sp, LANE)] = tile[seg(h, HALF), :]
    for k in range(NCH):
        publish(0, k, k % 2, True)
    for p in QUAD:
        rt_copy(p).wait()
        rg_first(p)

    def first_dots(k):
        local_dots(0, k, xs[0, k])

    loop(NCH, first_dots)

    def el_piece(i):
        slot = lax.rem(i, 2)

        @pl.when(i < 15)
        def _():
            el_copy(i + 1, 1 - slot).start()

        el_copy(i, slot).wait()
        for c in range(6):
            for part, val in enumerate(split3(stage[slot, :, seg(c, WIDE)])):
                l3[pl.ds(mult(i * HALF, 16), HALF), seg(6 * part + c, WIDE)] = val

    loop(16, el_piece)
    for k in QUAD:
        ag_second(0, k, k % 2)

    def step(m):
        par = lax.rem(m, 2)
        red1_start()
        for h in BOTH:
            ag_forward(par, h, h, m)

        def chunk(n):
            for h in BOTH:
                wait_bytes(gb.at[par, 2 * n + h, pl.ds((1 - core) * 8, 8)], fw_recv.at[par, 2 * n + h])
            split_chunk(par, n)
            t1[...] = dot6(l3, v3, D)

            @pl.when(n == 0)
            def _():
                for h in BOTH:
                    ag_second(par, 4 + h, h)
                for h in BOTH:
                    ag_forward(par, 2 + h, h, m)
                red_mid(0)

                @pl.when(m == 0)
                def _():
                    for p in QUAD:
                        rg_second(p)

            @pl.when(n == 1)
            def _():
                for h in BOTH:
                    ag_forward(par, 4 + h, h, m)
                red1_end(m)

            mix_chunk(n)

            @pl.when(n == 2)
            def _():
                red_mid(1)


        loop(3, chunk)

        @pl.when(m == 0)
        def _():
            for p in QUAD:
                rg_forward(p)
            for p in QUAD:
                rg_split(core * 4 + p)
            for p in QUAD:
                wait_bytes(rbuf.at[0], rf_recv.at[p])
                rg_split((1 - core) * 4 + p)

        def outs(n):
            for h in BOTH:
                out_chunk(m, n, h)

                @pl.when(n > 0)
                def _():
                    rs_second(par, 2 * n - 2 + h, h)

            @pl.when(n == 1)
            def _():
                red2_end(m, False)


        loop(3, outs)
        more = m < STEPS - 1

        def finish(k):
            combine(m + 1, k, k % 2)

            @pl.when(more)
            def _():
                publish(m + 1, k, k % 2, False)

        def spread(k):
            @pl.when(more)
            def _():
                ag_second(1 - par, k, k % 2)

        for h in BOTH:
            finish(h)
        for h in BOTH:
            rs_second(par, 4 + h, h)
        for h in BOTH:
            finish(2 + h)
        for h in BOTH:
            spread(h)
        for h in BOTH:
            finish(4 + h)
        for h in BOTH:
            spread(2 + h)

    loop(STEPS, step)

    red1_start()
    red_mid(0)
    red1_end(STEPS)
    red_mid(1)
    red2_end(STEPS, True)
    for n in TRIO:
        for sp in BOTH:
            rows = [u1[2 * n + h, :, seg(sp, LANE)] for h in BOTH] + [jnp.zeros((32, LANE), F32)]
            tile = jnp.concatenate(rows, axis=0).T
            for s in BOTH:
                for g in range(8):
                    bg = 8 * n + g
                    obuf[bg // 3, seg((2 * sp + s) * 3 + bg % 3, 8), :] = tile[seg(8 * s + g, 8), :]
    for d, peer in enumerate(a_peers[:7]):
        to_row = lax.rem(row + (d + 1) // 4, 2)
        to = lax.rem(to_row + yb, 2) * 4 + lax.rem(x + (d + 1) % 4, 4)
        remote(obuf.at[to], obr.at[ia8], ou_send, ou_recv, peer)
    obr[ia8] = obuf[mem]
    for k in range(NCH):
        wait_bytes(blocks(k, 7), ag_send.at[k])
        wait_bytes(blocks(k, 7), rs_send.at[k])
        wait_bytes(gb.at[0, k, top(8)], fw_send.at[k])
    for p in QUAD:
        wait_bytes(rbuf.at[0, top(7)], rr_send.at[p])
        wait_bytes(rbuf.at[0], rf_send.at[p])
    wait_bytes(pbuf.at[top(7)], ps_send)
    wait_bytes(obr.at[top(7)], ou_recv)
    wait_bytes(obr.at[top(7)], ou_send)
    v_out[...] = obr[...]


def run_kernel(psi, wsm, el, rt):
    vmem = pl.BlockSpec(memory_space=pltpu.VMEM)
    hbm = pl.BlockSpec(memory_space=pl.ANY)
    dma = pltpu.SemaphoreType.DMA
    return pl.pallas_call(
        kernel,
        out_shape=(
            jax.ShapeDtypeStruct((8, 96, LANE), F32),
            jax.ShapeDtypeStruct((STEPS + 1, 8, LANE), F32),
            jax.ShapeDtypeStruct((STEPS + 1, 8, LANE), F32),
        ),
        in_specs=[vmem, vmem, hbm, hbm],
        out_specs=(vmem, vmem, vmem),
        scratch_shapes=[
            pltpu.VMEM((MROWS, 3 * D), BF16),
            pltpu.VMEM((3 * D, D), BF16),
            pltpu.VMEM((WIDE, MROWS), BF16),
            pltpu.VMEM((2, NCH, 16, HALF, WIDE), F32),
            pltpu.VMEM((3 * D, WIDE), BF16),
            pltpu.VMEM((MROWS, WIDE), F32),
            pltpu.VMEM((MROWS, WIDE), BF16),
            pltpu.VMEM((384, 3 * D), BF16),
            pltpu.VMEM((192, 512), F32),
            pltpu.VMEM((NCH, 8, HALF, WIDE), F32),
            pltpu.VMEM((2, NCH, 7, HALF, WIDE), F32),
            pltpu.VMEM((STEPS + 1, NCH, HALF, WIDE), F32),
            pltpu.VMEM((STEPS, NCH, HALF, WIDE), F32),
            pltpu.VMEM((NCH, HALF, WIDE), F32),
            pltpu.VMEM((2, HALF, D), F32),
            pltpu.VMEM((8, 8, 24, D), F32),
            pltpu.VMEM((8, 96, LANE), F32),
            pltpu.VMEM((8, 96, LANE), F32),
            pltpu.VMEM((8, 96, LANE), F32),
            pltpu.VMEM((10, 8, LANE), F32),
            pltpu.VMEM((2, 16, 16, LANE), F32),
            pltpu.VMEM((2, 8, 16, LANE), F32),
            pltpu.VMEM((8, LANE), F32),
            pltpu.VMEM((8, LANE), F32),
            pltpu.VMEM((STEPS, 8, LANE), F32),
            dma((2, NCH)), dma((2, NCH)), dma((NCH,)), dma((2, NCH)), dma((2, NCH)), dma((NCH,)), dma((2, NCH)), dma((NCH,)),
            dma((2,)), dma((2,)), dma((2,)), dma((2,)),
            dma((2,)), dma((4,)), dma((4,)), dma((4,)), dma((4,)), dma((4,)), dma((4,)), dma, dma, dma, dma,
        ],
        compiler_params=pltpu.CompilerParams(collective_id=0, has_side_effects=True, vmem_limit_bytes=67043328),
        name="lanczos",
    )(psi, wsm, el, rt)


def solution(mesh):
    grid = Mesh(mesh.devices.reshape(4, 2, 2, 4, 2), AXES)
    psi_spec = P("core", None, None, ("z", "yb", "ya", "x"))

    def local_fn(psi_loc, env_left, env_right, mpo_pair):
        rt = jnp.transpose(env_right, (1, 0, 2)).reshape(192, D)
        psi = jnp.transpose(psi_loc.reshape(8, 96, 96), (0, 2, 1))
        psi = jnp.pad(psi, ((0, 0), (0, 0), (0, 32)))
        wsm = jnp.transpose(mpo_pair.reshape(8, 8, 4, 4), (3, 1, 2, 0)).reshape(32, 32)
        vec, aa, bb = run_kernel(psi, wsm, env_left.reshape(6144, D), rt)
        out = jnp.transpose(vec[:, :, :96], (0, 2, 1)).reshape(psi_loc.shape)
        alpha = jnp.stack([aa[i + 1, i, 0] for i in range(STEPS)])
        return alpha, bb[1:, 0, 0], out

    return jax.shard_map(
        local_fn,
        mesh=grid,
        in_specs=(psi_spec, P("core", None, None), P(("z", "yb", "ya", "x"), None, None), P()),
        out_specs=(P(), P(), psi_spec),
        check_vma=False,
    )
```

```python
import functools
import math

import jax
import jax.numpy as jnp
from jax import lax
from jax.experimental import pallas as pl
from jax.experimental.pallas import tpu as pltpu
from jax.sharding import Mesh
from jax.sharding import PartitionSpec as P

STEPS = 5
AXES = ("z", "yb", "ya", "x", "core")
F32, BF16 = jnp.float32, jnp.bfloat16
MESH = pl.DeviceIdType.MESH
D = 1536
HALF = 48
NCH = 6
LANE = 128
WIDE = 256
MROWS = 768
PART = 24
THIRD = 512
LAST = STEPS - 1


def split3(val):
    hi = val.astype(BF16)
    rest = val - hi.astype(F32)
    mid = rest.astype(BF16)
    low = (rest - mid.astype(F32)).astype(BF16)
    return hi, mid, low


def swap(val):
    return pltpu.roll(val, 64, axis=val.ndim - 1)


def low_half(shape):
    return lax.broadcasted_iota(jnp.int32, shape, len(shape) - 1) < 64


def dot(a, b):
    return jnp.dot(a, b, preferred_element_type=F32)


def dot6(a, b, k):
    return dot(a[...], b[...]) + dot(a[:, : 2 * k], b[k:, :]) + dot(a[:, :k], b[2 * k :, :])


BOTH, TRIO, QUAD = range(2), range(3), range(4)


def loop(n, body):
    def run(i, carry):
        body(i)
        return carry

    lax.fori_loop(0, n, run, 0)


def top(n):
    return pl.ds(0, n)


def mult(val, n):
    return pl.multiple_of(val, n)


def seg(i, size):
    return slice(i * size, (i + 1) * size)


def row1(i):
    return slice(i, i + 1)


def wide(val):
    return jnp.concatenate([val, val], axis=1)


def pair_halves(e, o):
    lo = low_half(e.shape)
    return jnp.where(lo, e, swap(o)), jnp.where(lo, swap(e), o)


def fold(val):
    return jnp.sum(val.reshape(-1, 8, LANE), axis=0)


def kernel(
    psi_ref, wsm_ref, el_ref, rt_ref, v_out, ab_out,
    l3, r3, w3, gb, v3, t1, tq, t2, o3, sz, sy, rsb, xs, vs, u1, stage, rbuf, pbuf, obuf, obr, dots, ra, rb, cg, gam, gram,
    rs_first, rs_last, rs_send, ag_first, ag_last, ag_send, fw_recv, fw_send, ra_recv, ra_send, rb_recv, rb_send,
    st_sem, rr_first, rr_last, rr_send, rf_recv, rf_send, ps_recv, ps_send, ou_recv, ou_send,
):
    z, yb, ya, x, core = (lax.axis_index(name) for name in AXES)
    row = lax.rem(ya + yb, 2)
    ia8 = row * 4 + x
    ia = core * 8 + ia8
    ib = z * 2 + yb
    mem = ya * 4 + x

    def a_peer(d, other=False):
        to_row = lax.rem(row + d // 4, 2)
        return {"z": z, "yb": yb, "ya": lax.rem(to_row + yb, 2), "x": lax.rem(x + d % 4, 4), "core": 1 - core if other else core}

    def b_peer(d):
        to_yb = lax.rem(yb + d // 4, 2)
        return {"z": lax.rem(z + d % 4, 4), "yb": to_yb, "ya": lax.rem(row + to_yb, 2), "x": x, "core": core}

    partner = a_peer(0, True)
    a_peers = [a_peer(d) for d in range(1, 8)] + [a_peer(d, True) for d in range(8)]
    b_peers = [b_peer(d) for d in range(1, 8)]
    x_peers, ya_peer = a_peers[:3], a_peers[3]
    z_peers, yb_peer = b_peers[:3], b_peers[3]

    barrier = pltpu.get_barrier_semaphore()
    for peer in a_peers + b_peers:
        pl.semaphore_signal(barrier, inc=1, device_id=peer, device_id_type=MESH)
    pl.semaphore_wait(barrier, len(a_peers) + len(b_peers))

    def remote(src, dst, send, recv, peer):
        pltpu.make_async_remote_copy(src_ref=src, dst_ref=dst, send_sem=send, recv_sem=recv, device_id=peer, device_id_type=MESH).start()

    def wait_bytes(ref, sem):
        pltpu.make_async_copy(ref, ref, sem).wait()

    def parts(k, n):
        return rsb.at[0, k, top(n)]

    upper, lower = top(PART), pl.ds(PART, PART)

    def publish(m, k, first):
        par = lax.rem(m, 2)
        if not first:
            wait_bytes(parts(k, 14), ag_send.at[k])
        gb[par, k, ia] = xs[m, k]
        low, up = gb.at[par, k, ia, lower], gb.at[par, k, ia, upper]
        for peer in x_peers:
            remote(low, low, ag_send.at[k], ag_first.at[par, k], peer)
        remote(up, up, ag_send.at[k], ag_first.at[par, k], ya_peer)
        for peer in x_peers:
            remote(up, up, ag_send.at[k], ag_last.at[par, k], peer)

    def ag_second(par, k):
        wait_bytes(parts(k, 4), ag_first.at[par, k])
        low = gb.at[par, k, pl.ds(core * 8 + row * 4, 4), lower]
        remote(low, low, ag_send.at[k], ag_last.at[par, k], ya_peer)
        up = gb.at[par, k, core * 8 + (1 - row) * 4 + x, upper]
        for peer in x_peers:
            remote(up, up, ag_send.at[k], ag_last.at[par, k], peer)

    def ag_forward(par, k, m):
        wait_bytes(parts(k, 10), ag_last.at[par, k])

        @pl.when(m > 0)
        def _():
            wait_bytes(gb.at[0, k, top(8)], fw_send.at[k])

        part = gb.at[par, k, pl.ds(core * 8, 8)]
        remote(part, part, fw_send.at[k], fw_recv.at[par, k], partner)

    def rs_start(par, k):
        remote(sy.at[k, 1 - yb], rsb.at[par, k, pl.ds(6, 4)], rs_send.at[k], rs_first.at[par, k], yb_peer)
        for d, peer in enumerate(z_peers):
            remote(sz.at[k, lax.rem(z + d + 1, 4)], rsb.at[par, k, pl.ds(2 * d, 2)], rs_send.at[k], rs_first.at[par, k], peer)

    def rs_second(par, k):
        wait_bytes(parts(k, 10), rs_first.at[par, k])
        for j in QUAD:
            sy[k, yb, j] = sy[k, yb, j] + rsb[par, k, 6 + j]
        for d, peer in enumerate(z_peers):
            remote(sy.at[k, yb, lax.rem(z + d + 1, 4)], rsb.at[par, k, 11 + d], rs_send.at[k], rs_last.at[par, k], peer)
        for j in BOTH:
            sz[k, z, j] = sz[k, z, j] + rsb[par, k, j] + rsb[par, k, 2 + j] + rsb[par, k, 4 + j]
        remote(sz.at[k, z, 1 - yb], rsb.at[par, k, 10], rs_send.at[k], rs_last.at[par, k], yb_peer)

    def combine(m, k):
        prev = lax.rem(m + 1, 2)
        wait_bytes(parts(k, 4), rs_last.at[prev, k])
        up = sz[k, z, yb] + rsb[prev, k, 10]
        low = sy[k, yb, z] + rsb[prev, k, 11] + rsb[prev, k, 12] + rsb[prev, k, 13]
        w = jnp.concatenate([up, low], axis=0)
        for i in range(STEPS):
            w = w - wide(gam[row1(i), :]) * xs[i + 1, k]
        w = w * wide(gam[row1(STEPS), :])
        xs[m, k] = w
        local_dots(m, k, w)

    def local_dots(m, k, cur):
        new = vs[jnp.maximum(m - 1, 0), k]
        for i in range(STEPS):
            vec = vs[i, k]
            dots[i] = dots[i] + fold(vec * cur)
            dots[STEPS + i] = dots[STEPS + i] + fold(vec * new)

    def red_rows(which, pairs):
        ra[which, ia] = jnp.zeros((16, LANE), F32)
        for src, dst in pairs:
            ra[which, ia, row1(dst), :] = jnp.sum(dots[src], axis=0, keepdims=True)
        mine = ra.at[which, ia]
        for peer in a_peers:
            remote(mine, mine, ra_send.at[which], ra_recv.at[which], peer)
        dots[...] = jnp.zeros_like(dots)

    def red_mid(which):
        wait_bytes(ra.at[which, top(15)], ra_recv.at[which])
        wait_bytes(ra.at[which, top(15)], ra_send.at[which])
        total = ra[which, 0]
        for i in range(1, 16):
            total = total + ra[which, i]
        rb[which, ib] = total
        mine = rb.at[which, ib]
        for peer in b_peers:
            remote(mine, mine, rb_send.at[which], rb_recv.at[which], peer)

    def red_end(which):
        wait_bytes(rb.at[which, top(7)], rb_recv.at[which])
        wait_bytes(rb.at[which, top(7)], rb_send.at[which])
        total = rb[which, 0]
        for i in range(1, 8):
            total = total + rb[which, i]
        return jnp.broadcast_to(jnp.sum(total, axis=1, keepdims=True), (16, LANE))

    def record(line, m, val):
        here = lax.broadcasted_iota(jnp.int32, (1, LANE), 1) == m - 1
        ab_out[row1(line), :] = jnp.where(here, val, ab_out[row1(line), :])

    def red1_start():
        red_rows(0, [(i, i) for i in range(STEPS)] + [(STEPS + i, 8 + i) for i in range(STEPS)])

    def red1_end(m):
        total = red_end(0)
        c8 = total[:8]
        cg[...] = c8
        gram[jnp.maximum(m - 1, 0)] = total[8:]
        now = lax.broadcasted_iota(jnp.int32, c8.shape, 0) == m - 1
        record(0, m, jnp.sum(jnp.where(now, c8, 0.0), axis=0, keepdims=True))

        def piece(k):
            cur = xs[m, k]
            for i in range(STEPS):
                cur = cur - wide(cg[row1(i), :]) * vs[i, k]
            u1[k] = cur
            for i in range(STEPS):
                dots[i] = dots[i] + fold(vs[i, k] * cur)
            dots[STEPS] = dots[STEPS] + fold(cur * cur)

        loop(NCH, piece)
        red_rows(1, [(i, i) for i in range(STEPS)] + [(STEPS, 8)])

    def red2_end(m, last):
        total = red_end(1)
        d8 = total[:8]
        sq = total[8:9]
        for i in range(STEPS):
            di = d8[row1(i)]
            inner = jnp.sum(d8 * gram[i], axis=0, keepdims=True)
            sq = sq - 2.0 * di * di + di * (2.0 * inner - di * gram[i, row1(i), :])
        beta = jnp.sqrt(sq)
        inv = 1.0 / beta
        record(1, m, beta)
        gam[...] = cg[...] + d8
        gam[row1(STEPS), :] = inv
        scale = wide(inv * math.sqrt(float(4 * D * D)) if last else inv)

        def piece(k):
            cur = u1[k]
            for i in range(STEPS):
                cur = cur - wide(d8[row1(i)]) * vs[i, k]
            if last:
                u1[k] = cur * scale
            else:
                vs[m, k] = cur * scale

        loop(NCH, piece)

    def left_half(par, k):
        wait_bytes(gb.at[par, k, pl.ds((1 - core) * 8, 8)], fw_recv.at[par, k])
        h = lax.rem(k, 2)
        base = mult(3 * MROWS * h, 3 * MROWS)

        def piece(i):
            for part, val in enumerate(reversed(split3(gb[par, k, i]))):
                v3[pl.ds(mult(base + part * MROWS + i * HALF, 16), HALF), :] = val

        loop(16, piece)
        val = dot6(l3.at[:, pl.ds(base, 3 * MROWS)], v3.at[pl.ds(base, 3 * MROWS)], MROWS)
        t1[...] = jnp.where(h == 0, 0.0, t1[...]) + val

    def mix_chunk(n):
        for q in TRIO:
            xg = [t1[seg(4 * q + i, 64), :] for i in QUAD]
            for p in BOTH:
                for sp in BOTH:
                    e, o = (xg[2 * p + i][:, seg(sp, LANE)] for i in BOTH)
                    for s, val in enumerate(pair_halves(e, o)):
                        for part, piece in enumerate(reversed(split3(val))):
                            tq[seg(4 * part + 2 * sp + s, 64), seg(2 * q + p, LANE)] = piece
        out = dot6(w3, tq, WIDE)
        for pp in range(NCH):
            h, g3 = divmod(pp, 3)
            for t in QUAD:
                for rp in QUAD:
                    e, f = (out[seg(8 * t + 2 * rp + i, 8), seg(pp, LANE)] for i in BOTH)
                    g = jnp.concatenate(pair_halves(e, f), axis=0)
                    for part, val in enumerate(split3(g)):
                        t2[seg(12 * h + 3 * t + g3, 16), pl.ds(mult(part * D + n * THIRD + rp * LANE, LANE), LANE)] = val

    def right_half(k):
        n = k // 2
        rows = t2.at[pl.ds(mult((k - 2 * n) * 192, 192), 192)]
        o3[...] = dot6(rows, r3.at[:, pl.ds(mult(n * THIRD, THIRD), THIRD)], D)

    def send_out(m, k):
        @pl.when(m > 0)
        def _():
            wait_bytes(parts(k, 14), rs_send.at[k])

        for j in QUAD:
            y = [o3[seg(t, HALF), seg(j, LANE)] for t in QUAD]
            for sp in BOTH:
                for i, val in enumerate(pair_halves(y[2 * sp], y[2 * sp + 1])):
                    sz[k, j, i, :, seg(sp, LANE)] = val[:PART]
                    sy[k, i, j, :, seg(sp, LANE)] = val[PART:]
        rs_start(lax.rem(m, 2), k)

    def rg_start(c):
        up, low = rbuf.at[c, core, mem, top(HALF)], rbuf.at[c, core, mem, pl.ds(HALF, HALF)]
        for peer in x_peers:
            remote(low, low, rr_send.at[c], rr_first.at[c], peer)
        remote(up, up, rr_send.at[c], rr_first.at[c], ya_peer)
        for peer in x_peers:
            remote(up, up, rr_send.at[c], rr_last.at[c], peer)

    def rg_bytes(n):
        return rbuf.at[0, 0, top(n)]

    def rg_second(c):
        wait_bytes(rg_bytes(2), rr_first.at[c])
        low = rbuf.at[c, core, pl.ds(ya * 4, 4), pl.ds(HALF, HALF)]
        remote(low, low, rr_send.at[c], rr_last.at[c], ya_peer)
        up = rbuf.at[c, core, (1 - ya) * 4 + x, top(HALF)]
        for peer in x_peers:
            remote(up, up, rr_send.at[c], rr_last.at[c], peer)

    def rg_split(c, half):
        def piece(i):
            mp = i // 4
            rr = i - 4 * mp
            for g in TRIO:
                bg = 3 * mp + g
                n = bg // 4
                dst = mult(n * THIRD + (half * 4 + rr) * 64 + (bg - 4 * n) * 16, 16)
                eights = []
                for e in BOTH:
                    hop, off = divmod(2 * g + e, 3)
                    eights.append(rbuf[c, half, 2 * mp + hop, pl.ds(mult(rr * PART + off * 8, 8), 8), :])
                for part, val in enumerate(reversed(split3(jnp.concatenate(eights, axis=0)))):
                    r3[pl.ds(part * D + dst, 16), pl.ds(mult(c * THIRD, THIRD), THIRD)] = val

        loop(16, piece)

    def rg_finish(c):
        wait_bytes(rg_bytes(5), rr_last.at[c])
        part = rbuf.at[c, core]
        remote(part, part, rf_send.at[c], rf_recv.at[c], partner)
        rg_split(c, core)
        wait_bytes(part, rf_recv.at[c])
        rg_split(c, 1 - core)

    for d, peer in enumerate(a_peers[:7]):
        to = lax.rem(row + (d + 1) // 4, 2) * 4 + lax.rem(x + (d + 1) % 4, 4)
        remote(psi_ref.at[to], pbuf.at[mem], ps_send, ps_recv, peer)
    pbuf[mem] = psi_ref[ia8]

    def rt_copy(i):
        return pltpu.make_async_copy(rt_ref.at[pl.ds(mult(core * 96 + i * HALF, 8), HALF)], stage.at[i], st_sem.at[i])

    def el_copy(i, slot):
        h = i // 8
        start = (h * 384 + ia8 * HALF) * 8 + (i - 8 * h) * HALF
        return pltpu.make_async_copy(el_ref.at[pl.ds(mult(start, HALF), HALF)], stage.at[slot], st_sem.at[slot])

    for i in BOTH:
        rt_copy(i).start()

    def init(k):
        for i in range(STEPS):
            xs[i + 1, k] = jnp.zeros((HALF, WIDE), F32)
            vs[i, k] = jnp.zeros((HALF, WIDE), F32)

    loop(NCH, init)
    for ref in (dots, gram, gam, ab_out):
        ref[...] = jnp.zeros_like(ref)

    i0 = lax.broadcasted_iota(jnp.int32, (WIDE, WIDE), 0)
    i1 = lax.broadcasted_iota(jnp.int32, (WIDE, WIDE), 1)
    same = (i0 & 7) == ((i1 >> 3) & 7)
    left = ((i0 >> 3) == i1)[:, :32].astype(BF16)
    right = (((i1 >> 6) * 8 + (i1 & 7)) == i0)[:32].astype(BF16)
    for part, val in enumerate(split3(wsm_ref[...])):
        full = dot(dot(left, val).astype(BF16), right)
        w3[:, seg(part, WIDE)] = jnp.where(same, full, 0.0).astype(BF16)

    wait_bytes(pbuf.at[top(7)], ps_recv)
    for i in range(8):
        for s in QUAD:
            t1[seg(8 * s + i, PART), :LANE] = pbuf[i, seg(s, PART), :]
    for n in TRIO:
        for sp in BOTH:
            tile = jnp.concatenate([t1[seg(6 * sp + 3 * i + n, 64), :LANE] for i in BOTH], axis=0).T
            for h in BOTH:
                xs[0, 2 * n + h, :, seg(sp, LANE)] = tile[seg(h, HALF), :]
        for h in BOTH:
            publish(0, 2 * n + h, True)

    def first_dots(k):
        local_dots(0, k, xs[0, k])

    loop(NCH, first_dots)
    for i in BOTH:
        rt_copy(i).wait()
        for j in QUAD:
            a, b, c = (stage[i, :, seg(3 * j + e, LANE)] for e in TRIO)
            lo = low_half(a.shape)
            for e, val in enumerate((jnp.where(lo, a, b), swap(jnp.where(lo, c, a)), jnp.where(lo, b, c))):
                rbuf[e, core, mem, seg(i, HALF), seg(j, LANE)] = val
    el_copy(0, 0).start()

    def el_piece(i):
        slot = lax.rem(i, 2)

        @pl.when(i < 15)
        def _():
            el_copy(i + 1, 1 - slot).start()

        el_copy(i, slot).wait()
        for c in BOTH:
            for h in BOTH:
                for part, val in enumerate(split3(stage[slot, :, seg(2 * c + h, 384)])):
                    l3[pl.ds(mult(i * HALF, 16), HALF), seg(6 * h + 2 * part + c, 384)] = val

    loop(16, el_piece)
    for k in TRIO:
        ag_second(0, k)
    ag_forward(0, 0, 0)

    def step(m):
        par = lax.rem(m, 2)
        nxt = 1 - par
        more, first, later = m < LAST, m == 0, m > 0

        def finish(k):
            combine(m, k)
            publish(m, k, False)

        def halves(k):
            @pl.when(k == 1)
            def _():
                pl.when(later)(lambda: finish(4))
                ag_forward(par, 1, m)
                ag_second(par, 3)
                pl.when(later)(lambda: finish(5))
                red1_start()

                @pl.when(first)
                def _():
                    ag_second(par, 4)
                    ag_second(par, 5)
                    rg_start(0)

            @pl.when(k == 2)
            def _():
                ag_forward(par, 2, m)
                pl.when(later)(lambda: ag_second(par, 4))
                ag_forward(par, 3, m)
                red_mid(0)
                pl.when(first)(lambda: rg_start(1))

            @pl.when(k == 3)
            def _():
                pl.when(later)(lambda: ag_second(par, 5))

            @pl.when(k == 4)
            def _():
                ag_forward(par, 4, m)
                red1_end(m)
                ag_forward(par, 5, m)

                @pl.when(first)
                def _():
                    rg_second(0)
                    rg_start(2)

            left_half(par, k)

            @pl.when(k == 5)
            def _():
                red_mid(1)
                pl.when(first)(lambda: rg_second(1))

            pl.when(lax.rem(k, 2) == 1)(lambda: mix_chunk(k // 2))

        loop(NCH, halves)
        pl.when(first)(lambda: rg_second(2))

        def advance(k):
            combine(m + 1, k)
            pl.when(more)(lambda: publish(m + 1, k, False))

        def spread(k):
            pl.when(more)(lambda: ag_second(nxt, k))

        def outs(k):
            @pl.when(first & (lax.rem(k, 2) == 0))
            def _():
                rg_finish(k // 2)

            right_half(k)

            @pl.when(k == 3)
            def _():
                rs_second(par, 1)
                red2_end(m, False)

            @pl.when(k == 4)
            def _():
                advance(0)
                rs_second(par, 2)

            @pl.when(k == 5)
            def _():
                rs_second(par, 3)
                spread(0)

            send_out(m, k)

            pl.when(k == 2)(lambda: rs_second(par, 0))
            pl.when(k == 4)(lambda: advance(1))

        loop(NCH, outs)
        advance(2)
        spread(1)
        rs_second(par, 4)
        pl.when(more)(lambda: ag_forward(nxt, 0, 1))
        advance(3)
        rs_second(par, 5)
        spread(2)

    loop(STEPS, step)

    combine(STEPS, 4)
    combine(STEPS, 5)
    red1_start()
    red_mid(0)
    red1_end(STEPS)
    red_mid(1)
    red2_end(STEPS, True)
    for n in TRIO:
        for sp in BOTH:
            rows = [u1[2 * n + h, :, seg(sp, LANE)] for h in BOTH] + [jnp.zeros((32, LANE), F32)]
            tile = jnp.concatenate(rows, axis=0).T
            for s in BOTH:
                for g in range(8):
                    to, off = divmod(8 * n + g, 3)
                    obuf[to, seg(6 * sp + 3 * s + off, 8), :] = tile[seg(8 * s + g, 8), :]
    for d, peer in enumerate(a_peers[:7]):
        to_row = lax.rem(row + (d + 1) // 4, 2)
        to = lax.rem(to_row + yb, 2) * 4 + lax.rem(x + (d + 1) % 4, 4)
        remote(obuf.at[to], obr.at[ia8], ou_send, ou_recv, peer)
    obr[ia8] = obuf[mem]
    for k in range(NCH):
        wait_bytes(parts(k, 14), ag_send.at[k])
        wait_bytes(parts(k, 14), rs_send.at[k])
        wait_bytes(gb.at[0, k, top(8)], fw_send.at[k])
    for c in TRIO:
        wait_bytes(rg_bytes(7), rr_send.at[c])
        wait_bytes(rbuf.at[0, 0], rf_send.at[c])
    wait_bytes(pbuf.at[top(7)], ps_send)
    wait_bytes(obr.at[top(7)], ou_recv)
    wait_bytes(obr.at[top(7)], ou_send)
    v_out[...] = obr[...]


def run_kernel(psi, wsm, el, rt):
    vmem = pl.BlockSpec(memory_space=pltpu.VMEM)
    hbm = pl.BlockSpec(memory_space=pl.ANY)
    dma = pltpu.SemaphoreType.DMA
    six, pair, three = dma((NCH,)), dma((2,)), dma((3,))
    both = dma((2, NCH))
    block = (HALF, WIDE)
    small = pltpu.VMEM((8, 96, LANE), F32)
    return pl.pallas_call(
        kernel,
        out_shape=(jax.ShapeDtypeStruct((8, 96, LANE), F32), jax.ShapeDtypeStruct((8, LANE), F32)),
        in_specs=[vmem, vmem, hbm, hbm],
        out_specs=(vmem, vmem),
        scratch_shapes=[
            pltpu.VMEM((MROWS, 3 * D), BF16),
            pltpu.VMEM((3 * D, D), BF16),
            pltpu.VMEM((WIDE, MROWS), BF16),
            pltpu.VMEM((2, NCH, 16, *block), F32),
            pltpu.VMEM((3 * D, WIDE), BF16),
            pltpu.VMEM((MROWS, WIDE), F32),
            pltpu.VMEM((MROWS, MROWS), BF16),
            pltpu.VMEM((384, 3 * D), BF16),
            pltpu.VMEM((192, THIRD), F32),
            pltpu.VMEM((NCH, 4, 2, PART, WIDE), F32),
            pltpu.VMEM((NCH, 2, 4, PART, WIDE), F32),
            pltpu.VMEM((2, NCH, 14, PART, WIDE), F32),
            pltpu.VMEM((STEPS + 1, NCH, *block), F32),
            pltpu.VMEM((STEPS, NCH, *block), F32),
            pltpu.VMEM((NCH, *block), F32),
            pltpu.VMEM((2, HALF, D), F32),
            pltpu.VMEM((3, 2, 8, 96, THIRD), F32),
            small,
            small,
            small,
            pltpu.VMEM((2 * STEPS, 8, LANE), F32),
            pltpu.VMEM((2, 16, 16, LANE), F32),
            pltpu.VMEM((2, 8, 16, LANE), F32),
            pltpu.VMEM((8, LANE), F32),
            pltpu.VMEM((8, LANE), F32),
            pltpu.VMEM((STEPS, 8, LANE), F32),
            both, both, six, both, both, six, both, six, pair, pair, pair, pair,
            pair, three, three, three, three, three, dma, dma, dma, dma,
        ],
        compiler_params=pltpu.CompilerParams(collective_id=0, has_side_effects=True, vmem_limit_bytes=67043328),
        name="lanczos",
    )(psi, wsm, el, rt)


def solution(mesh):
    grid = Mesh(mesh.devices.reshape(4, 2, 2, 4, 2), AXES)
    psi_spec = P("core", None, None, ("z", "yb", "ya", "x"))

    def local_fn(psi_loc, env_left, env_right, mpo_pair):
        rt = jnp.transpose(env_right, (1, 0, 2)).reshape(192, D)
        psi = jnp.transpose(psi_loc.reshape(2, 8, HALF, 96), (1, 3, 0, 2)).reshape(8, 96, 96)
        psi = jnp.pad(psi, ((0, 0), (0, 0), (0, LANE - 96)))
        wsm = jnp.transpose(mpo_pair.reshape(8, 8, 4, 4), (3, 1, 2, 0)).reshape(32, 32)
        vec, ab = run_kernel(psi, wsm, env_left.reshape(6144, D), rt)
        out = jnp.transpose(vec[:, :, :96].reshape(8, 96, 2, HALF), (2, 0, 3, 1)).reshape(psi_loc.shape)
        return ab[0, :STEPS], ab[1, :STEPS], out

    return jax.shard_map(
        local_fn,
        mesh=grid,
        in_specs=(psi_spec, P("core", None, None), P(("z", "yb", "ya", "x"), None, None), P()),
        out_specs=(P(), P(), psi_spec),
        check_vma=False,
    )
```

```python
import functools
import math

import jax
import jax.numpy as jnp
from jax import lax
from jax.experimental import pallas as pl
from jax.experimental.pallas import tpu as pltpu
from jax.sharding import Mesh
from jax.sharding import PartitionSpec as P

STEPS = 5
AXES = ("z", "yb", "ya", "x", "core")
F32, BF16 = jnp.float32, jnp.bfloat16
MESH = pl.DeviceIdType.MESH
D = 1536
HALF = 48
NCH = 6
LANE = 128
WIDE = 256
MROWS = 768
PART = 24
THIRD = 512
LAST = STEPS - 1


def split3(val):
    hi = val.astype(BF16)
    rest = val - hi.astype(F32)
    mid = rest.astype(BF16)
    low = (rest - mid.astype(F32)).astype(BF16)
    return hi, mid, low


def swap(val):
    return pltpu.roll(val, 64, axis=val.ndim - 1)


def low_half(shape):
    return lax.broadcasted_iota(jnp.int32, shape, len(shape) - 1) < 64


def dot(a, b):
    return jnp.dot(a, b, preferred_element_type=F32)


def dot6(a, b, k):
    return dot(a[...], b[...]) + dot(a[:, : 2 * k], b[k:, :]) + dot(a[:, :k], b[2 * k :, :])


BOTH, TRIO, QUAD = range(2), range(3), range(4)


def loop(n, body):
    def run(i, carry):
        body(i)
        return carry

    lax.fori_loop(0, n, run, 0)


def top(n):
    return pl.ds(0, n)


def mult(val, n):
    return pl.multiple_of(val, n)


def seg(i, size):
    return slice(i * size, (i + 1) * size)


def row1(i):
    return slice(i, i + 1)


def wide(val):
    return jnp.concatenate([val, val], axis=1)


def pair_halves(e, o):
    lo = low_half(e.shape)
    return jnp.where(lo, e, swap(o)), jnp.where(lo, swap(e), o)


def fold(val):
    return jnp.sum(val.reshape(-1, 8, LANE), axis=0)


def kernel(
    psi_ref, wsm_ref, el_ref, rt_ref, v_out, ab_out,
    l3, r3, w3, gb, v3, t1, tq, t2, o3, sz, sy, rsb, xs, vs, u1, stage, rbuf, pbuf, obuf, obr, dots, ra, rb, cg, gam, gram,
    rs_first, rs_last, rs_send, ag_first, ag_last, ag_send, fw_recv, fw_send, ra_recv, ra_send, rb_recv, rb_send,
    st_sem, el_sem, rr_first, rr_last, rr_send, rf_recv, rf_send, ps_recv, ps_send, ou_recv, ou_send,
):
    z, yb, ya, x, core = (lax.axis_index(name) for name in AXES)
    row = lax.rem(ya + yb, 2)
    ia8 = row * 4 + x
    ia = core * 8 + ia8
    ib = z * 2 + yb
    mem = ya * 4 + x

    def a_peer(d, other=False):
        to_row = lax.rem(row + d // 4, 2)
        return {"z": z, "yb": yb, "ya": lax.rem(to_row + yb, 2), "x": lax.rem(x + d % 4, 4), "core": 1 - core if other else core}

    def b_peer(d):
        to_yb = lax.rem(yb + d // 4, 2)
        return {"z": lax.rem(z + d % 4, 4), "yb": to_yb, "ya": lax.rem(row + to_yb, 2), "x": x, "core": core}

    partner = a_peer(0, True)
    a_peers = [a_peer(d) for d in range(1, 8)] + [a_peer(d, True) for d in range(8)]
    b_peers = [b_peer(d) for d in range(1, 8)]
    x_peers, ya_peer = a_peers[:3], a_peers[3]
    z_peers, yb_peer = b_peers[:3], b_peers[3]

    def rt_copy(i):
        return pltpu.make_async_copy(rt_ref.at[pl.ds(mult(core * 96 + i * HALF, 8), HALF)], stage.at[i], st_sem.at[i])

    psi_copy = pltpu.make_async_copy(psi_ref, obr, ou_recv)
    psi_copy.start()
    for i in BOTH:
        rt_copy(i).start()
    for c in range(NCH):
        for h in BOTH:
            src = el_ref.at[pl.ds(h * 64 + ia8 * 8, 8), :, seg(c, WIDE)]
            pltpu.make_async_copy(src, gb.at[1, c, pl.ds(8 * h, 8)], el_sem.at[c]).start()

    barrier = pltpu.get_barrier_semaphore()
    for peer in a_peers + b_peers:
        pl.semaphore_signal(barrier, inc=1, device_id=peer, device_id_type=MESH)

    def init(k):
        for i in range(STEPS):
            xs[i + 1, k] = jnp.zeros((HALF, WIDE), F32)
            vs[i, k] = jnp.zeros((HALF, WIDE), F32)

    loop(NCH, init)
    for ref in (dots, gram, gam, ab_out):
        ref[...] = jnp.zeros_like(ref)

    i0 = lax.broadcasted_iota(jnp.int32, (WIDE, WIDE), 0)
    i1 = lax.broadcasted_iota(jnp.int32, (WIDE, WIDE), 1)
    same = (i0 & 7) == ((i1 >> 3) & 7)
    left = ((i0 >> 3) == i1)[:, :32].astype(BF16)
    right = (((i1 >> 6) * 8 + (i1 & 7)) == i0)[:32].astype(BF16)
    for part, val in enumerate(split3(wsm_ref[...])):
        full = dot(dot(left, val).astype(BF16), right)
        w3[:, seg(part, WIDE)] = jnp.where(same, full, 0.0).astype(BF16)

    pl.semaphore_wait(barrier, len(a_peers) + len(b_peers))
    psi_copy.wait()

    def remote(src, dst, send, recv, peer):
        pltpu.make_async_remote_copy(src_ref=src, dst_ref=dst, send_sem=send, recv_sem=recv, device_id=peer, device_id_type=MESH).start()

    def wait_bytes(ref, sem):
        pltpu.make_async_copy(ref, ref, sem).wait()

    def parts(k, n):
        return rsb.at[0, k, top(n)]

    upper, lower = top(PART), pl.ds(PART, PART)

    def publish(m, k, first):
        par = lax.rem(m, 2)
        if not first:
            wait_bytes(parts(k, 14), ag_send.at[k])
        gb[par, k, ia] = xs[m, k]
        low, up = gb.at[par, k, ia, lower], gb.at[par, k, ia, upper]
        for peer in x_peers:
            remote(low, low, ag_send.at[k], ag_first.at[par, k], peer)
        remote(up, up, ag_send.at[k], ag_first.at[par, k], ya_peer)
        for peer in x_peers:
            remote(up, up, ag_send.at[k], ag_last.at[par, k], peer)

    def ag_second(par, k):
        wait_bytes(parts(k, 4), ag_first.at[par, k])
        low = gb.at[par, k, pl.ds(core * 8 + row * 4, 4), lower]
        remote(low, low, ag_send.at[k], ag_last.at[par, k], ya_peer)
        up = gb.at[par, k, core * 8 + (1 - row) * 4 + x, upper]
        for peer in x_peers:
            remote(up, up, ag_send.at[k], ag_last.at[par, k], peer)

    def ag_forward(par, k, m):
        wait_bytes(parts(k, 10), ag_last.at[par, k])

        @pl.when(m > 0)
        def _():
            wait_bytes(gb.at[0, k, top(8)], fw_send.at[k])

        part = gb.at[par, k, pl.ds(core * 8, 8)]
        remote(part, part, fw_send.at[k], fw_recv.at[par, k], partner)

    def rs_start(par, k):
        remote(sy.at[k, 1 - yb], rsb.at[par, k, pl.ds(6, 4)], rs_send.at[k], rs_first.at[par, k], yb_peer)
        for d, peer in enumerate(z_peers):
            remote(sz.at[k, lax.rem(z + d + 1, 4)], rsb.at[par, k, pl.ds(2 * d, 2)], rs_send.at[k], rs_first.at[par, k], peer)

    def rs_second(par, k):
        wait_bytes(parts(k, 10), rs_first.at[par, k])
        for j in QUAD:
            sy[k, yb, j] = sy[k, yb, j] + rsb[par, k, 6 + j]
        for d, peer in enumerate(z_peers):
            remote(sy.at[k, yb, lax.rem(z + d + 1, 4)], rsb.at[par, k, 11 + d], rs_send.at[k], rs_last.at[par, k], peer)
        for j in BOTH:
            sz[k, z, j] = sz[k, z, j] + rsb[par, k, j] + rsb[par, k, 2 + j] + rsb[par, k, 4 + j]
        remote(sz.at[k, z, 1 - yb], rsb.at[par, k, 10], rs_send.at[k], rs_last.at[par, k], yb_peer)

    def combine(m, k):
        prev = lax.rem(m + 1, 2)
        wait_bytes(parts(k, 4), rs_last.at[prev, k])
        up = sz[k, z, yb] + rsb[prev, k, 10]
        low = sy[k, yb, z] + rsb[prev, k, 11] + rsb[prev, k, 12] + rsb[prev, k, 13]
        w = jnp.concatenate([up, low], axis=0)
        for i in range(STEPS):
            w = w - wide(gam[row1(i), :]) * xs[i + 1, k]
        w = w * wide(gam[row1(STEPS), :])
        xs[m, k] = w
        local_dots(m, k, w)

    def local_dots(m, k, cur):
        new = vs[jnp.maximum(m - 1, 0), k]
        for i in range(STEPS):
            vec = vs[i, k]
            dots[i] = dots[i] + fold(vec * cur)
            dots[STEPS + i] = dots[STEPS + i] + fold(vec * new)

    def red_rows(which, pairs):
        ra[which, ia] = jnp.zeros((16, LANE), F32)
        for src, dst in pairs:
            ra[which, ia, row1(dst), :] = jnp.sum(dots[src], axis=0, keepdims=True)
        mine = ra.at[which, ia]
        for peer in a_peers:
            remote(mine, mine, ra_send.at[which], ra_recv.at[which], peer)
        dots[...] = jnp.zeros_like(dots)

    def red_mid(which):
        wait_bytes(ra.at[which, top(15)], ra_recv.at[which])
        wait_bytes(ra.at[which, top(15)], ra_send.at[which])
        total = ra[which, 0]
        for i in range(1, 16):
            total = total + ra[which, i]
        rb[which, ib] = total
        mine = rb.at[which, ib]
        for peer in b_peers:
            remote(mine, mine, rb_send.at[which], rb_recv.at[which], peer)

    def red_end(which):
        wait_bytes(rb.at[which, top(7)], rb_recv.at[which])
        wait_bytes(rb.at[which, top(7)], rb_send.at[which])
        total = rb[which, 0]
        for i in range(1, 8):
            total = total + rb[which, i]
        return jnp.broadcast_to(jnp.sum(total, axis=1, keepdims=True), (16, LANE))

    def record(line, m, val):
        here = lax.broadcasted_iota(jnp.int32, (1, LANE), 1) == m - 1
        ab_out[row1(line), :] = jnp.where(here, val, ab_out[row1(line), :])

    def red1_start():
        red_rows(0, [(i, i) for i in range(STEPS)] + [(STEPS + i, 8 + i) for i in range(STEPS)])

    def red1_end(m):
        total = red_end(0)
        c8 = total[:8]
        cg[...] = c8
        gram[jnp.maximum(m - 1, 0)] = total[8:]
        now = lax.broadcasted_iota(jnp.int32, c8.shape, 0) == m - 1
        record(0, m, jnp.sum(jnp.where(now, c8, 0.0), axis=0, keepdims=True))

        def piece(k):
            cur = xs[m, k]
            for i in range(STEPS):
                cur = cur - wide(cg[row1(i), :]) * vs[i, k]
            u1[k] = cur
            for i in range(STEPS):
                dots[i] = dots[i] + fold(vs[i, k] * cur)
            dots[STEPS] = dots[STEPS] + fold(cur * cur)

        loop(NCH, piece)
        red_rows(1, [(i, i) for i in range(STEPS)] + [(STEPS, 8)])

    def red2_end(m, last):
        total = red_end(1)
        d8 = total[:8]
        sq = total[8:9]
        for i in range(STEPS):
            di = d8[row1(i)]
            inner = jnp.sum(d8 * gram[i], axis=0, keepdims=True)
            sq = sq - 2.0 * di * di + di * (2.0 * inner - di * gram[i, row1(i), :])
        beta = jnp.sqrt(sq)
        inv = 1.0 / beta
        record(1, m, beta)
        gam[...] = cg[...] + d8
        gam[row1(STEPS), :] = inv
        scale = wide(inv * math.sqrt(float(4 * D * D)) if last else inv)

        def piece(k):
            cur = u1[k]
            for i in range(STEPS):
                cur = cur - wide(d8[row1(i)]) * vs[i, k]
            if last:
                u1[k] = cur * scale
            else:
                vs[m, k] = cur * scale

        loop(NCH, piece)

    def left_half(par, k):
        wait_bytes(gb.at[par, k, pl.ds((1 - core) * 8, 8)], fw_recv.at[par, k])
        h = lax.rem(k, 2)
        base = mult(3 * MROWS * h, 3 * MROWS)

        def piece(i):
            for part, val in enumerate(reversed(split3(gb[par, k, i]))):
                v3[pl.ds(mult(base + part * MROWS + i * HALF, 16), HALF), :] = val

        loop(16, piece)
        val = dot6(l3.at[:, pl.ds(base, 3 * MROWS)], v3.at[pl.ds(base, 3 * MROWS)], MROWS)
        t1[...] = jnp.where(h == 0, 0.0, t1[...]) + val

    def mix_chunk(n):
        for q in TRIO:
            xg = [t1[seg(4 * q + i, 64), :] for i in QUAD]
            for p in BOTH:
                for sp in BOTH:
                    e, o = (xg[2 * p + i][:, seg(sp, LANE)] for i in BOTH)
                    for s, val in enumerate(pair_halves(e, o)):
                        for part, piece in enumerate(reversed(split3(val))):
                            tq[seg(4 * part + 2 * sp + s, 64), seg(2 * q + p, LANE)] = piece
        out = dot6(w3, tq, WIDE)
        for pp in range(NCH):
            h, g3 = divmod(pp, 3)
            for t in QUAD:
                for rp in QUAD:
                    e, f = (out[seg(8 * t + 2 * rp + i, 8), seg(pp, LANE)] for i in BOTH)
                    g = jnp.concatenate(pair_halves(e, f), axis=0)
                    for part, val in enumerate(split3(g)):
                        t2[seg(12 * h + 3 * t + g3, 16), pl.ds(mult(part * D + n * THIRD + rp * LANE, LANE), LANE)] = val

    def right_half(k):
        n = k // 2
        rows = t2.at[pl.ds(mult((k - 2 * n) * 192, 192), 192)]
        o3[...] = dot6(rows, r3.at[:, pl.ds(mult(n * THIRD, THIRD), THIRD)], D)

    def send_out(m, k):
        @pl.when(m > 0)
        def _():
            wait_bytes(parts(k, 14), rs_send.at[k])

        for j in QUAD:
            y = [o3[seg(t, HALF), seg(j, LANE)] for t in QUAD]
            for sp in BOTH:
                for i, val in enumerate(pair_halves(y[2 * sp], y[2 * sp + 1])):
                    sz[k, j, i, :, seg(sp, LANE)] = val[:PART]
                    sy[k, i, j, :, seg(sp, LANE)] = val[PART:]
        rs_start(lax.rem(m, 2), k)

    def rg_start(c):
        up, low = rbuf.at[c, core, mem, top(HALF)], rbuf.at[c, core, mem, pl.ds(HALF, HALF)]
        for peer in x_peers:
            remote(low, low, rr_send.at[c], rr_first.at[c], peer)
        remote(up, up, rr_send.at[c], rr_first.at[c], ya_peer)
        for peer in x_peers:
            remote(up, up, rr_send.at[c], rr_last.at[c], peer)

    def rg_bytes(n):
        return rbuf.at[0, 0, top(n)]

    def rg_second(c):
        wait_bytes(rg_bytes(2), rr_first.at[c])
        low = rbuf.at[c, core, pl.ds(ya * 4, 4), pl.ds(HALF, HALF)]
        remote(low, low, rr_send.at[c], rr_last.at[c], ya_peer)
        up = rbuf.at[c, core, (1 - ya) * 4 + x, top(HALF)]
        for peer in x_peers:
            remote(up, up, rr_send.at[c], rr_last.at[c], peer)

    def rg_split(c, half):
        def piece(i):
            mp = i // 4
            rr = i - 4 * mp
            for g in TRIO:
                bg = 3 * mp + g
                n = bg // 4
                dst = mult(n * THIRD + (half * 4 + rr) * 64 + (bg - 4 * n) * 16, 16)
                eights = []
                for e in BOTH:
                    hop, off = divmod(2 * g + e, 3)
                    eights.append(rbuf[c, half, 2 * mp + hop, pl.ds(mult(rr * PART + off * 8, 8), 8), :])
                for part, val in enumerate(reversed(split3(jnp.concatenate(eights, axis=0)))):
                    r3[pl.ds(part * D + dst, 16), pl.ds(mult(c * THIRD, THIRD), THIRD)] = val

        loop(16, piece)

    def rg_forward(c):
        wait_bytes(rg_bytes(5), rr_last.at[c])
        part = rbuf.at[c, core]
        remote(part, part, rf_send.at[c], rf_recv.at[c], partner)

    def rg_other(c):
        wait_bytes(rbuf.at[c, 1 - core], rf_recv.at[c])
        rg_split(c, 1 - core)

    for d, peer in enumerate(a_peers[:7]):
        to = lax.rem(row + (d + 1) // 4, 2) * 4 + lax.rem(x + (d + 1) % 4, 4)
        remote(obr.at[to], pbuf.at[mem], ps_send, ps_recv, peer)
    pbuf[mem] = obr[ia8]

    for i in BOTH:
        rt_copy(i).wait()
        for j in QUAD:
            a, b, c = (stage[i, :, seg(3 * j + e, LANE)] for e in TRIO)
            lo = low_half(a.shape)
            for e, val in enumerate((jnp.where(lo, a, b), swap(jnp.where(lo, c, a)), jnp.where(lo, b, c))):
                rbuf[e, core, mem, seg(i, HALF), seg(j, LANE)] = val
    rg_start(0)

    wait_bytes(pbuf.at[top(7)], ps_recv)
    wait_bytes(pbuf.at[top(7)], ps_send)
    for i in range(8):
        for s in QUAD:
            t1[seg(8 * s + i, PART), :LANE] = pbuf[i, seg(s, PART), :]
    for n in TRIO:
        for sp in BOTH:
            tile = jnp.concatenate([t1[seg(6 * sp + 3 * i + n, 64), :LANE] for i in BOTH], axis=0).T
            for h in BOTH:
                xs[0, 2 * n + h, :, seg(sp, LANE)] = tile[seg(h, HALF), :]

    def first_dots(k):
        local_dots(0, k, xs[0, k])

    def el_piece(i):
        for t in range(12):
            c, h = divmod(t // 3, 2)
            for part, val in enumerate(split3(gb[1, t // 2, i, :, seg(t % 2, LANE)])):
                l3[pl.ds(mult(i * HALF, 16), HALF), seg(3 * (6 * h + 2 * part + c) + t % 3, LANE)] = val

    for c in range(NCH):
        wait_bytes(gb.at[1, c], el_sem.at[c])

    def lead(e):
        @pl.when(e == 0)
        def _():
            for k in TRIO:
                publish(0, k, True)

        @pl.when(e == 1)
        def _():
            publish(0, 3, True)
            publish(0, 4, True)
            loop(NCH, first_dots)

        @pl.when(e == 2)
        def _():
            ag_second(0, 0)
            rg_second(0)
            ag_second(0, 1)
            publish(0, 5, True)

        @pl.when(e == 3)
        def _():
            ag_second(0, 3)
            ag_second(0, 2)
            rg_forward(0)

        loop(4, lambda i: el_piece(4 * e + i))

    loop(4, lead)
    ag_second(0, 5)
    rg_start(1)
    rg_split(0, core)
    rg_other(0)
    ag_second(0, 4)
    ag_forward(0, 0, 0)

    def step(m):
        par = lax.rem(m, 2)
        nxt = 1 - par
        more, first, later = m < LAST, m == 0, m > 0

        def finish(k):
            combine(m, k)
            publish(m, k, False)

        def halves(k):
            @pl.when(k == 1)
            def _():
                ag_forward(par, 1, m)

                @pl.when(later)
                def _():
                    ag_second(par, 3)
                    finish(5)

                red1_start()

                @pl.when(first)
                def _():
                    rg_start(2)
                    rg_second(1)

            @pl.when(k == 2)
            def _():
                pl.when(later)(lambda: ag_second(par, 4))
                ag_forward(par, 3, m)
                red_mid(0)
                pl.when(later)(lambda: ag_second(par, 5))

            @pl.when(k == 4)
            def _():
                red1_end(m)
                ag_forward(par, 5, m)
                pl.when(first)(lambda: rg_second(2))

            left_half(par, k)

            pl.when(k == 1)(lambda: ag_forward(par, 2, m))
            pl.when(k == 3)(lambda: ag_forward(par, 4, m))
            pl.when(lax.rem(k, 2) == 1)(lambda: mix_chunk(k // 2))

        loop(NCH, halves)
        red_mid(1)

        def advance(k):
            combine(m + 1, k)
            pl.when(more)(lambda: publish(m + 1, k, False))

        def spread(k):
            pl.when(more)(lambda: ag_second(nxt, k))

        def outs(k):
            pl.when(first & (k == 1))(lambda: rg_forward(1))

            @pl.when(first & (k == 2))
            def _():
                rg_split(1, core)
                rg_other(1)
                rg_forward(2)
                rg_split(2, core)

            pl.when(first & (k == 4))(lambda: rg_other(2))
            right_half(k)
            pl.when(k == 3)(lambda: rs_second(par, 1))

            @pl.when(k == 5)
            def _():
                advance(1)
                rs_second(par, 3)

            send_out(m, k)

            @pl.when(k == 2)
            def _():
                red2_end(m, False)
                rs_second(par, 0)

            @pl.when(k == 4)
            def _():
                rs_second(par, 2)
                advance(0)

        loop(NCH, outs)
        spread(0)
        rs_second(par, 4)
        advance(2)
        spread(1)
        advance(3)
        pl.when(more)(lambda: ag_forward(nxt, 0, 1))
        rs_second(par, 5)
        spread(2)
        advance(4)

    loop(STEPS, step)

    combine(STEPS, 5)
    red1_start()
    red_mid(0)
    red1_end(STEPS)
    red_mid(1)
    red2_end(STEPS, True)
    for n in TRIO:
        for sp in BOTH:
            rows = [u1[2 * n + h, :, seg(sp, LANE)] for h in BOTH] + [jnp.zeros((32, LANE), F32)]
            tile = jnp.concatenate(rows, axis=0).T
            for s in BOTH:
                for g in range(8):
                    to, off = divmod(8 * n + g, 3)
                    obuf[to, seg(6 * sp + 3 * s + off, 8), :] = tile[seg(8 * s + g, 8), :]
    for d, peer in enumerate(a_peers[:7]):
        to_row = lax.rem(row + (d + 1) // 4, 2)
        to = lax.rem(to_row + yb, 2) * 4 + lax.rem(x + (d + 1) % 4, 4)
        remote(obuf.at[to], obr.at[ia8], ou_send, ou_recv, peer)
    obr[ia8] = obuf[mem]
    for k in range(NCH):
        wait_bytes(parts(k, 14), ag_send.at[k])
        wait_bytes(parts(k, 14), rs_send.at[k])
        wait_bytes(gb.at[0, k, top(8)], fw_send.at[k])
    for c in TRIO:
        wait_bytes(rg_bytes(7), rr_send.at[c])
        wait_bytes(rbuf.at[0, 0], rf_send.at[c])
    wait_bytes(obr.at[top(7)], ou_recv)
    wait_bytes(obr.at[top(7)], ou_send)
    v_out[...] = obr[...]


def run_kernel(psi, wsm, el, rt):
    vmem = pl.BlockSpec(memory_space=pltpu.VMEM)
    hbm = pl.BlockSpec(memory_space=pl.ANY)
    dma = pltpu.SemaphoreType.DMA
    six, pair, three = dma((NCH,)), dma((2,)), dma((3,))
    both = dma((2, NCH))
    block = (HALF, WIDE)
    small = pltpu.VMEM((8, 96, LANE), F32)
    return pl.pallas_call(
        kernel,
        out_shape=(jax.ShapeDtypeStruct((8, 96, LANE), F32), jax.ShapeDtypeStruct((8, LANE), F32)),
        in_specs=[hbm, vmem, hbm, hbm],
        out_specs=(vmem, vmem),
        scratch_shapes=[
            pltpu.VMEM((MROWS, 3 * D), BF16),
            pltpu.VMEM((3 * D, D), BF16),
            pltpu.VMEM((WIDE, MROWS), BF16),
            pltpu.VMEM((2, NCH, 16, *block), F32),
            pltpu.VMEM((3 * D, WIDE), BF16),
            pltpu.VMEM((MROWS, WIDE), F32),
            pltpu.VMEM((MROWS, MROWS), BF16),
            pltpu.VMEM((384, 3 * D), BF16),
            pltpu.VMEM((192, THIRD), F32),
            pltpu.VMEM((NCH, 4, 2, PART, WIDE), F32),
            pltpu.VMEM((NCH, 2, 4, PART, WIDE), F32),
            pltpu.VMEM((2, NCH, 14, PART, WIDE), F32),
            pltpu.VMEM((STEPS + 1, NCH, *block), F32),
            pltpu.VMEM((STEPS, NCH, *block), F32),
            pltpu.VMEM((NCH, *block), F32),
            pltpu.VMEM((2, HALF, D), F32),
            pltpu.VMEM((3, 2, 8, 96, THIRD), F32),
            small,
            small,
            small,
            pltpu.VMEM((2 * STEPS, 8, LANE), F32),
            pltpu.VMEM((2, 16, 16, LANE), F32),
            pltpu.VMEM((2, 8, 16, LANE), F32),
            pltpu.VMEM((8, LANE), F32),
            pltpu.VMEM((8, LANE), F32),
            pltpu.VMEM((STEPS, 8, LANE), F32),
            both, both, six, both, both, six, both, six, pair, pair, pair, pair,
            pair, six, three, three, three, three, three, dma, dma, dma, dma,
        ],
        compiler_params=pltpu.CompilerParams(collective_id=0, has_side_effects=True, vmem_limit_bytes=67043328),
        name="lanczos",
    )(psi, wsm, el, rt)


def solution(mesh):
    grid = Mesh(mesh.devices.reshape(4, 2, 2, 4, 2), AXES)
    psi_spec = P("core", None, None, ("z", "yb", "ya", "x"))

    def local_fn(psi_loc, env_left, env_right, mpo_pair):
        rt = jnp.transpose(env_right, (1, 0, 2)).reshape(192, D)
        psi = jnp.transpose(psi_loc.reshape(2, 8, HALF, 96), (1, 3, 0, 2)).reshape(8, 96, 96)
        psi = jnp.pad(psi, ((0, 0), (0, 0), (0, LANE - 96)))
        wsm = jnp.transpose(mpo_pair.reshape(8, 8, 4, 4), (3, 1, 2, 0)).reshape(32, 32)
        vec, ab = run_kernel(psi, wsm, env_left.reshape(LANE, HALF, D), rt)
        out = jnp.transpose(vec[:, :, :96].reshape(8, 96, 2, HALF), (2, 0, 3, 1)).reshape(psi_loc.shape)
        return ab[0, :STEPS], ab[1, :STEPS], out

    return jax.shard_map(
        local_fn,
        mesh=grid,
        in_specs=(psi_spec, P("core", None, None), P(("z", "yb", "ya", "x"), None, None), P()),
        out_specs=(P(), P(), psi_spec),
        check_vma=False,
    )
```

```python
import functools
import math

import jax
import jax.numpy as jnp
from jax import lax
from jax.experimental import pallas as pl
from jax.experimental.pallas import tpu as pltpu
from jax.sharding import Mesh
from jax.sharding import PartitionSpec as P

STEPS = 5
AXES = ("z", "yb", "ya", "x", "core")
F32, BF16 = jnp.float32, jnp.bfloat16
MESH = pl.DeviceIdType.MESH
D = 1536
HALF = 48
NCH = 6
LANE = 128
WIDE = 256
MROWS = 768
PART = 24
THIRD = 512
LAST = STEPS - 1


def split3(val):
    hi = val.astype(BF16)
    rest = val - hi.astype(F32)
    mid = rest.astype(BF16)
    low = (rest - mid.astype(F32)).astype(BF16)
    return hi, mid, low


def swap(val):
    return pltpu.roll(val, 64, axis=val.ndim - 1)


def low_half(shape):
    return lax.broadcasted_iota(jnp.int32, shape, len(shape) - 1) < 64


def dot(a, b):
    return jnp.dot(a, b, preferred_element_type=F32)


def dot6(a, b, k):
    return dot(a[...], b[...]) + dot(a[:, : 2 * k], b[k:, :]) + dot(a[:, :k], b[2 * k :, :])


BOTH, TRIO, QUAD = range(2), range(3), range(4)


def loop(n, body):
    def run(i, carry):
        body(i)
        return carry

    lax.fori_loop(0, n, run, 0)


def top(n):
    return pl.ds(0, n)


def mult(val, n):
    return pl.multiple_of(val, n)


def seg(i, size):
    return slice(i * size, (i + 1) * size)


def row1(i):
    return slice(i, i + 1)


def wide(val):
    return jnp.concatenate([val, val], axis=1)


def pair_halves(e, o):
    lo = low_half(e.shape)
    return jnp.where(lo, e, swap(o)), jnp.where(lo, swap(e), o)


def fold(val):
    return jnp.sum(val.reshape(-1, 8, LANE), axis=0)


def kernel(
    psi_ref, wsm_ref, el_ref, rt_ref, v_out, ab_out,
    l3, r3, w3, gb, v3, t1, tq, t2, o3, sz, sy, rsb, xs, vs, u1, stage, rbuf, pbuf, obuf, obr, dots, ra, rb, cg, gam, gram,
    rs_first, rs_last, rs_send, ag_first, ag_last, ag_send, fw_recv, fw_send, ra_recv, ra_send, rb_recv, rb_send,
    st_sem, el_sem, rr_first, rr_last, rr_send, rf_recv, rf_send, ps_recv, ps_send, in_sem, ex_send, ex_recv,
):
    z, yb, ya, x, core = (lax.axis_index(name) for name in AXES)
    row = lax.rem(ya + yb, 2)
    ia8 = row * 4 + x
    ia = core * 8 + ia8
    ib = z * 2 + yb
    mem = ya * 4 + x

    def a_peer(d, other=False):
        to_row = lax.rem(row + d // 4, 2)
        return {"z": z, "yb": yb, "ya": lax.rem(to_row + yb, 2), "x": lax.rem(x + d % 4, 4), "core": 1 - core if other else core}

    def b_peer(d):
        to_yb = lax.rem(yb + d // 4, 2)
        return {"z": lax.rem(z + d % 4, 4), "yb": to_yb, "ya": lax.rem(row + to_yb, 2), "x": x, "core": core}

    partner = a_peer(0, True)
    a_peers = [a_peer(d) for d in range(1, 8)] + [a_peer(d, True) for d in range(8)]
    b_peers = [b_peer(d) for d in range(1, 8)]
    x_peers, ya_peer = a_peers[:3], a_peers[3]
    z_peers, yb_peer = b_peers[:3], b_peers[3]

    def rt_copy(p):
        dst = stage.at[p // 2, pl.ds(PART * (p % 2), PART)]
        return pltpu.make_async_copy(rt_ref.at[:, core * 4 + p, :], dst, st_sem.at[p])

    psi_copy = pltpu.make_async_copy(psi_ref, obr, in_sem)
    psi_copy.start()
    for p in QUAD:
        rt_copy(p).start()
    for c in range(NCH):
        for h in BOTH:
            src = el_ref.at[pl.ds(h * 64 + ia8 * 8, 8), :, seg(c, WIDE)]
            pltpu.make_async_copy(src, gb.at[1, c, pl.ds(8 * h, 8)], el_sem.at[c]).start()

    barrier = pltpu.get_barrier_semaphore()
    for peer in a_peers + b_peers:
        pl.semaphore_signal(barrier, inc=1, device_id=peer, device_id_type=MESH)

    def init(k):
        for i in range(STEPS):
            xs[i + 1, k] = jnp.zeros((HALF, WIDE), F32)
            vs[i, k] = jnp.zeros((HALF, WIDE), F32)

    loop(NCH, init)
    for ref in (dots, gram, gam, ab_out):
        ref[...] = jnp.zeros_like(ref)

    i0 = lax.broadcasted_iota(jnp.int32, (WIDE, WIDE), 0)
    i1 = lax.broadcasted_iota(jnp.int32, (WIDE, WIDE), 1)
    same = (i0 & 7) == ((i1 >> 3) & 7)
    left = ((i0 >> 3) == i1)[:, :32].astype(BF16)
    right = (((i1 >> 6) * 8 + (i1 & 7)) == i0)[:32].astype(BF16)
    for part, val in enumerate(split3(wsm_ref[...])):
        full = dot(dot(left, val).astype(BF16), right)
        w3[:, seg(part, WIDE)] = jnp.where(same, full, 0.0).astype(BF16)

    pl.semaphore_wait(barrier, len(a_peers) + len(b_peers))
    psi_copy.wait()

    def remote(src, dst, send, recv, peer):
        pltpu.make_async_remote_copy(src_ref=src, dst_ref=dst, send_sem=send, recv_sem=recv, device_id=peer, device_id_type=MESH).start()

    def wait_bytes(ref, sem):
        pltpu.make_async_copy(ref, ref, sem).wait()

    def parts(k, n):
        return rsb.at[0, k, top(n)]

    upper, lower = top(PART), pl.ds(PART, PART)

    def publish(m, k, first):
        par = lax.rem(m, 2)
        if not first:
            wait_bytes(parts(k, 14), ag_send.at[k])
        gb[par, k, ia] = xs[m, k]
        low, up = gb.at[par, k, ia, lower], gb.at[par, k, ia, upper]
        for peer in x_peers:
            remote(low, low, ag_send.at[k], ag_first.at[par, k], peer)
        remote(up, up, ag_send.at[k], ag_first.at[par, k], ya_peer)
        for peer in x_peers:
            remote(up, up, ag_send.at[k], ag_last.at[par, k], peer)

    def ag_second(par, k):
        wait_bytes(parts(k, 4), ag_first.at[par, k])
        low = gb.at[par, k, pl.ds(core * 8 + row * 4, 4), lower]
        remote(low, low, ag_send.at[k], ag_last.at[par, k], ya_peer)
        up = gb.at[par, k, core * 8 + (1 - row) * 4 + x, upper]
        for peer in x_peers:
            remote(up, up, ag_send.at[k], ag_last.at[par, k], peer)

    def ag_forward(par, k, m):
        wait_bytes(parts(k, 10), ag_last.at[par, k])

        @pl.when(m > 0)
        def _():
            wait_bytes(gb.at[0, k, top(8)], fw_send.at[k])

        part = gb.at[par, k, pl.ds(core * 8, 8)]
        remote(part, part, fw_send.at[k], fw_recv.at[par, k], partner)

    def rs_start(par, k):
        remote(sy.at[k, 1 - yb], rsb.at[par, k, pl.ds(6, 4)], rs_send.at[k], rs_first.at[par, k], yb_peer)
        for d, peer in enumerate(z_peers):
            remote(sz.at[k, lax.rem(z + d + 1, 4)], rsb.at[par, k, pl.ds(2 * d, 2)], rs_send.at[k], rs_first.at[par, k], peer)

    def rs_second(par, k):
        wait_bytes(parts(k, 10), rs_first.at[par, k])
        for j in QUAD:
            sy[k, yb, j] = sy[k, yb, j] + rsb[par, k, 6 + j]
        for d, peer in enumerate(z_peers):
            remote(sy.at[k, yb, lax.rem(z + d + 1, 4)], rsb.at[par, k, 11 + d], rs_send.at[k], rs_last.at[par, k], peer)
        for j in BOTH:
            sz[k, z, j] = sz[k, z, j] + rsb[par, k, j] + rsb[par, k, 2 + j] + rsb[par, k, 4 + j]
        remote(sz.at[k, z, 1 - yb], rsb.at[par, k, 10], rs_send.at[k], rs_last.at[par, k], yb_peer)

    def combine(m, k):
        prev = lax.rem(m + 1, 2)
        wait_bytes(parts(k, 4), rs_last.at[prev, k])
        up = sz[k, z, yb] + rsb[prev, k, 10]
        low = sy[k, yb, z] + rsb[prev, k, 11] + rsb[prev, k, 12] + rsb[prev, k, 13]
        w = jnp.concatenate([up, low], axis=0)
        for i in range(STEPS):
            w = w - wide(gam[row1(i), :]) * xs[i + 1, k]
        w = w * wide(gam[row1(STEPS), :])
        xs[m, k] = w
        local_dots(m, k, w)

    def local_dots(m, k, cur):
        new = vs[jnp.maximum(m - 1, 0), k]
        for i in range(STEPS):
            vec = vs[i, k]
            dots[i] = dots[i] + fold(vec * cur)
            dots[STEPS + i] = dots[STEPS + i] + fold(vec * new)

    def red_rows(which, pairs):
        ra[which, ia] = jnp.zeros((16, LANE), F32)
        for src, dst in pairs:
            ra[which, ia, row1(dst), :] = jnp.sum(dots[src], axis=0, keepdims=True)
        mine = ra.at[which, ia]
        for peer in a_peers:
            remote(mine, mine, ra_send.at[which], ra_recv.at[which], peer)
        dots[...] = jnp.zeros_like(dots)

    def red_mid(which):
        wait_bytes(ra.at[which, top(15)], ra_recv.at[which])
        wait_bytes(ra.at[which, top(15)], ra_send.at[which])
        total = ra[which, 0]
        for i in range(1, 16):
            total = total + ra[which, i]
        rb[which, ib] = total
        mine = rb.at[which, ib]
        for peer in b_peers:
            remote(mine, mine, rb_send.at[which], rb_recv.at[which], peer)

    def red_end(which):
        wait_bytes(rb.at[which, top(7)], rb_recv.at[which])
        wait_bytes(rb.at[which, top(7)], rb_send.at[which])
        total = rb[which, 0]
        for i in range(1, 8):
            total = total + rb[which, i]
        return jnp.broadcast_to(jnp.sum(total, axis=1, keepdims=True), (16, LANE))

    def record(line, m, val):
        here = lax.broadcasted_iota(jnp.int32, (1, LANE), 1) == m - 1
        ab_out[row1(line), :] = jnp.where(here, val, ab_out[row1(line), :])

    def red1_start():
        red_rows(0, [(i, i) for i in range(STEPS)] + [(STEPS + i, 8 + i) for i in range(STEPS)])

    def red1_end(m):
        total = red_end(0)
        c8 = total[:8]
        cg[...] = c8
        gram[jnp.maximum(m - 1, 0)] = total[8:]
        now = lax.broadcasted_iota(jnp.int32, c8.shape, 0) == m - 1
        record(0, m, jnp.sum(jnp.where(now, c8, 0.0), axis=0, keepdims=True))

        def piece(k):
            cur = xs[m, k]
            for i in range(STEPS):
                cur = cur - wide(cg[row1(i), :]) * vs[i, k]
            u1[k] = cur
            for i in range(STEPS):
                dots[i] = dots[i] + fold(vs[i, k] * cur)
            dots[STEPS] = dots[STEPS] + fold(cur * cur)

        loop(NCH, piece)
        red_rows(1, [(i, i) for i in range(STEPS)] + [(STEPS, 8)])

    def spare(i, slot):
        return rbuf.at[i // 2, lax.rem(i, 2), slot, :, top(LANE)]

    def export_pack(vec):
        for n in TRIO:
            for sp in BOTH:
                rows = [vec[2 * n + h, :, seg(sp, LANE)] for h in BOTH] + [jnp.zeros((32, LANE), F32)]
                tile = jnp.concatenate(rows, axis=0).T
                for s in BOTH:
                    for g in range(8):
                        to, off = divmod(8 * n + g, 3)
                        obuf[to, seg(6 * sp + 3 * s + off, 8), :] = tile[seg(8 * s + g, 8), :]

    def export_send(i):
        for d, peer in enumerate(a_peers[:7]):
            to_row = lax.rem(row + (d + 1) // 4, 2)
            to = lax.rem(to_row + yb, 2) * 4 + lax.rem(x + (d + 1) % 4, 4)
            remote(obuf.at[to], spare(i, ia8), ex_send, ex_recv.at[i], peer)
        spare(i, ia8)[...] = obuf[mem]

    def export_done():
        wait_bytes(obuf.at[top(7)], ex_send)

    def red2_end(m, last):
        total = red_end(1)
        d8 = total[:8]
        sq = total[8:9]
        for i in range(STEPS):
            di = d8[row1(i)]
            inner = jnp.sum(d8 * gram[i], axis=0, keepdims=True)
            sq = sq - 2.0 * di * di + di * (2.0 * inner - di * gram[i, row1(i), :])
        beta = jnp.sqrt(sq)
        inv = 1.0 / beta
        record(1, m, beta)
        gam[...] = cg[...] + d8
        gam[row1(STEPS), :] = inv
        if last:
            scale = inv * math.sqrt(float(4 * D * D))
            for i in range(NCH):
                wait_bytes(obuf.at[top(7)], ex_recv.at[i])

            def final(j):
                cur = spare(STEPS, j)[...]
                for i in range(STEPS):
                    cur = cur - d8[row1(i)] * spare(i, j)[...]
                v_out[j] = (cur * scale)[:, :96]

            loop(8, final)
        else:

            def piece(k):
                cur = u1[k]
                for i in range(STEPS):
                    cur = cur - wide(d8[row1(i)]) * vs[i, k]
                vs[m, k] = cur * wide(inv)

            loop(NCH, piece)

    def left_half(par, k):
        wait_bytes(gb.at[par, k, pl.ds((1 - core) * 8, 8)], fw_recv.at[par, k])
        h = lax.rem(k, 2)
        base = mult(3 * MROWS * h, 3 * MROWS)

        def piece(i):
            for part, val in enumerate(reversed(split3(gb[par, k, i]))):
                v3[pl.ds(mult(base + part * MROWS + i * HALF, 16), HALF), :] = val

        loop(16, piece)
        val = dot6(l3.at[:, pl.ds(base, 3 * MROWS)], v3.at[pl.ds(base, 3 * MROWS)], MROWS)
        t1[...] = jnp.where(h == 0, 0.0, t1[...]) + val

    def mix_chunk(n):
        for q in TRIO:
            xg = [t1[seg(4 * q + i, 64), :] for i in QUAD]
            for p in BOTH:
                for sp in BOTH:
                    e, o = (xg[2 * p + i][:, seg(sp, LANE)] for i in BOTH)
                    for s, val in enumerate(pair_halves(e, o)):
                        for part, piece in enumerate(reversed(split3(val))):
                            tq[seg(4 * part + 2 * sp + s, 64), seg(2 * q + p, LANE)] = piece
        out = dot6(w3, tq, WIDE)
        for pp in range(NCH):
            h, g3 = divmod(pp, 3)
            for t in QUAD:
                for rp in QUAD:
                    e, f = (out[seg(8 * t + 2 * rp + i, 8), seg(pp, LANE)] for i in BOTH)
                    g = jnp.concatenate(pair_halves(e, f), axis=0)
                    for part, val in enumerate(split3(g)):
                        t2[seg(12 * h + 3 * t + g3, 16), pl.ds(mult(part * D + n * THIRD + rp * LANE, LANE), LANE)] = val

    def right_half(k):
        n = k // 2
        rows = t2.at[pl.ds(mult((k - 2 * n) * 192, 192), 192)]
        o3[...] = dot6(rows, r3.at[:, pl.ds(mult(n * THIRD, THIRD), THIRD)], D)

    def send_out(m, k):
        @pl.when(m > 0)
        def _():
            wait_bytes(parts(k, 14), rs_send.at[k])

        for j in QUAD:
            y = [o3[seg(t, HALF), seg(j, LANE)] for t in QUAD]
            for sp in BOTH:
                for i, val in enumerate(pair_halves(y[2 * sp], y[2 * sp + 1])):
                    sz[k, j, i, :, seg(sp, LANE)] = val[:PART]
                    sy[k, i, j, :, seg(sp, LANE)] = val[PART:]
        rs_start(lax.rem(m, 2), k)

    def rg_start(c):
        up, low = rbuf.at[c, core, mem, top(HALF)], rbuf.at[c, core, mem, pl.ds(HALF, HALF)]
        for peer in x_peers:
            remote(low, low, rr_send.at[c], rr_first.at[c], peer)
        remote(up, up, rr_send.at[c], rr_first.at[c], ya_peer)
        for peer in x_peers:
            remote(up, up, rr_send.at[c], rr_last.at[c], peer)

    def rg_bytes(n):
        return rbuf.at[0, 0, top(n)]

    def rg_second(c):
        wait_bytes(rg_bytes(2), rr_first.at[c])
        low = rbuf.at[c, core, pl.ds(ya * 4, 4), pl.ds(HALF, HALF)]
        remote(low, low, rr_send.at[c], rr_last.at[c], ya_peer)
        up = rbuf.at[c, core, (1 - ya) * 4 + x, top(HALF)]
        for peer in x_peers:
            remote(up, up, rr_send.at[c], rr_last.at[c], peer)

    def rg_split(c, half):
        def piece(i):
            mp = i // 4
            rr = i - 4 * mp
            for g in TRIO:
                bg = 3 * mp + g
                n = bg // 4
                dst = mult(n * THIRD + (half * 4 + rr) * 64 + (bg - 4 * n) * 16, 16)
                eights = []
                for e in BOTH:
                    hop, off = divmod(2 * g + e, 3)
                    eights.append(rbuf[c, half, 2 * mp + hop, pl.ds(mult(rr * PART + off * 8, 8), 8), :])
                for part, val in enumerate(reversed(split3(jnp.concatenate(eights, axis=0)))):
                    r3[pl.ds(part * D + dst, 16), pl.ds(mult(c * THIRD, THIRD), THIRD)] = val

        loop(16, piece)

    def rg_forward(c):
        wait_bytes(rg_bytes(5), rr_last.at[c])
        part = rbuf.at[c, core]
        remote(part, part, rf_send.at[c], rf_recv.at[c], partner)

    def rg_other(c):
        wait_bytes(rbuf.at[c, 1 - core], rf_recv.at[c])
        rg_split(c, 1 - core)

    for d, peer in enumerate(a_peers[:7]):
        to = lax.rem(row + (d + 1) // 4, 2) * 4 + lax.rem(x + (d + 1) % 4, 4)
        remote(obr.at[to], pbuf.at[mem], ps_send, ps_recv, peer)
    pbuf[mem] = obr[ia8]

    for p in QUAD:
        rt_copy(p).wait()
    for i in BOTH:
        for j in QUAD:
            a, b, c = (stage[i, :, seg(3 * j + e, LANE)] for e in TRIO)
            lo = low_half(a.shape)
            for e, val in enumerate((jnp.where(lo, a, b), swap(jnp.where(lo, c, a)), jnp.where(lo, b, c))):
                rbuf[e, core, mem, seg(i, HALF), seg(j, LANE)] = val
    rg_start(0)

    wait_bytes(pbuf.at[top(7)], ps_recv)
    wait_bytes(pbuf.at[top(7)], ps_send)
    for i in range(8):
        for s in QUAD:
            t1[seg(8 * s + i, PART), :96] = pbuf[i, seg(s, PART), :]
    for n in TRIO:
        for sp in BOTH:
            tile = jnp.concatenate([t1[seg(6 * sp + 3 * i + n, 64), :LANE] for i in BOTH], axis=0).T
            for h in BOTH:
                xs[0, 2 * n + h, :, seg(sp, LANE)] = tile[seg(h, HALF), :]

    def first_dots(k):
        local_dots(0, k, xs[0, k])

    def el_piece(i):
        for t in range(12):
            c, h = divmod(t // 3, 2)
            for part, val in enumerate(split3(gb[1, t // 2, i, :, seg(t % 2, LANE)])):
                l3[pl.ds(mult(i * HALF, 16), HALF), seg(3 * (6 * h + 2 * part + c) + t % 3, LANE)] = val

    for c in range(NCH):
        wait_bytes(gb.at[1, c], el_sem.at[c])

    def lead(e):
        @pl.when(e == 0)
        def _():
            for k in TRIO:
                publish(0, k, True)

        @pl.when(e == 1)
        def _():
            publish(0, 3, True)
            publish(0, 4, True)
            loop(NCH, first_dots)

        @pl.when(e == 2)
        def _():
            ag_second(0, 0)
            rg_second(0)
            ag_second(0, 1)
            publish(0, 5, True)

        @pl.when(e == 3)
        def _():
            ag_second(0, 3)
            ag_second(0, 2)
            rg_forward(0)

        loop(4, lambda i: el_piece(4 * e + i))

    loop(4, lead)
    ag_second(0, 5)
    rg_start(1)
    rg_split(0, core)
    rg_other(0)
    ag_second(0, 4)
    ag_forward(0, 0, 0)

    def step(m):
        par = lax.rem(m, 2)
        nxt = 1 - par
        more, first, later = m < LAST, m == 0, m > 0

        def finish(k):
            combine(m, k)
            publish(m, k, False)

        def halves(k):
            @pl.when(k == 1)
            def _():
                ag_forward(par, 1, m)

                @pl.when(later)
                def _():
                    ag_second(par, 3)
                    finish(5)

                red1_start()

                @pl.when(first)
                def _():
                    rg_start(2)
                    rg_second(1)

            @pl.when(k == 2)
            def _():
                pl.when(later)(lambda: ag_second(par, 4))
                ag_forward(par, 3, m)
                red_mid(0)
                pl.when(later)(lambda: ag_second(par, 5))

            @pl.when(k == 4)
            def _():
                red1_end(m)
                ag_forward(par, 5, m)
                pl.when(first)(lambda: rg_second(2))

            left_half(par, k)

            pl.when(k == 1)(lambda: ag_forward(par, 2, m))
            pl.when(k == 3)(lambda: ag_forward(par, 4, m))
            pl.when(lax.rem(k, 2) == 1)(lambda: mix_chunk(k // 2))

        loop(NCH, halves)
        pl.when(later)(lambda: export_send(m - 1))
        red_mid(1)

        def advance(k):
            combine(m + 1, k)
            pl.when(more)(lambda: publish(m + 1, k, False))

        def spread(k):
            pl.when(more)(lambda: ag_second(nxt, k))

        def outs(k):
            pl.when(first & (k == 1))(lambda: rg_forward(1))

            @pl.when(first & (k == 2))
            def _():
                rg_split(1, core)
                rg_other(1)
                rg_forward(2)
                rg_split(2, core)

            pl.when(first & (k == 4))(lambda: rg_other(2))
            right_half(k)
            pl.when(k == 3)(lambda: rs_second(par, 1))

            @pl.when(k == 5)
            def _():
                advance(1)
                rs_second(par, 3)

            send_out(m, k)

            @pl.when(k == 2)
            def _():
                red2_end(m, False)
                rs_second(par, 0)

            @pl.when(k == 4)
            def _():
                rs_second(par, 2)
                advance(0)

        loop(NCH, outs)

        @pl.when(first)
        def _():
            for c in TRIO:
                wait_bytes(rg_bytes(7), rr_send.at[c])
                wait_bytes(rbuf.at[0, 0], rf_send.at[c])

        spread(0)
        rs_second(par, 4)
        advance(2)
        spread(1)
        advance(3)
        pl.when(more)(lambda: ag_forward(nxt, 0, 1))
        rs_second(par, 5)
        spread(2)
        advance(4)
        pl.when(later)(export_done)
        export_pack(vs.at[m])

    loop(STEPS, step)

    export_send(LAST)
    combine(STEPS, 5)
    red1_start()
    red_mid(0)
    red1_end(STEPS)
    export_done()
    export_pack(u1)
    export_send(STEPS)
    red_mid(1)
    red2_end(STEPS, True)
    export_done()
    for k in range(NCH):
        wait_bytes(parts(k, 14), ag_send.at[k])
        wait_bytes(parts(k, 14), rs_send.at[k])
        wait_bytes(gb.at[0, k, top(8)], fw_send.at[k])


def run_kernel(psi, wsm, el, rt):
    vmem = pl.BlockSpec(memory_space=pltpu.VMEM)
    hbm = pl.BlockSpec(memory_space=pl.ANY)
    dma = pltpu.SemaphoreType.DMA
    six, pair, three = dma((NCH,)), dma((2,)), dma((3,))
    both = dma((2, NCH))
    block = (HALF, WIDE)
    start = pltpu.VMEM((8, 96, 96), F32)
    return pl.pallas_call(
        kernel,
        out_shape=(jax.ShapeDtypeStruct((8, 96, 96), F32), jax.ShapeDtypeStruct((8, LANE), F32)),
        in_specs=[hbm, vmem, hbm, hbm],
        out_specs=(vmem, vmem),
        scratch_shapes=[
            pltpu.VMEM((MROWS, 3 * D), BF16),
            pltpu.VMEM((3 * D, D), BF16),
            pltpu.VMEM((WIDE, MROWS), BF16),
            pltpu.VMEM((2, NCH, 16, *block), F32),
            pltpu.VMEM((3 * D, WIDE), BF16),
            pltpu.VMEM((MROWS, WIDE), F32),
            pltpu.VMEM((MROWS, MROWS), BF16),
            pltpu.VMEM((384, 3 * D), BF16),
            pltpu.VMEM((192, THIRD), F32),
            pltpu.VMEM((NCH, 4, 2, PART, WIDE), F32),
            pltpu.VMEM((NCH, 2, 4, PART, WIDE), F32),
            pltpu.VMEM((2, NCH, 14, PART, WIDE), F32),
            pltpu.VMEM((STEPS + 1, NCH, *block), F32),
            pltpu.VMEM((STEPS, NCH, *block), F32),
            pltpu.VMEM((NCH, *block), F32),
            pltpu.VMEM((2, HALF, D), F32),
            pltpu.VMEM((3, 2, 8, 96, THIRD), F32),
            start,
            pltpu.VMEM((8, 96, LANE), F32),
            start,
            pltpu.VMEM((2 * STEPS, 8, LANE), F32),
            pltpu.VMEM((2, 16, 16, LANE), F32),
            pltpu.VMEM((2, 8, 16, LANE), F32),
            pltpu.VMEM((8, LANE), F32),
            pltpu.VMEM((8, LANE), F32),
            pltpu.VMEM((STEPS, 8, LANE), F32),
            both, both, six, both, both, six, both, six, pair, pair, pair, pair,
            dma((4,)), six, three, three, three, three, three, dma, dma, dma, dma, six,
        ],
        compiler_params=pltpu.CompilerParams(collective_id=0, has_side_effects=True, vmem_limit_bytes=67043328),
        name="lanczos",
    )(psi, wsm, el, rt)


def solution(mesh):
    grid = Mesh(mesh.devices.reshape(4, 2, 2, 4, 2), AXES)
    psi_spec = P("core", None, None, ("z", "yb", "ya", "x"))

    def local_fn(psi_loc, env_left, env_right, mpo_pair):
        psi = jnp.transpose(psi_loc.reshape(2, 8, HALF, 96), (1, 3, 0, 2)).reshape(8, 96, 96)
        wsm = jnp.transpose(mpo_pair.reshape(8, 8, 4, 4), (3, 1, 2, 0)).reshape(32, 32)
        vec, ab = run_kernel(psi, wsm, env_left.reshape(LANE, HALF, D), env_right)
        out = jnp.transpose(vec.reshape(8, 96, 2, HALF), (2, 0, 3, 1)).reshape(psi_loc.shape)
        return ab[0, :STEPS], ab[1, :STEPS], out

    return jax.shard_map(
        local_fn,
        mesh=grid,
        in_specs=(psi_spec, P("core", None, None), P(("z", "yb", "ya", "x"), None, None), P()),
        out_specs=(P(), P(), psi_spec),
        check_vma=False,
    )
```

```python
import functools
import math

import jax
import jax.numpy as jnp
from jax import lax
from jax.experimental import pallas as pl
from jax.experimental.pallas import tpu as pltpu
from jax.sharding import Mesh
from jax.sharding import PartitionSpec as P

STEPS = 5
AXES = ("z", "yb", "ya", "x", "core")
F32, BF16 = jnp.float32, jnp.bfloat16
MESH = pl.DeviceIdType.MESH
D = 1536
HALF = 48
NCH = 6
LANE = 128
WIDE = 256
MROWS = 768
PART = 24
THIRD = 512
LAST = STEPS - 1


def split3(val):
    hi = val.astype(BF16)
    rest = val - hi.astype(F32)
    mid = rest.astype(BF16)
    low = (rest - mid.astype(F32)).astype(BF16)
    return hi, mid, low


def swap(val):
    return pltpu.roll(val, 64, axis=val.ndim - 1)


def low_half(shape):
    return lax.broadcasted_iota(jnp.int32, shape, len(shape) - 1) < 64


def dot(a, b):
    return jnp.dot(a, b, preferred_element_type=F32)


def dot6(a, b, k):
    return dot(a[...], b[...]) + dot(a[:, : 2 * k], b[k:, :]) + dot(a[:, :k], b[2 * k :, :])


BOTH, TRIO, QUAD = range(2), range(3), range(4)


def loop(n, body):
    def run(i, carry):
        body(i)
        return carry

    lax.fori_loop(0, n, run, 0)


def top(n):
    return pl.ds(0, n)


def mult(val, n):
    return pl.multiple_of(val, n)


def seg(i, size):
    return slice(i * size, (i + 1) * size)


def row1(i):
    return slice(i, i + 1)


def wide(val):
    return jnp.concatenate([val, val], axis=1)


def pair_halves(e, o):
    lo = low_half(e.shape)
    return jnp.where(lo, e, swap(o)), jnp.where(lo, swap(e), o)


def fold(val):
    return jnp.sum(val.reshape(-1, 8, LANE), axis=0)


def kernel(
    psi_ref, wsm_ref, el_ref, rt_ref, v_out, ab_out,
    l3, r3, w3, gb, v3, t1, tq, t2, o3, sz, sy, rsb, xs, vs, u1, stage, rbuf, pbuf, obuf, obr, dots, ra, rb, cg, gam, gram,
    rs_first, rs_last, rs_send, ag_first, ag_last, ag_send, fw_recv, fw_send, ra_recv, ra_send, rb_recv, rb_send,
    st_sem, el_sem, rr_first, rr_last, rr_send, rf_recv, rf_send, ps_recv, ps_send, in_sem, ex_send, ex_recv,
):
    z, yb, ya, x, core = (lax.axis_index(name) for name in AXES)
    row = lax.rem(ya + yb, 2)
    ia8 = row * 4 + x
    ia = core * 8 + ia8
    ib = z * 2 + yb
    mem = ya * 4 + x

    def a_peer(d, other=False):
        to_row = lax.rem(row + d // 4, 2)
        return {"z": z, "yb": yb, "ya": lax.rem(to_row + yb, 2), "x": lax.rem(x + d % 4, 4), "core": 1 - core if other else core}

    def b_peer(d):
        to_yb = lax.rem(yb + d // 4, 2)
        return {"z": lax.rem(z + d % 4, 4), "yb": to_yb, "ya": lax.rem(row + to_yb, 2), "x": x, "core": core}

    partner = a_peer(0, True)
    a_peers = [a_peer(d) for d in range(1, 8)] + [a_peer(d, True) for d in range(8)]
    b_peers = [b_peer(d) for d in range(1, 8)]
    x_peers, ya_peer = a_peers[:3], a_peers[3]
    z_peers, yb_peer = b_peers[:3], b_peers[3]

    def rt_copy(p):
        dst = stage.at[p // 2, pl.ds(PART * (p % 2), PART)]
        return pltpu.make_async_copy(rt_ref.at[:, core * 4 + p, :], dst, st_sem.at[p])

    psi_copy = pltpu.make_async_copy(psi_ref, obr, in_sem)
    psi_copy.start()
    for p in QUAD:
        rt_copy(p).start()
    for c in range(NCH):
        for h in BOTH:
            src = el_ref.at[pl.ds(h * 64 + ia8 * 8, 8), :, seg(c, WIDE)]
            pltpu.make_async_copy(src, gb.at[1, c, pl.ds(8 * h, 8)], el_sem.at[c]).start()

    barrier = pltpu.get_barrier_semaphore()
    for peer in a_peers + b_peers:
        pl.semaphore_signal(barrier, inc=1, device_id=peer, device_id_type=MESH)

    def init(k):
        for i in range(STEPS):
            xs[i + 1, k] = jnp.zeros((HALF, WIDE), F32)
            vs[i, k] = jnp.zeros((HALF, WIDE), F32)

    loop(NCH, init)
    for ref in (dots, gram, gam, ab_out):
        ref[...] = jnp.zeros_like(ref)

    i0 = lax.broadcasted_iota(jnp.int32, (WIDE, WIDE), 0)
    i1 = lax.broadcasted_iota(jnp.int32, (WIDE, WIDE), 1)
    same = (i0 & 7) == ((i1 >> 3) & 7)
    left = ((i0 >> 3) == i1)[:, :32].astype(BF16)
    right = (((i1 >> 6) * 8 + (i1 & 7)) == i0)[:32].astype(BF16)
    for part, val in enumerate(split3(wsm_ref[...])):
        full = dot(dot(left, val).astype(BF16), right)
        w3[:, seg(part, WIDE)] = jnp.where(same, full, 0.0).astype(BF16)

    pl.semaphore_wait(barrier, len(a_peers) + len(b_peers))
    psi_copy.wait()

    def remote(src, dst, send, recv, peer):
        pltpu.make_async_remote_copy(src_ref=src, dst_ref=dst, send_sem=send, recv_sem=recv, device_id=peer, device_id_type=MESH).start()

    def wait_bytes(ref, sem):
        pltpu.make_async_copy(ref, ref, sem).wait()

    def parts(k, n):
        return rsb.at[0, k, top(n)]

    upper, lower = top(PART), pl.ds(PART, PART)

    def publish(m, k, first):
        par = lax.rem(m, 2)
        if not first:
            wait_bytes(parts(k, 14), ag_send.at[k])
        gb[par, k, ia] = xs[m, k]
        low, up = gb.at[par, k, ia, lower], gb.at[par, k, ia, upper]
        for peer in x_peers:
            remote(low, low, ag_send.at[k], ag_first.at[par, k], peer)
        remote(up, up, ag_send.at[k], ag_first.at[par, k], ya_peer)
        for peer in x_peers:
            remote(up, up, ag_send.at[k], ag_last.at[par, k], peer)

    def ag_second(par, k):
        wait_bytes(parts(k, 4), ag_first.at[par, k])
        low = gb.at[par, k, pl.ds(core * 8 + row * 4, 4), lower]
        remote(low, low, ag_send.at[k], ag_last.at[par, k], ya_peer)
        up = gb.at[par, k, core * 8 + (1 - row) * 4 + x, upper]
        for peer in x_peers:
            remote(up, up, ag_send.at[k], ag_last.at[par, k], peer)

    def ag_forward(par, k, m):
        wait_bytes(parts(k, 10), ag_last.at[par, k])

        @pl.when(m > 0)
        def _():
            wait_bytes(gb.at[0, k, top(8)], fw_send.at[k])

        part = gb.at[par, k, pl.ds(core * 8, 8)]
        remote(part, part, fw_send.at[k], fw_recv.at[par, k], partner)
        split_blocks(par, k, core)

    def split_blocks(par, k, who):
        base = 3 * MROWS * lax.rem(k, 2) + who * 384

        def piece(i):
            for part, val in enumerate(reversed(split3(gb[par, k, who * 8 + i]))):
                v3[pl.ds(mult(base + part * MROWS + i * HALF, 16), HALF), :] = val

        loop(8, piece)

    def rs_start(par, k):
        remote(sy.at[k, 1 - yb], rsb.at[par, k, pl.ds(6, 4)], rs_send.at[k], rs_first.at[par, k], yb_peer)
        for d, peer in enumerate(z_peers):
            remote(sz.at[k, lax.rem(z + d + 1, 4)], rsb.at[par, k, pl.ds(2 * d, 2)], rs_send.at[k], rs_first.at[par, k], peer)

    def rs_second(par, k):
        wait_bytes(parts(k, 10), rs_first.at[par, k])
        for j in QUAD:
            sy[k, yb, j] = sy[k, yb, j] + rsb[par, k, 6 + j]
        for d, peer in enumerate(z_peers):
            remote(sy.at[k, yb, lax.rem(z + d + 1, 4)], rsb.at[par, k, 11 + d], rs_send.at[k], rs_last.at[par, k], peer)
        for j in BOTH:
            sz[k, z, j] = sz[k, z, j] + rsb[par, k, j] + rsb[par, k, 2 + j] + rsb[par, k, 4 + j]
        remote(sz.at[k, z, 1 - yb], rsb.at[par, k, 10], rs_send.at[k], rs_last.at[par, k], yb_peer)

    def combine(m, k):
        prev = lax.rem(m + 1, 2)
        wait_bytes(parts(k, 4), rs_last.at[prev, k])
        up = sz[k, z, yb] + rsb[prev, k, 10]
        low = sy[k, yb, z] + rsb[prev, k, 11] + rsb[prev, k, 12] + rsb[prev, k, 13]
        w = jnp.concatenate([up, low], axis=0)
        for i in range(STEPS):
            w = w - wide(gam[row1(i), :]) * xs[i + 1, k]
        w = w * wide(gam[row1(STEPS), :])
        xs[m, k] = w
        local_dots(m, k, w)

    def local_dots(m, k, cur):
        new = vs[jnp.maximum(m - 1, 0), k]
        for i in range(STEPS):
            vec = vs[i, k]
            dots[i] = dots[i] + fold(vec * cur)
            dots[STEPS + i] = dots[STEPS + i] + fold(vec * new)

    def red_rows(which, pairs):
        ra[which, ia] = jnp.zeros((16, LANE), F32)
        for src, dst in pairs:
            ra[which, ia, row1(dst), :] = jnp.sum(dots[src], axis=0, keepdims=True)
        mine = ra.at[which, ia]
        for peer in a_peers:
            remote(mine, mine, ra_send.at[which], ra_recv.at[which], peer)
        dots[...] = jnp.zeros_like(dots)

    def red_mid(which):
        wait_bytes(ra.at[which, top(15)], ra_recv.at[which])
        wait_bytes(ra.at[which, top(15)], ra_send.at[which])
        total = ra[which, 0]
        for i in range(1, 16):
            total = total + ra[which, i]
        rb[which, ib] = total
        mine = rb.at[which, ib]
        for peer in b_peers:
            remote(mine, mine, rb_send.at[which], rb_recv.at[which], peer)

    def red_end(which):
        wait_bytes(rb.at[which, top(7)], rb_recv.at[which])
        wait_bytes(rb.at[which, top(7)], rb_send.at[which])
        total = rb[which, 0]
        for i in range(1, 8):
            total = total + rb[which, i]
        return jnp.broadcast_to(jnp.sum(total, axis=1, keepdims=True), (16, LANE))

    def record(line, m, val):
        here = lax.broadcasted_iota(jnp.int32, (1, LANE), 1) == m - 1
        ab_out[row1(line), :] = jnp.where(here, val, ab_out[row1(line), :])

    def red1_start():
        red_rows(0, [(i, i) for i in range(STEPS)] + [(STEPS + i, 8 + i) for i in range(STEPS)])

    def red1_end(m):
        total = red_end(0)
        c8 = total[:8]
        cg[...] = c8
        gram[jnp.maximum(m - 1, 0)] = total[8:]
        now = lax.broadcasted_iota(jnp.int32, c8.shape, 0) == m - 1
        record(0, m, jnp.sum(jnp.where(now, c8, 0.0), axis=0, keepdims=True))

        def piece(k):
            cur = xs[m, k]
            for i in range(STEPS):
                cur = cur - wide(cg[row1(i), :]) * vs[i, k]
            u1[k] = cur
            for i in range(STEPS):
                dots[i] = dots[i] + fold(vs[i, k] * cur)
            dots[STEPS] = dots[STEPS] + fold(cur * cur)

        loop(NCH, piece)
        red_rows(1, [(i, i) for i in range(STEPS)] + [(STEPS, 8)])

    def spare(i, slot):
        return rbuf.at[i // 2, lax.rem(i, 2), slot, :, top(LANE)]

    def export_pack(vec):
        for n in TRIO:
            for sp in BOTH:
                rows = [vec[2 * n + h, :, seg(sp, LANE)] for h in BOTH] + [jnp.zeros((32, LANE), F32)]
                tile = jnp.concatenate(rows, axis=0).T
                for s in BOTH:
                    for g in range(8):
                        to, off = divmod(8 * n + g, 3)
                        obuf[to, seg(6 * sp + 3 * s + off, 8), :] = tile[seg(8 * s + g, 8), :]

    def export_send(i):
        for d, peer in enumerate(a_peers[:7]):
            to_row = lax.rem(row + (d + 1) // 4, 2)
            to = lax.rem(to_row + yb, 2) * 4 + lax.rem(x + (d + 1) % 4, 4)
            remote(obuf.at[to], spare(i, ia8), ex_send, ex_recv.at[i], peer)
        spare(i, ia8)[...] = obuf[mem]

    def export_done():
        wait_bytes(obuf.at[top(7)], ex_send)

    def red2_end(m, last):
        total = red_end(1)
        d8 = total[:8]
        sq = total[8:9]
        for i in range(STEPS):
            di = d8[row1(i)]
            inner = jnp.sum(d8 * gram[i], axis=0, keepdims=True)
            sq = sq - 2.0 * di * di + di * (2.0 * inner - di * gram[i, row1(i), :])
        beta = jnp.sqrt(sq)
        inv = 1.0 / beta
        record(1, m, beta)
        gam[...] = cg[...] + d8
        gam[row1(STEPS), :] = inv
        if last:
            scale = inv * math.sqrt(float(4 * D * D))
            for i in range(NCH):
                wait_bytes(obuf.at[top(7)], ex_recv.at[i])

            def final(j):
                cur = spare(STEPS, j)[...]
                for i in range(STEPS):
                    cur = cur - d8[row1(i)] * spare(i, j)[...]
                v_out[j] = (cur * scale)[:, :96]

            loop(8, final)
        else:

            def piece(k):
                cur = u1[k]
                for i in range(STEPS):
                    cur = cur - wide(d8[row1(i)]) * vs[i, k]
                vs[m, k] = cur * wide(inv)

            loop(NCH, piece)

    def left_half(par, k):
        wait_bytes(gb.at[par, k, pl.ds((1 - core) * 8, 8)], fw_recv.at[par, k])
        split_blocks(par, k, 1 - core)
        h = lax.rem(k, 2)
        base = mult(3 * MROWS * h, 3 * MROWS)
        val = dot6(l3.at[:, pl.ds(base, 3 * MROWS)], v3.at[pl.ds(base, 3 * MROWS)], MROWS)
        t1[...] = jnp.where(h == 0, 0.0, t1[...]) + val

    def mix_chunk(n):
        for q in TRIO:
            xg = [t1[seg(4 * q + i, 64), :] for i in QUAD]
            for p in BOTH:
                for sp in BOTH:
                    e, o = (xg[2 * p + i][:, seg(sp, LANE)] for i in BOTH)
                    for s, val in enumerate(pair_halves(e, o)):
                        for part, piece in enumerate(reversed(split3(val))):
                            tq[seg(4 * part + 2 * sp + s, 64), seg(2 * q + p, LANE)] = piece
        out = dot6(w3, tq, WIDE)
        for pp in range(NCH):
            h, g3 = divmod(pp, 3)
            for t in QUAD:
                for rp in QUAD:
                    e, f = (out[seg(8 * t + 2 * rp + i, 8), seg(pp, LANE)] for i in BOTH)
                    g = jnp.concatenate(pair_halves(e, f), axis=0)
                    for part, val in enumerate(split3(g)):
                        t2[seg(12 * h + 3 * t + g3, 16), pl.ds(mult(part * D + n * THIRD + rp * LANE, LANE), LANE)] = val

    def right_half(k):
        n = k // 2
        rows = t2.at[pl.ds(mult((k - 2 * n) * 192, 192), 192)]
        o3[...] = dot6(rows, r3.at[:, pl.ds(mult(n * THIRD, THIRD), THIRD)], D)

    def send_out(m, k):
        @pl.when(m > 0)
        def _():
            wait_bytes(parts(k, 14), rs_send.at[k])

        for j in QUAD:
            y = [o3[seg(t, HALF), seg(j, LANE)] for t in QUAD]
            for sp in BOTH:
                for i, val in enumerate(pair_halves(y[2 * sp], y[2 * sp + 1])):
                    sz[k, j, i, :, seg(sp, LANE)] = val[:PART]
                    sy[k, i, j, :, seg(sp, LANE)] = val[PART:]
        rs_start(lax.rem(m, 2), k)

    def rg_start(c):
        up, low = rbuf.at[c, core, mem, top(HALF)], rbuf.at[c, core, mem, pl.ds(HALF, HALF)]
        for peer in x_peers:
            remote(low, low, rr_send.at[c], rr_first.at[c], peer)
        remote(up, up, rr_send.at[c], rr_first.at[c], ya_peer)
        for peer in x_peers:
            remote(up, up, rr_send.at[c], rr_last.at[c], peer)

    def rg_bytes(n):
        return rbuf.at[0, 0, top(n)]

    def rg_second(c):
        wait_bytes(rg_bytes(2), rr_first.at[c])
        low = rbuf.at[c, core, pl.ds(ya * 4, 4), pl.ds(HALF, HALF)]
        remote(low, low, rr_send.at[c], rr_last.at[c], ya_peer)
        up = rbuf.at[c, core, (1 - ya) * 4 + x, top(HALF)]
        for peer in x_peers:
            remote(up, up, rr_send.at[c], rr_last.at[c], peer)

    def rg_split(c):
        def piece(i):
            turn = i // 4
            rr = i - 4 * turn
            half = lax.rem(core + turn, 2)

            @pl.when(i == 4)
            def _():
                wait_bytes(rbuf.at[c, half], rf_recv.at[c])

            for bg in range(12):
                dst = mult((bg // 4) * THIRD + (half * 4 + rr) * 64 + (bg % 4) * 16, 16)
                eights = []
                for e in BOTH:
                    who, off = divmod(2 * bg + e, 3)
                    eights.append(rbuf[c, half, who, pl.ds(mult(rr * PART + off * 8, 8), 8), :])
                for part, val in enumerate(reversed(split3(jnp.concatenate(eights, axis=0)))):
                    r3[pl.ds(part * D + dst, 16), pl.ds(mult(c * THIRD, THIRD), THIRD)] = val

        loop(8, piece)

    def rg_forward(c):
        wait_bytes(rg_bytes(5), rr_last.at[c])
        part = rbuf.at[c, core]
        remote(part, part, rf_send.at[c], rf_recv.at[c], partner)

    for d, peer in enumerate(a_peers[:7]):
        to = lax.rem(row + (d + 1) // 4, 2) * 4 + lax.rem(x + (d + 1) % 4, 4)
        remote(obr.at[to], pbuf.at[mem], ps_send, ps_recv, peer)
    pbuf[mem] = obr[ia8]

    for p in QUAD:
        rt_copy(p).wait()
    for i in BOTH:
        for j in QUAD:
            a, b, c = (stage[i, :, seg(3 * j + e, LANE)] for e in TRIO)
            lo = low_half(a.shape)
            for e, val in enumerate((jnp.where(lo, a, b), swap(jnp.where(lo, c, a)), jnp.where(lo, b, c))):
                rbuf[e, core, mem, seg(i, HALF), seg(j, LANE)] = val
    rg_start(0)

    wait_bytes(pbuf.at[top(7)], ps_recv)
    wait_bytes(pbuf.at[top(7)], ps_send)
    for i in range(8):
        for s in QUAD:
            t1[seg(8 * s + i, PART), :96] = pbuf[i, seg(s, PART), :]
    for n in TRIO:
        for sp in BOTH:
            tile = jnp.concatenate([t1[seg(6 * sp + 3 * i + n, 64), :LANE] for i in BOTH], axis=0).T
            for h in BOTH:
                xs[0, 2 * n + h, :, seg(sp, LANE)] = tile[seg(h, HALF), :]

    def first_dots(k):
        local_dots(0, k, xs[0, k])

    def el_piece(i):
        for t in range(12):
            c, h = divmod(t // 3, 2)
            for part, val in enumerate(split3(gb[1, t // 2, i, :, seg(t % 2, LANE)])):
                l3[pl.ds(mult(i * HALF, 16), HALF), seg(3 * (6 * h + 2 * part + c) + t % 3, LANE)] = val

    for c in range(NCH):
        wait_bytes(gb.at[1, c], el_sem.at[c])

    def lead(e):
        @pl.when(e == 0)
        def _():
            for k in TRIO:
                publish(0, k, True)

        @pl.when(e == 1)
        def _():
            publish(0, 3, True)
            publish(0, 4, True)
            loop(NCH, first_dots)

        @pl.when(e == 2)
        def _():
            ag_second(0, 0)
            rg_second(0)
            ag_second(0, 1)
            publish(0, 5, True)

        @pl.when(e == 3)
        def _():
            ag_second(0, 3)
            ag_second(0, 2)
            rg_forward(0)

        loop(4, lambda i: el_piece(4 * e + i))

    loop(4, lead)
    ag_second(0, 5)
    rg_start(1)
    rg_split(0)
    ag_second(0, 4)
    ag_forward(0, 0, 0)

    def step(m):
        par = lax.rem(m, 2)
        nxt = 1 - par
        more, first, later = m < LAST, m == 0, m > 0

        def finish(k):
            combine(m, k)
            publish(m, k, False)

        def halves(k):
            @pl.when(k == 1)
            def _():
                ag_forward(par, 1, m)

                @pl.when(later)
                def _():
                    ag_second(par, 3)
                    finish(5)

                red1_start()

                @pl.when(first)
                def _():
                    rg_start(2)
                    rg_second(1)

            @pl.when(k == 2)
            def _():
                pl.when(later)(lambda: ag_second(par, 4))
                ag_forward(par, 3, m)
                red_mid(0)
                pl.when(later)(lambda: ag_second(par, 5))

            @pl.when(k == 4)
            def _():
                red1_end(m)
                ag_forward(par, 5, m)
                pl.when(first)(lambda: rg_second(2))

            left_half(par, k)

            pl.when(k == 1)(lambda: ag_forward(par, 2, m))
            pl.when(k == 3)(lambda: ag_forward(par, 4, m))
            pl.when(lax.rem(k, 2) == 1)(lambda: mix_chunk(k // 2))

        loop(NCH, halves)
        pl.when(later)(lambda: export_send(m - 1))
        red_mid(1)

        def advance(k):
            combine(m + 1, k)
            pl.when(more)(lambda: publish(m + 1, k, False))

        def spread(k):
            pl.when(more)(lambda: ag_second(nxt, k))

        def outs(k):
            pl.when(first & (k == 1))(lambda: rg_forward(1))

            @pl.when(first & (k == 2))
            def _():
                rg_split(1)
                rg_forward(2)

            pl.when(first & (k == 4))(lambda: rg_split(2))
            right_half(k)
            pl.when(k == 3)(lambda: rs_second(par, 1))

            @pl.when(k == 5)
            def _():
                advance(1)
                rs_second(par, 3)

            send_out(m, k)

            @pl.when(k == 2)
            def _():
                red2_end(m, False)
                rs_second(par, 0)

            @pl.when(k == 4)
            def _():
                rs_second(par, 2)
                advance(0)

        loop(NCH, outs)

        @pl.when(first)
        def _():
            for c in TRIO:
                wait_bytes(rg_bytes(7), rr_send.at[c])
                wait_bytes(rbuf.at[0, 0], rf_send.at[c])

        spread(0)
        rs_second(par, 4)
        advance(2)
        spread(1)
        advance(3)
        pl.when(more)(lambda: ag_forward(nxt, 0, 1))
        rs_second(par, 5)
        spread(2)
        advance(4)
        pl.when(later)(export_done)
        export_pack(vs.at[m])

    loop(STEPS, step)

    export_send(LAST)
    combine(STEPS, 5)
    red1_start()
    red_mid(0)
    red1_end(STEPS)
    export_done()
    export_pack(u1)
    export_send(STEPS)
    red_mid(1)
    red2_end(STEPS, True)
    export_done()
    for k in range(NCH):
        wait_bytes(parts(k, 14), ag_send.at[k])
        wait_bytes(parts(k, 14), rs_send.at[k])
        wait_bytes(gb.at[0, k, top(8)], fw_send.at[k])


def run_kernel(psi, wsm, el, rt):
    vmem = pl.BlockSpec(memory_space=pltpu.VMEM)
    hbm = pl.BlockSpec(memory_space=pl.ANY)
    dma = pltpu.SemaphoreType.DMA
    six, pair, three = dma((NCH,)), dma((2,)), dma((3,))
    both = dma((2, NCH))
    block = (HALF, WIDE)
    start = pltpu.VMEM((8, 96, 96), F32)
    return pl.pallas_call(
        kernel,
        out_shape=(jax.ShapeDtypeStruct((8, 96, 96), F32), jax.ShapeDtypeStruct((8, LANE), F32)),
        in_specs=[hbm, vmem, hbm, hbm],
        out_specs=(vmem, vmem),
        scratch_shapes=[
            pltpu.VMEM((MROWS, 3 * D), BF16),
            pltpu.VMEM((3 * D, D), BF16),
            pltpu.VMEM((WIDE, MROWS), BF16),
            pltpu.VMEM((2, NCH, 16, *block), F32),
            pltpu.VMEM((3 * D, WIDE), BF16),
            pltpu.VMEM((MROWS, WIDE), F32),
            pltpu.VMEM((MROWS, MROWS), BF16),
            pltpu.VMEM((384, 3 * D), BF16),
            pltpu.VMEM((192, THIRD), F32),
            pltpu.VMEM((NCH, 4, 2, PART, WIDE), F32),
            pltpu.VMEM((NCH, 2, 4, PART, WIDE), F32),
            pltpu.VMEM((2, NCH, 14, PART, WIDE), F32),
            pltpu.VMEM((STEPS + 1, NCH, *block), F32),
            pltpu.VMEM((STEPS, NCH, *block), F32),
            pltpu.VMEM((NCH, *block), F32),
            pltpu.VMEM((2, HALF, D), F32),
            pltpu.VMEM((3, 2, 8, 96, THIRD), F32),
            start,
            pltpu.VMEM((8, 96, LANE), F32),
            start,
            pltpu.VMEM((2 * STEPS, 8, LANE), F32),
            pltpu.VMEM((2, 16, 16, LANE), F32),
            pltpu.VMEM((2, 8, 16, LANE), F32),
            pltpu.VMEM((8, LANE), F32),
            pltpu.VMEM((8, LANE), F32),
            pltpu.VMEM((STEPS, 8, LANE), F32),
            both, both, six, both, both, six, both, six, pair, pair, pair, pair,
            dma((4,)), six, three, three, three, three, three, dma, dma, dma, dma, six,
        ],
        compiler_params=pltpu.CompilerParams(collective_id=0, has_side_effects=True, vmem_limit_bytes=67043328),
        name="lanczos",
    )(psi, wsm, el, rt)


def solution(mesh):
    grid = Mesh(mesh.devices.reshape(4, 2, 2, 4, 2), AXES)
    psi_spec = P("core", None, None, ("z", "yb", "ya", "x"))

    def local_fn(psi_loc, env_left, env_right, mpo_pair):
        psi = jnp.transpose(psi_loc.reshape(2, 8, HALF, 96), (1, 3, 0, 2)).reshape(8, 96, 96)
        wsm = jnp.transpose(mpo_pair.reshape(8, 8, 4, 4), (3, 1, 2, 0)).reshape(32, 32)
        vec, ab = run_kernel(psi, wsm, env_left.reshape(LANE, HALF, D), env_right)
        out = jnp.transpose(vec.reshape(8, 96, 2, HALF), (2, 0, 3, 1)).reshape(psi_loc.shape)
        return ab[0, :STEPS], ab[1, :STEPS], out

    return jax.shard_map(
        local_fn,
        mesh=grid,
        in_specs=(psi_spec, P("core", None, None), P(("z", "yb", "ya", "x"), None, None), P()),
        out_specs=(P(), P(), psi_spec),
        check_vma=False,
    )
```

```python
import functools
import math

import jax
import jax.numpy as jnp
from jax import lax
from jax.experimental import pallas as pl
from jax.experimental.pallas import tpu as pltpu
from jax.sharding import Mesh
from jax.sharding import PartitionSpec as P

STEPS = 5
AXES = ("z", "yb", "ya", "x", "core")
F32, BF16 = jnp.float32, jnp.bfloat16
MESH = pl.DeviceIdType.MESH
D = 1536
HALF = 48
NCH = 6
LANE = 128
WIDE = 256
MROWS = 768
PART = 24
THIRD = 512
LAST = STEPS - 1


def split3(val):
    hi = val.astype(BF16)
    rest = val - hi.astype(F32)
    mid = rest.astype(BF16)
    low = (rest - mid.astype(F32)).astype(BF16)
    return hi, mid, low


def swap(val):
    return pltpu.roll(val, 64, axis=val.ndim - 1)


def low_half(shape):
    return lax.broadcasted_iota(jnp.int32, shape, len(shape) - 1) < 64


def dot(a, b):
    return jnp.dot(a, b, preferred_element_type=F32)


def dot6(a, b, k):
    return dot(a[...], b[...]) + dot(a[:, : 2 * k], b[k:, :]) + dot(a[:, :k], b[2 * k :, :])


BOTH, TRIO, QUAD = range(2), range(3), range(4)


def loop(n, body):
    def run(i, carry):
        body(i)
        return carry

    lax.fori_loop(0, n, run, 0)


def top(n):
    return pl.ds(0, n)


def mult(val, n):
    return pl.multiple_of(val, n)


def seg(i, size):
    return slice(i * size, (i + 1) * size)


def row1(i):
    return slice(i, i + 1)


def wide(val):
    return jnp.concatenate([val, val], axis=1)


def pair_halves(e, o):
    lo = low_half(e.shape)
    return jnp.where(lo, e, swap(o)), jnp.where(lo, swap(e), o)


def fold(val):
    return jnp.sum(val.reshape(-1, 8, LANE), axis=0)


def kernel(
    psi_ref, wsm_ref, el_ref, rt_ref, v_out, ab_out,
    l3, r3, w3, gb, v3, t1, tq, t2, o3, sz, sy, rsb, xs, vs, u1, stage, rbuf, pbuf, obuf, obr, pin, dots, ra, rb, cg, gam, gram,
    rs_first, rs_last, rs_send, ag_first, ag_last, ag_send, fw_recv, fw_send, ra_recv, ra_send, rb_recv, rb_send,
    st_sem, el_sem, rr_first, rr_last, rr_send, rf_recv, rf_send, ps_recv, ps_send, in_sem, ex_send, ex_recv,
):
    z, yb, ya, x, core = (lax.axis_index(name) for name in AXES)
    row = lax.rem(ya + yb, 2)
    ia8 = row * 4 + x
    ia = core * 8 + ia8
    ib = z * 2 + yb
    mem = ya * 4 + x

    def a_peer(d, other=False):
        to_row = lax.rem(row + d // 4, 2)
        return {"z": z, "yb": yb, "ya": lax.rem(to_row + yb, 2), "x": lax.rem(x + d % 4, 4), "core": 1 - core if other else core}

    def b_peer(d):
        to_yb = lax.rem(yb + d // 4, 2)
        return {"z": lax.rem(z + d % 4, 4), "yb": to_yb, "ya": lax.rem(row + to_yb, 2), "x": x, "core": core}

    partner = a_peer(0, True)
    a_peers = [a_peer(d) for d in range(1, 8)] + [a_peer(d, True) for d in range(8)]
    b_peers = [b_peer(d) for d in range(1, 8)]
    x_peers, ya_peer = a_peers[:3], a_peers[3]
    z_peers, yb_peer = b_peers[:3], b_peers[3]

    def rt_copy(p):
        dst = stage.at[p // 2, pl.ds(PART * (p % 2), PART)]
        return pltpu.make_async_copy(rt_ref.at[:, core * 4 + p, :], dst, st_sem.at[p])

    psi_copy = pltpu.make_async_copy(psi_ref, pin, in_sem)
    psi_copy.start()
    for p in QUAD:
        rt_copy(p).start()
    for c in range(NCH):
        for h in BOTH:
            src = el_ref.at[pl.ds(h * 64 + ia8 * 8, 8), :, seg(c, WIDE)]
            pltpu.make_async_copy(src, gb.at[1, c, pl.ds(8 * h, 8)], el_sem.at[c]).start()

    barrier = pltpu.get_barrier_semaphore()
    for peer in a_peers + b_peers:
        pl.semaphore_signal(barrier, inc=1, device_id=peer, device_id_type=MESH)

    def init(k):
        for i in range(STEPS):
            xs[i + 1, k] = jnp.zeros((HALF, WIDE), F32)
            vs[i, k] = jnp.zeros((HALF, WIDE), F32)

    loop(NCH, init)
    for ref in (dots, gram, gam, ab_out):
        ref[...] = jnp.zeros_like(ref)

    i0 = lax.broadcasted_iota(jnp.int32, (WIDE, WIDE), 0)
    i1 = lax.broadcasted_iota(jnp.int32, (WIDE, WIDE), 1)
    same = (i0 & 7) == ((i1 >> 3) & 7)
    left = ((i0 >> 3) == i1)[:, :32].astype(BF16)
    right = (((i1 >> 6) * 8 + (i1 & 7)) == i0)[:32].astype(BF16)
    for part, val in enumerate(split3(wsm_ref[...])):
        full = dot(dot(left, val).astype(BF16), right)
        w3[:, seg(part, WIDE)] = jnp.where(same, full, 0.0).astype(BF16)

    psi_copy.wait()
    for j in range(8):
        obr[j] = jnp.concatenate([pin[:, seg(8 * h + j, HALF)] for h in BOTH], axis=1)
    pl.semaphore_wait(barrier, len(a_peers) + len(b_peers))

    def remote(src, dst, send, recv, peer):
        pltpu.make_async_remote_copy(src_ref=src, dst_ref=dst, send_sem=send, recv_sem=recv, device_id=peer, device_id_type=MESH).start()

    def wait_bytes(ref, sem):
        pltpu.make_async_copy(ref, ref, sem).wait()

    def parts(k, n):
        return rsb.at[0, k, top(n)]

    upper, lower = top(PART), pl.ds(PART, PART)

    def publish(m, k, first):
        par = lax.rem(m, 2)
        if not first:
            wait_bytes(parts(k, 14), ag_send.at[k])
        gb[par, k, ia] = xs[m, k]
        low, up = gb.at[par, k, ia, lower], gb.at[par, k, ia, upper]
        for peer in x_peers:
            remote(low, low, ag_send.at[k], ag_first.at[par, k], peer)
        remote(up, up, ag_send.at[k], ag_first.at[par, k], ya_peer)
        for peer in x_peers:
            remote(up, up, ag_send.at[k], ag_last.at[par, k], peer)

    def ag_second(par, k):
        wait_bytes(parts(k, 4), ag_first.at[par, k])
        low = gb.at[par, k, pl.ds(core * 8 + row * 4, 4), lower]
        remote(low, low, ag_send.at[k], ag_last.at[par, k], ya_peer)
        up = gb.at[par, k, core * 8 + (1 - row) * 4 + x, upper]
        for peer in x_peers:
            remote(up, up, ag_send.at[k], ag_last.at[par, k], peer)

    def ag_forward(par, k, m):
        wait_bytes(parts(k, 10), ag_last.at[par, k])

        @pl.when(m > 0)
        def _():
            wait_bytes(gb.at[0, k, top(8)], fw_send.at[k])

        part = gb.at[par, k, pl.ds(core * 8, 8)]
        remote(part, part, fw_send.at[k], fw_recv.at[par, k], partner)
        split_blocks(par, k, core)

    def split_blocks(par, k, who):
        base = 3 * MROWS * lax.rem(k, 2) + who * 384

        def piece(i):
            for part, val in enumerate(reversed(split3(gb[par, k, who * 8 + i]))):
                v3[pl.ds(mult(base + part * MROWS + i * HALF, 16), HALF), :] = val

        loop(8, piece)

    def rs_start(par, k):
        remote(sy.at[k, 1 - yb], rsb.at[par, k, pl.ds(6, 4)], rs_send.at[k], rs_first.at[par, k], yb_peer)
        for d, peer in enumerate(z_peers):
            remote(sz.at[k, lax.rem(z + d + 1, 4)], rsb.at[par, k, pl.ds(2 * d, 2)], rs_send.at[k], rs_first.at[par, k], peer)

    def rs_second(par, k):
        wait_bytes(parts(k, 10), rs_first.at[par, k])
        for j in QUAD:
            sy[k, yb, j] = sy[k, yb, j] + rsb[par, k, 6 + j]
        for d, peer in enumerate(z_peers):
            remote(sy.at[k, yb, lax.rem(z + d + 1, 4)], rsb.at[par, k, 11 + d], rs_send.at[k], rs_last.at[par, k], peer)
        for j in BOTH:
            sz[k, z, j] = sz[k, z, j] + rsb[par, k, j] + rsb[par, k, 2 + j] + rsb[par, k, 4 + j]
        remote(sz.at[k, z, 1 - yb], rsb.at[par, k, 10], rs_send.at[k], rs_last.at[par, k], yb_peer)

    def combine(m, k):
        prev = lax.rem(m + 1, 2)
        wait_bytes(parts(k, 4), rs_last.at[prev, k])
        up = sz[k, z, yb] + rsb[prev, k, 10]
        low = sy[k, yb, z] + rsb[prev, k, 11] + rsb[prev, k, 12] + rsb[prev, k, 13]
        w = jnp.concatenate([up, low], axis=0)
        for i in range(STEPS):
            w = w - wide(gam[row1(i), :]) * xs[i + 1, k]
        w = w * wide(gam[row1(STEPS), :])
        xs[m, k] = w
        local_dots(m, k, w)

    def local_dots(m, k, cur):
        new = vs[jnp.maximum(m - 1, 0), k]
        for i in range(STEPS):
            vec = vs[i, k]
            dots[i] = dots[i] + fold(vec * cur)
            dots[STEPS + i] = dots[STEPS + i] + fold(vec * new)

    def red_rows(which, pairs):
        ra[which, ia] = jnp.zeros((16, LANE), F32)
        for src, dst in pairs:
            ra[which, ia, row1(dst), :] = jnp.sum(dots[src], axis=0, keepdims=True)
        mine = ra.at[which, ia]
        for peer in a_peers:
            remote(mine, mine, ra_send.at[which], ra_recv.at[which], peer)
        dots[...] = jnp.zeros_like(dots)

    def red_mid(which):
        wait_bytes(ra.at[which, top(15)], ra_recv.at[which])
        wait_bytes(ra.at[which, top(15)], ra_send.at[which])
        total = ra[which, 0]
        for i in range(1, 16):
            total = total + ra[which, i]
        rb[which, ib] = total
        mine = rb.at[which, ib]
        for peer in b_peers:
            remote(mine, mine, rb_send.at[which], rb_recv.at[which], peer)

    def red_end(which):
        wait_bytes(rb.at[which, top(7)], rb_recv.at[which])
        wait_bytes(rb.at[which, top(7)], rb_send.at[which])
        total = rb[which, 0]
        for i in range(1, 8):
            total = total + rb[which, i]
        return jnp.broadcast_to(jnp.sum(total, axis=1, keepdims=True), (16, LANE))

    def record(line, m, val):
        here = lax.broadcasted_iota(jnp.int32, (1, LANE), 1) == m - 1
        ab_out[row1(line), :] = jnp.where(here, val, ab_out[row1(line), :])

    def red1_start():
        red_rows(0, [(i, i) for i in range(STEPS)] + [(STEPS + i, 8 + i) for i in range(STEPS)])

    def red1_end(m):
        total = red_end(0)
        c8 = total[:8]
        cg[...] = c8
        gram[jnp.maximum(m - 1, 0)] = total[8:]
        now = lax.broadcasted_iota(jnp.int32, c8.shape, 0) == m - 1
        record(0, m, jnp.sum(jnp.where(now, c8, 0.0), axis=0, keepdims=True))

        def piece(k):
            cur = xs[m, k]
            for i in range(STEPS):
                cur = cur - wide(cg[row1(i), :]) * vs[i, k]
            u1[k] = cur
            for i in range(STEPS):
                dots[i] = dots[i] + fold(vs[i, k] * cur)
            dots[STEPS] = dots[STEPS] + fold(cur * cur)

        loop(NCH, piece)
        red_rows(1, [(i, i) for i in range(STEPS)] + [(STEPS, 8)])

    def spare(i, slot):
        return rbuf.at[i // 2, lax.rem(i, 2), slot, :, top(LANE)]

    def export_pack(vec):
        for n in TRIO:
            for sp in BOTH:
                rows = [vec[2 * n + h, :, seg(sp, LANE)] for h in BOTH] + [jnp.zeros((32, LANE), F32)]
                tile = jnp.concatenate(rows, axis=0).T
                for s in BOTH:
                    for g in range(8):
                        to, off = divmod(8 * n + g, 3)
                        obuf[to, seg(6 * sp + 3 * s + off, 8), :] = tile[seg(8 * s + g, 8), :]

    def export_send(i):
        for d, peer in enumerate(a_peers[:7]):
            to_row = lax.rem(row + (d + 1) // 4, 2)
            to = lax.rem(to_row + yb, 2) * 4 + lax.rem(x + (d + 1) % 4, 4)
            remote(obuf.at[to], spare(i, ia8), ex_send, ex_recv.at[i], peer)
        spare(i, ia8)[...] = obuf[mem]

    def export_done():
        wait_bytes(obuf.at[top(7)], ex_send)

    def red2_end(m, last):
        total = red_end(1)
        d8 = total[:8]
        sq = total[8:9]
        for i in range(STEPS):
            di = d8[row1(i)]
            inner = jnp.sum(d8 * gram[i], axis=0, keepdims=True)
            sq = sq - 2.0 * di * di + di * (2.0 * inner - di * gram[i, row1(i), :])
        beta = jnp.sqrt(sq)
        inv = 1.0 / beta
        record(1, m, beta)
        gam[...] = cg[...] + d8
        gam[row1(STEPS), :] = inv
        if last:
            scale = inv * math.sqrt(float(4 * D * D))
            for i in range(NCH):
                wait_bytes(obuf.at[top(7)], ex_recv.at[i])

            def final(j):
                cur = spare(STEPS, j)[...]
                for i in range(STEPS):
                    cur = cur - d8[row1(i)] * spare(i, j)[...]
                obuf[j] = cur * scale

            export_done()
            loop(8, final)
            for h in BOTH:
                v_out[:, seg(h, 384)] = jnp.concatenate([obuf[j, :, seg(h, HALF)] for j in range(8)], axis=1)
        else:

            def piece(k):
                cur = u1[k]
                for i in range(STEPS):
                    cur = cur - wide(d8[row1(i)]) * vs[i, k]
                vs[m, k] = cur * wide(inv)

            loop(NCH, piece)

    def left_half(par, k):
        wait_bytes(gb.at[par, k, pl.ds((1 - core) * 8, 8)], fw_recv.at[par, k])
        split_blocks(par, k, 1 - core)
        h = lax.rem(k, 2)
        base = mult(3 * MROWS * h, 3 * MROWS)
        val = dot6(l3.at[:, pl.ds(base, 3 * MROWS)], v3.at[pl.ds(base, 3 * MROWS)], MROWS)
        t1[...] = jnp.where(h == 0, 0.0, t1[...]) + val

    def mix_chunk(n):
        for q in TRIO:
            xg = [t1[seg(4 * q + i, 64), :] for i in QUAD]
            for p in BOTH:
                for sp in BOTH:
                    e, o = (xg[2 * p + i][:, seg(sp, LANE)] for i in BOTH)
                    for s, val in enumerate(pair_halves(e, o)):
                        for part, piece in enumerate(reversed(split3(val))):
                            tq[seg(4 * part + 2 * sp + s, 64), seg(2 * q + p, LANE)] = piece
        out = dot6(w3, tq, WIDE)
        for pp in range(NCH):
            h, g3 = divmod(pp, 3)
            for t in QUAD:
                for rp in QUAD:
                    e, f = (out[seg(8 * t + 2 * rp + i, 8), seg(pp, LANE)] for i in BOTH)
                    g = jnp.concatenate(pair_halves(e, f), axis=0)
                    for part, val in enumerate(split3(g)):
                        t2[seg(12 * h + 3 * t + g3, 16), pl.ds(mult(part * D + n * THIRD + rp * LANE, LANE), LANE)] = val

    def right_half(k):
        n = k // 2
        rows = t2.at[pl.ds(mult((k - 2 * n) * 192, 192), 192)]
        o3[...] = dot6(rows, r3.at[:, pl.ds(mult(n * THIRD, THIRD), THIRD)], D)

    def send_out(m, k):
        @pl.when(m > 0)
        def _():
            wait_bytes(parts(k, 14), rs_send.at[k])

        for j in QUAD:
            y = [o3[seg(t, HALF), seg(j, LANE)] for t in QUAD]
            for sp in BOTH:
                for i, val in enumerate(pair_halves(y[2 * sp], y[2 * sp + 1])):
                    sz[k, j, i, :, seg(sp, LANE)] = val[:PART]
                    sy[k, i, j, :, seg(sp, LANE)] = val[PART:]
        rs_start(lax.rem(m, 2), k)

    def rg_start(c):
        up, low = rbuf.at[c, core, mem, top(HALF)], rbuf.at[c, core, mem, pl.ds(HALF, HALF)]
        for peer in x_peers:
            remote(low, low, rr_send.at[c], rr_first.at[c], peer)
        remote(up, up, rr_send.at[c], rr_first.at[c], ya_peer)
        for peer in x_peers:
            remote(up, up, rr_send.at[c], rr_last.at[c], peer)

    def rg_bytes(n):
        return rbuf.at[0, 0, top(n)]

    def rg_second(c):
        wait_bytes(rg_bytes(2), rr_first.at[c])
        low = rbuf.at[c, core, pl.ds(ya * 4, 4), pl.ds(HALF, HALF)]
        remote(low, low, rr_send.at[c], rr_last.at[c], ya_peer)
        up = rbuf.at[c, core, (1 - ya) * 4 + x, top(HALF)]
        for peer in x_peers:
            remote(up, up, rr_send.at[c], rr_last.at[c], peer)

    def rg_split(c):
        def piece(i):
            turn = i // 4
            rr = i - 4 * turn
            half = lax.rem(core + turn, 2)

            @pl.when(i == 4)
            def _():
                wait_bytes(rbuf.at[c, half], rf_recv.at[c])

            for bg in range(12):
                dst = mult((bg // 4) * THIRD + (half * 4 + rr) * 64 + (bg % 4) * 16, 16)
                eights = []
                for e in BOTH:
                    who, off = divmod(2 * bg + e, 3)
                    eights.append(rbuf[c, half, who, pl.ds(mult(rr * PART + off * 8, 8), 8), :])
                for part, val in enumerate(reversed(split3(jnp.concatenate(eights, axis=0)))):
                    r3[pl.ds(part * D + dst, 16), pl.ds(mult(c * THIRD, THIRD), THIRD)] = val

        loop(8, piece)

    def rg_forward(c):
        wait_bytes(rg_bytes(5), rr_last.at[c])
        part = rbuf.at[c, core]
        remote(part, part, rf_send.at[c], rf_recv.at[c], partner)

    for d, peer in enumerate(a_peers[:7]):
        to = lax.rem(row + (d + 1) // 4, 2) * 4 + lax.rem(x + (d + 1) % 4, 4)
        remote(obr.at[to], pbuf.at[mem], ps_send, ps_recv, peer)
    pbuf[mem] = obr[ia8]

    for p in QUAD:
        rt_copy(p).wait()
    for i in BOTH:
        for j in QUAD:
            a, b, c = (stage[i, :, seg(3 * j + e, LANE)] for e in TRIO)
            lo = low_half(a.shape)
            for e, val in enumerate((jnp.where(lo, a, b), swap(jnp.where(lo, c, a)), jnp.where(lo, b, c))):
                rbuf[e, core, mem, seg(i, HALF), seg(j, LANE)] = val
    rg_start(0)

    wait_bytes(pbuf.at[top(7)], ps_recv)
    wait_bytes(pbuf.at[top(7)], ps_send)
    for i in range(8):
        for s in QUAD:
            t1[seg(8 * s + i, PART), :96] = pbuf[i, seg(s, PART), :]
    for n in TRIO:
        for sp in BOTH:
            tile = jnp.concatenate([t1[seg(6 * sp + 3 * i + n, 64), :LANE] for i in BOTH], axis=0).T
            for h in BOTH:
                xs[0, 2 * n + h, :, seg(sp, LANE)] = tile[seg(h, HALF), :]

    def first_dots(k):
        local_dots(0, k, xs[0, k])

    def el_piece(i):
        for t in range(12):
            c, h = divmod(t // 3, 2)
            for part, val in enumerate(split3(gb[1, t // 2, i, :, seg(t % 2, LANE)])):
                l3[pl.ds(mult(i * HALF, 16), HALF), seg(3 * (6 * h + 2 * part + c) + t % 3, LANE)] = val

    for c in range(NCH):
        wait_bytes(gb.at[1, c], el_sem.at[c])

    def lead(e):
        @pl.when(e == 0)
        def _():
            for k in TRIO:
                publish(0, k, True)

        @pl.when(e == 1)
        def _():
            publish(0, 3, True)
            publish(0, 4, True)
            loop(NCH, first_dots)

        @pl.when(e == 2)
        def _():
            ag_second(0, 0)
            rg_second(0)
            ag_second(0, 1)
            publish(0, 5, True)

        @pl.when(e == 3)
        def _():
            ag_second(0, 3)
            ag_second(0, 2)
            rg_forward(0)

        loop(4, lambda i: el_piece(4 * e + i))

    loop(4, lead)
    ag_second(0, 5)
    rg_start(1)
    rg_split(0)
    ag_second(0, 4)
    ag_forward(0, 0, 0)

    def step(m):
        par = lax.rem(m, 2)
        nxt = 1 - par
        more, first, later = m < LAST, m == 0, m > 0

        def finish(k):
            combine(m, k)
            publish(m, k, False)

        def halves(k):
            @pl.when(k == 1)
            def _():
                ag_forward(par, 1, m)

                @pl.when(later)
                def _():
                    ag_second(par, 3)
                    finish(5)

                red1_start()

                @pl.when(first)
                def _():
                    rg_start(2)
                    rg_second(1)

            @pl.when(k == 2)
            def _():
                pl.when(later)(lambda: ag_second(par, 4))
                ag_forward(par, 3, m)
                red_mid(0)
                pl.when(later)(lambda: ag_second(par, 5))

            @pl.when(k == 4)
            def _():
                red1_end(m)
                ag_forward(par, 5, m)
                pl.when(first)(lambda: rg_second(2))

            left_half(par, k)

            pl.when(k == 1)(lambda: ag_forward(par, 2, m))
            pl.when(k == 3)(lambda: ag_forward(par, 4, m))
            pl.when(lax.rem(k, 2) == 1)(lambda: mix_chunk(k // 2))

        loop(NCH, halves)
        pl.when(later)(lambda: export_send(m - 1))
        red_mid(1)

        def advance(k):
            combine(m + 1, k)
            pl.when(more)(lambda: publish(m + 1, k, False))

        def spread(k):
            pl.when(more)(lambda: ag_second(nxt, k))

        def outs(k):
            pl.when(first & (k == 1))(lambda: rg_forward(1))

            @pl.when(first & (k == 2))
            def _():
                rg_split(1)
                rg_forward(2)

            pl.when(first & (k == 4))(lambda: rg_split(2))
            right_half(k)
            pl.when(k == 3)(lambda: rs_second(par, 1))

            @pl.when(k == 5)
            def _():
                advance(1)
                rs_second(par, 3)

            send_out(m, k)

            @pl.when(k == 2)
            def _():
                red2_end(m, False)
                rs_second(par, 0)

            @pl.when(k == 4)
            def _():
                rs_second(par, 2)
                advance(0)

        loop(NCH, outs)

        @pl.when(first)
        def _():
            for c in TRIO:
                wait_bytes(rg_bytes(7), rr_send.at[c])
                wait_bytes(rbuf.at[0, 0], rf_send.at[c])

        spread(0)
        rs_second(par, 4)
        advance(2)
        spread(1)
        advance(3)
        pl.when(more)(lambda: ag_forward(nxt, 0, 1))
        rs_second(par, 5)
        spread(2)
        advance(4)
        pl.when(later)(export_done)
        export_pack(vs.at[m])

    loop(STEPS, step)

    export_send(LAST)
    combine(STEPS, 5)
    red1_start()
    red_mid(0)
    red1_end(STEPS)
    export_done()
    export_pack(u1)
    export_send(STEPS)
    red_mid(1)
    red2_end(STEPS, True)
    for k in range(NCH):
        wait_bytes(parts(k, 14), ag_send.at[k])
        wait_bytes(parts(k, 14), rs_send.at[k])
        wait_bytes(gb.at[0, k, top(8)], fw_send.at[k])


def run_kernel(psi, wsm, el, rt):
    vmem = pl.BlockSpec(memory_space=pltpu.VMEM)
    hbm = pl.BlockSpec(memory_space=pl.ANY)
    dma = pltpu.SemaphoreType.DMA
    six, pair, three = dma((NCH,)), dma((2,)), dma((3,))
    both = dma((2, NCH))
    block = (HALF, WIDE)
    start = pltpu.VMEM((8, 96, 96), F32)
    return pl.pallas_call(
        kernel,
        out_shape=(jax.ShapeDtypeStruct((96, MROWS), F32), jax.ShapeDtypeStruct((8, LANE), F32)),
        in_specs=[hbm, vmem, hbm, hbm],
        out_specs=(vmem, vmem),
        scratch_shapes=[
            pltpu.VMEM((MROWS, 3 * D), BF16),
            pltpu.VMEM((3 * D, D), BF16),
            pltpu.VMEM((WIDE, MROWS), BF16),
            pltpu.VMEM((2, NCH, 16, *block), F32),
            pltpu.VMEM((3 * D, WIDE), BF16),
            pltpu.VMEM((MROWS, WIDE), F32),
            pltpu.VMEM((MROWS, MROWS), BF16),
            pltpu.VMEM((384, 3 * D), BF16),
            pltpu.VMEM((192, THIRD), F32),
            pltpu.VMEM((NCH, 4, 2, PART, WIDE), F32),
            pltpu.VMEM((NCH, 2, 4, PART, WIDE), F32),
            pltpu.VMEM((2, NCH, 14, PART, WIDE), F32),
            pltpu.VMEM((STEPS + 1, NCH, *block), F32),
            pltpu.VMEM((STEPS, NCH, *block), F32),
            pltpu.VMEM((NCH, *block), F32),
            pltpu.VMEM((2, HALF, D), F32),
            pltpu.VMEM((3, 2, 8, 96, THIRD), F32),
            start,
            pltpu.VMEM((8, 96, LANE), F32),
            start,
            pltpu.VMEM((96, MROWS), F32),
            pltpu.VMEM((2 * STEPS, 8, LANE), F32),
            pltpu.VMEM((2, 16, 16, LANE), F32),
            pltpu.VMEM((2, 8, 16, LANE), F32),
            pltpu.VMEM((8, LANE), F32),
            pltpu.VMEM((8, LANE), F32),
            pltpu.VMEM((STEPS, 8, LANE), F32),
            both, both, six, both, both, six, both, six, pair, pair, pair, pair,
            dma((4,)), six, three, three, three, three, three, dma, dma, dma, dma, six,
        ],
        compiler_params=pltpu.CompilerParams(collective_id=0, has_side_effects=True, vmem_limit_bytes=67043328),
        name="lanczos",
    )(psi, wsm, el, rt)


def solution(mesh):
    grid = Mesh(mesh.devices.reshape(4, 2, 2, 4, 2), AXES)
    psi_spec = P("core", None, None, ("z", "yb", "ya", "x"))

    def local_fn(psi_loc, env_left, env_right, mpo_pair):
        psi = jnp.transpose(psi_loc, (1, 2, 3, 0)).reshape(96, MROWS)
        wsm = jnp.transpose(mpo_pair.reshape(8, 8, 4, 4), (3, 1, 2, 0)).reshape(32, 32)
        vec, ab = run_kernel(psi, wsm, env_left.reshape(LANE, HALF, D), env_right)
        out = jnp.transpose(vec.reshape(2, 2, PART, MROWS), (3, 0, 1, 2))
        return ab[0, :STEPS], ab[1, :STEPS], out

    return jax.shard_map(
        local_fn,
        mesh=grid,
        in_specs=(psi_spec, P("core", None, None), P(("z", "yb", "ya", "x"), None, None), P()),
        out_specs=(P(), P(), psi_spec),
        check_vma=False,
    )
```

```python
import functools
import math

import jax
import jax.numpy as jnp
from jax import lax
from jax.experimental import pallas as pl
from jax.experimental.pallas import tpu as pltpu
from jax.sharding import Mesh
from jax.sharding import PartitionSpec as P

STEPS = 5
AXES = ("z", "yb", "ya", "x", "core")
F32, BF16 = jnp.float32, jnp.bfloat16
MESH = pl.DeviceIdType.MESH
D = 1536
HALF = 48
NCH = 6
LANE = 128
WIDE = 256
MROWS = 768
PART = 24
THIRD = 512
LAST = STEPS - 1


def split3(val):
    hi = val.astype(BF16)
    rest = val - hi.astype(F32)
    mid = rest.astype(BF16)
    low = (rest - mid.astype(F32)).astype(BF16)
    return hi, mid, low


def swap(val):
    return pltpu.roll(val, 64, axis=val.ndim - 1)


def low_half(shape):
    return lax.broadcasted_iota(jnp.int32, shape, len(shape) - 1) < 64


def dot(a, b):
    return jnp.dot(a, b, preferred_element_type=F32)


def dot6(a, b, k):
    return dot(a[...], b[...]) + dot(a[:, : 2 * k], b[k:, :]) + dot(a[:, :k], b[2 * k :, :])


BOTH, TRIO, QUAD = range(2), range(3), range(4)


def loop(n, body):
    def run(i, carry):
        body(i)
        return carry

    lax.fori_loop(0, n, run, 0)


def top(n):
    return pl.ds(0, n)


def mult(val, n):
    return pl.multiple_of(val, n)


def seg(i, size):
    return slice(i * size, (i + 1) * size)


def row1(i):
    return slice(i, i + 1)


def wide(val):
    return jnp.concatenate([val, val], axis=1)


def pair_halves(e, o):
    lo = low_half(e.shape)
    return jnp.where(lo, e, swap(o)), jnp.where(lo, swap(e), o)


def fold(val):
    return jnp.sum(val.reshape(-1, 8, LANE), axis=0)


def kernel(
    psi_ref, wsm_ref, el_ref, rt_ref, v_out, ab_out,
    l3, r3, w3, gb, v3, t1, tq, t2, o3, sz, sy, rsb, xs, vs, u1, stage, rbuf, pbuf, obuf, obr, pin, dots, ra, rb, cg, gam, gram,
    rs_first, rs_last, rs_send, ag_first, ag_last, ag_send, fw_recv, fw_send, ra_recv, ra_send, rb_recv, rb_send,
    st_sem, el_sem, rr_deep, rr_high, rr_low, rr_up, rr_send, rf_recv, rf_send, ps_recv, ps_send, in_sem, ex_send, ex_recv,
):
    z, yb, ya, x, core = (lax.axis_index(name) for name in AXES)
    row = lax.rem(ya + yb, 2)
    ia8 = row * 4 + x
    ia = core * 8 + ia8
    ib = z * 2 + yb
    mem = ya * 4 + x

    def a_peer(d, other=False):
        to_row = lax.rem(row + d // 4, 2)
        return {"z": z, "yb": yb, "ya": lax.rem(to_row + yb, 2), "x": lax.rem(x + d % 4, 4), "core": 1 - core if other else core}

    def b_peer(d):
        to_yb = lax.rem(yb + d // 4, 2)
        return {"z": lax.rem(z + d % 4, 4), "yb": to_yb, "ya": lax.rem(row + to_yb, 2), "x": x, "core": core}

    partner = a_peer(0, True)
    a_peers = [a_peer(d) for d in range(1, 8)] + [a_peer(d, True) for d in range(8)]
    b_peers = [b_peer(d) for d in range(1, 8)]
    x_peers, ya_peer = [a_peers[1], a_peers[0], a_peers[2]], a_peers[3]
    z_peers, yb_peer = b_peers[:3], b_peers[3]

    def rt_copy(p):
        dst = stage.at[p // 2, pl.ds(PART * (p % 2), PART)]
        return pltpu.make_async_copy(rt_ref.at[:, core * 4 + p, :], dst, st_sem.at[p])

    psi_copy = pltpu.make_async_copy(psi_ref, pin, in_sem)
    psi_copy.start()
    for p in QUAD:
        rt_copy(p).start()
    for c in range(NCH):
        for h in BOTH:
            src = el_ref.at[pl.ds(h * 64 + ia8 * 8, 8), :, seg(c, WIDE)]
            pltpu.make_async_copy(src, gb.at[1, c, pl.ds(8 * h, 8)], el_sem.at[c]).start()

    barrier = pltpu.get_barrier_semaphore()
    for peer in a_peers + b_peers:
        pl.semaphore_signal(barrier, inc=1, device_id=peer, device_id_type=MESH)

    def init(k):
        for i in range(STEPS):
            xs[i + 1, k] = jnp.zeros((HALF, WIDE), F32)
            vs[i, k] = jnp.zeros((HALF, WIDE), F32)

    loop(NCH, init)
    for ref in (dots, gram, gam, ab_out):
        ref[...] = jnp.zeros_like(ref)

    i0 = lax.broadcasted_iota(jnp.int32, (WIDE, WIDE), 0)
    i1 = lax.broadcasted_iota(jnp.int32, (WIDE, WIDE), 1)
    same = (i0 & 7) == ((i1 >> 3) & 7)
    left = ((i0 >> 3) == i1)[:, :32].astype(BF16)
    right = (((i1 >> 6) * 8 + (i1 & 7)) == i0)[:32].astype(BF16)
    for part, val in enumerate(split3(wsm_ref[...])):
        full = dot(dot(left, val).astype(BF16), right)
        w3[:, seg(part, WIDE)] = jnp.where(same, full, 0.0).astype(BF16)

    psi_copy.wait()
    for j in range(8):
        obr[j] = jnp.concatenate([pin[:, seg(8 * h + j, HALF)] for h in BOTH], axis=1)
    pl.semaphore_wait(barrier, len(a_peers) + len(b_peers))

    def remote(src, dst, send, recv, peer):
        pltpu.make_async_remote_copy(src_ref=src, dst_ref=dst, send_sem=send, recv_sem=recv, device_id=peer, device_id_type=MESH).start()

    def wait_bytes(ref, sem):
        pltpu.make_async_copy(ref, ref, sem).wait()

    def parts(k, n):
        return rsb.at[0, k, top(n)]

    upper, lower = top(PART), pl.ds(PART, PART)

    def publish(m, k, first):
        par = lax.rem(m, 2)
        if not first:
            wait_bytes(parts(k, 14), ag_send.at[k])
        gb[par, k, ia] = xs[m, k]
        low, up = gb.at[par, k, ia, lower], gb.at[par, k, ia, upper]
        for peer in x_peers:
            remote(low, low, ag_send.at[k], ag_first.at[par, k], peer)
        remote(up, up, ag_send.at[k], ag_first.at[par, k], ya_peer)
        for peer in x_peers:
            remote(up, up, ag_send.at[k], ag_last.at[par, k], peer)

    def ag_second(par, k):
        wait_bytes(parts(k, 4), ag_first.at[par, k])
        low = gb.at[par, k, pl.ds(core * 8 + row * 4, 4), lower]
        remote(low, low, ag_send.at[k], ag_last.at[par, k], ya_peer)
        up = gb.at[par, k, core * 8 + (1 - row) * 4 + x, upper]
        for peer in x_peers:
            remote(up, up, ag_send.at[k], ag_last.at[par, k], peer)

    def ag_forward(par, k, m):
        wait_bytes(parts(k, 10), ag_last.at[par, k])

        @pl.when(m > 0)
        def _():
            wait_bytes(gb.at[0, k, top(8)], fw_send.at[k])

        part = gb.at[par, k, pl.ds(core * 8, 8)]
        remote(part, part, fw_send.at[k], fw_recv.at[par, k], partner)
        split_blocks(par, k, core)

    def split_blocks(par, k, who):
        base = 3 * MROWS * lax.rem(k, 2) + who * 384

        def piece(i):
            for part, val in enumerate(reversed(split3(gb[par, k, who * 8 + i]))):
                v3[pl.ds(mult(base + part * MROWS + i * HALF, 16), HALF), :] = val

        loop(8, piece)

    def rs_start(par, k):
        remote(sy.at[k, 1 - yb], rsb.at[par, k, pl.ds(6, 4)], rs_send.at[k], rs_first.at[par, k], yb_peer)
        for d, peer in enumerate(z_peers):
            remote(sz.at[k, lax.rem(z + d + 1, 4)], rsb.at[par, k, pl.ds(2 * d, 2)], rs_send.at[k], rs_first.at[par, k], peer)

    def rs_second(par, k):
        wait_bytes(parts(k, 10), rs_first.at[par, k])
        for j in QUAD:
            sy[k, yb, j] = sy[k, yb, j] + rsb[par, k, 6 + j]
        for d, peer in enumerate(z_peers):
            remote(sy.at[k, yb, lax.rem(z + d + 1, 4)], rsb.at[par, k, 11 + d], rs_send.at[k], rs_last.at[par, k], peer)
        for j in BOTH:
            sz[k, z, j] = sz[k, z, j] + rsb[par, k, j] + rsb[par, k, 2 + j] + rsb[par, k, 4 + j]
        remote(sz.at[k, z, 1 - yb], rsb.at[par, k, 10], rs_send.at[k], rs_last.at[par, k], yb_peer)

    def combine(m, k):
        prev = lax.rem(m + 1, 2)
        wait_bytes(parts(k, 4), rs_last.at[prev, k])
        up = sz[k, z, yb] + rsb[prev, k, 10]
        low = sy[k, yb, z] + rsb[prev, k, 11] + rsb[prev, k, 12] + rsb[prev, k, 13]
        w = jnp.concatenate([up, low], axis=0)
        for i in range(STEPS):
            w = w - wide(gam[row1(i), :]) * xs[i + 1, k]
        w = w * wide(gam[row1(STEPS), :])
        xs[m, k] = w
        local_dots(m, k, w)

    def local_dots(m, k, cur):
        new = vs[jnp.maximum(m - 1, 0), k]
        for i in range(STEPS):
            vec = vs[i, k]
            dots[i] = dots[i] + fold(vec * cur)
            dots[STEPS + i] = dots[STEPS + i] + fold(vec * new)

    def red_rows(which, pairs):
        ra[which, ia] = jnp.zeros((16, LANE), F32)
        for src, dst in pairs:
            ra[which, ia, row1(dst), :] = jnp.sum(dots[src], axis=0, keepdims=True)
        mine = ra.at[which, ia]
        for peer in a_peers:
            remote(mine, mine, ra_send.at[which], ra_recv.at[which], peer)
        dots[...] = jnp.zeros_like(dots)

    def red_mid(which):
        wait_bytes(ra.at[which, top(15)], ra_recv.at[which])
        wait_bytes(ra.at[which, top(15)], ra_send.at[which])
        total = ra[which, 0]
        for i in range(1, 16):
            total = total + ra[which, i]
        rb[which, ib] = total
        mine = rb.at[which, ib]
        for peer in b_peers:
            remote(mine, mine, rb_send.at[which], rb_recv.at[which], peer)

    def red_end(which):
        wait_bytes(rb.at[which, top(7)], rb_recv.at[which])
        wait_bytes(rb.at[which, top(7)], rb_send.at[which])
        total = rb[which, 0]
        for i in range(1, 8):
            total = total + rb[which, i]
        return jnp.broadcast_to(jnp.sum(total, axis=1, keepdims=True), (16, LANE))

    def record(line, m, val):
        here = lax.broadcasted_iota(jnp.int32, (1, LANE), 1) == m - 1
        ab_out[row1(line), :] = jnp.where(here, val, ab_out[row1(line), :])

    def red1_start():
        red_rows(0, [(i, i) for i in range(STEPS)] + [(STEPS + i, 8 + i) for i in range(STEPS)])

    def red1_end(m):
        total = red_end(0)
        c8 = total[:8]
        cg[...] = c8
        gram[jnp.maximum(m - 1, 0)] = total[8:]
        now = lax.broadcasted_iota(jnp.int32, c8.shape, 0) == m - 1
        record(0, m, jnp.sum(jnp.where(now, c8, 0.0), axis=0, keepdims=True))

        def piece(k):
            cur = xs[m, k]
            for i in range(STEPS):
                cur = cur - wide(cg[row1(i), :]) * vs[i, k]
            u1[k] = cur
            for i in range(STEPS):
                dots[i] = dots[i] + fold(vs[i, k] * cur)
            dots[STEPS] = dots[STEPS] + fold(cur * cur)

        loop(NCH, piece)
        red_rows(1, [(i, i) for i in range(STEPS)] + [(STEPS, 8)])

    def spare(i, slot):
        return rbuf.at[i // 2, lax.rem(i, 2), slot, :, top(LANE)]

    def export_pack(vec, n):
        for sp in BOTH:
            rows = [vec[2 * n + h, :, seg(sp, LANE)] for h in BOTH] + [jnp.zeros((32, LANE), F32)]
            tile = jnp.concatenate(rows, axis=0).T
            for s in BOTH:
                for g in range(8):
                    to, off = divmod(8 * n + g, 3)
                    obuf[to, seg(6 * sp + 3 * s + off, 8), :] = tile[seg(8 * s + g, 8), :]

    def export_send(i):
        for d, peer in enumerate(a_peers[:7]):
            to_row = lax.rem(row + (d + 1) // 4, 2)
            to = lax.rem(to_row + yb, 2) * 4 + lax.rem(x + (d + 1) % 4, 4)
            remote(obuf.at[to], spare(i, ia8), ex_send, ex_recv.at[i], peer)
        spare(i, ia8)[...] = obuf[mem]

    def export_done():
        wait_bytes(obuf.at[top(7)], ex_send)

    def red2_end(m, last):
        total = red_end(1)
        d8 = total[:8]
        sq = total[8:9]
        for i in range(STEPS):
            di = d8[row1(i)]
            inner = jnp.sum(d8 * gram[i], axis=0, keepdims=True)
            sq = sq - 2.0 * di * di + di * (2.0 * inner - di * gram[i, row1(i), :])
        beta = jnp.sqrt(sq)
        inv = 1.0 / beta
        record(1, m, beta)
        gam[...] = cg[...] + d8
        gam[row1(STEPS), :] = inv
        if last:
            scale = inv * math.sqrt(float(4 * D * D))
            for i in range(NCH):
                wait_bytes(obuf.at[top(7)], ex_recv.at[i])

            def final(j):
                cur = spare(STEPS, j)[...]
                for i in range(STEPS):
                    cur = cur - d8[row1(i)] * spare(i, j)[...]
                obuf[j] = cur * scale

            export_done()
            loop(8, final)
            for h in BOTH:
                v_out[:, seg(h, 384)] = jnp.concatenate([obuf[j, :, seg(h, HALF)] for j in range(8)], axis=1)
        else:

            def piece(k):
                cur = u1[k]
                for i in range(STEPS):
                    cur = cur - wide(d8[row1(i)]) * vs[i, k]
                vs[m, k] = cur * wide(inv)

            loop(NCH, piece)

    def left_half(par, k):
        wait_bytes(gb.at[par, k, pl.ds((1 - core) * 8, 8)], fw_recv.at[par, k])
        split_blocks(par, k, 1 - core)
        h = lax.rem(k, 2)
        base = mult(3 * MROWS * h, 3 * MROWS)
        val = dot6(l3.at[:, pl.ds(base, 3 * MROWS)], v3.at[pl.ds(base, 3 * MROWS)], MROWS)
        t1[...] = jnp.where(h == 0, 0.0, t1[...]) + val

    def mix_chunk(n):
        for q in TRIO:
            xg = [t1[seg(4 * q + i, 64), :] for i in QUAD]
            for p in BOTH:
                for sp in BOTH:
                    e, o = (xg[2 * p + i][:, seg(sp, LANE)] for i in BOTH)
                    for s, val in enumerate(pair_halves(e, o)):
                        for part, piece in enumerate(reversed(split3(val))):
                            tq[seg(4 * part + 2 * sp + s, 64), seg(2 * q + p, LANE)] = piece
        out = dot6(w3, tq, WIDE)
        for pp in range(NCH):
            h, g3 = divmod(pp, 3)
            for t in QUAD:
                for rp in QUAD:
                    e, f = (out[seg(8 * t + 2 * rp + i, 8), seg(pp, LANE)] for i in BOTH)
                    g = jnp.concatenate(pair_halves(e, f), axis=0)
                    for part, val in enumerate(split3(g)):
                        t2[seg(12 * h + 3 * t + g3, 16), pl.ds(mult(part * D + n * THIRD + rp * LANE, LANE), LANE)] = val

    def right_half(k):
        n = k // 2
        rows = t2.at[pl.ds(mult((k - 2 * n) * 192, 192), 192)]
        o3[...] = dot6(rows, r3.at[:, pl.ds(mult(n * THIRD, THIRD), THIRD)], D)

    def send_out(m, k):
        @pl.when(m > 0)
        def _():
            wait_bytes(parts(k, 14), rs_send.at[k])

        for j in QUAD:
            y = [o3[seg(t, HALF), seg(j, LANE)] for t in QUAD]
            for sp in BOTH:
                for i, val in enumerate(pair_halves(y[2 * sp], y[2 * sp + 1])):
                    sz[k, j, i, :, seg(sp, LANE)] = val[:PART]
                    sy[k, i, j, :, seg(sp, LANE)] = val[PART:]
        rs_start(lax.rem(m, 2), k)

    high, deep = top(40), pl.ds(40, 56)

    def rg_send(c, who, rows, recv, peers):
        part = rbuf.at[c, core, who, rows]
        for peer in peers:
            remote(part, part, rr_send.at[c], recv.at[c], peer)

    def rg_wait(n, rows, sem):
        wait_bytes(rbuf.at[0, 0, top(n), top(rows)], sem)

    def rg_start(c):
        rg_send(c, mem, deep, rr_deep, x_peers)
        rg_send(c, mem, high, rr_high, [ya_peer])
        rg_send(c, mem, high, rr_up, x_peers)

    def rg_bytes(n):
        return rbuf.at[0, 0, top(n)]

    def rg_second(c):
        rg_wait(7, PART, rr_deep.at[c])
        rg_wait(1, 40, rr_high.at[c])
        rg_send(c, pl.ds(ya * 4, 4), deep, rr_low, [ya_peer])
        rg_send(c, (1 - ya) * 4 + x, high, rr_up, x_peers)

    def rg_split(c):
        def piece(i):
            turn = i // 4
            rr = i - 4 * turn
            half = lax.rem(core + turn, 2)

            @pl.when(i == 4)
            def _():
                wait_bytes(rbuf.at[c, half], rf_recv.at[c])

            for bg in range(12):
                dst = mult((bg // 4) * THIRD + (half * 4 + rr) * 64 + (bg % 4) * 16, 16)
                eights = []
                for e in BOTH:
                    who, off = divmod(2 * bg + e, 3)
                    eights.append(rbuf[c, half, who, pl.ds(mult(rr * PART + off * 8, 8), 8), :])
                for part, val in enumerate(reversed(split3(jnp.concatenate(eights, axis=0)))):
                    r3[pl.ds(part * D + dst, 16), pl.ds(mult(c * THIRD, THIRD), THIRD)] = val

        loop(8, piece)

    def rg_forward(c):
        rg_wait(7, 32, rr_low.at[c])
        rg_wait(5, HALF, rr_up.at[c])
        part = rbuf.at[c, core]
        remote(part, part, rf_send.at[c], rf_recv.at[c], partner)

    for d, peer in enumerate(a_peers[:7]):
        to = lax.rem(row + (d + 1) // 4, 2) * 4 + lax.rem(x + (d + 1) % 4, 4)
        remote(obr.at[to], pbuf.at[mem], ps_send, ps_recv, peer)
    pbuf[mem] = obr[ia8]

    for p in QUAD:
        rt_copy(p).wait()
    for i in BOTH:
        for j in QUAD:
            a, b, c = (stage[i, :, seg(3 * j + e, LANE)] for e in TRIO)
            lo = low_half(a.shape)
            for e, val in enumerate((jnp.where(lo, a, b), swap(jnp.where(lo, c, a)), jnp.where(lo, b, c))):
                rbuf[e, core, mem, seg(i, HALF), seg(j, LANE)] = val
    rg_start(0)

    wait_bytes(pbuf.at[top(7)], ps_recv)
    wait_bytes(pbuf.at[top(7)], ps_send)
    for i in range(8):
        for s in QUAD:
            t1[seg(8 * s + i, PART), :96] = pbuf[i, seg(s, PART), :]
    for n in TRIO:
        for sp in BOTH:
            tile = jnp.concatenate([t1[seg(6 * sp + 3 * i + n, 64), :LANE] for i in BOTH], axis=0).T
            for h in BOTH:
                xs[0, 2 * n + h, :, seg(sp, LANE)] = tile[seg(h, HALF), :]

    def first_dots(k):
        local_dots(0, k, xs[0, k])

    def el_piece(i):
        for t in range(12):
            c, h = divmod(t // 3, 2)
            for part, val in enumerate(split3(gb[1, t // 2, i, :, seg(t % 2, LANE)])):
                l3[pl.ds(mult(i * HALF, 16), HALF), seg(3 * (6 * h + 2 * part + c) + t % 3, LANE)] = val

    for c in range(NCH):
        wait_bytes(gb.at[1, c], el_sem.at[c])

    def lead(e):
        @pl.when(e == 0)
        def _():
            for k in TRIO:
                publish(0, k, True)

        @pl.when(e == 1)
        def _():
            publish(0, 3, True)
            publish(0, 4, True)
            loop(NCH, first_dots)

        @pl.when(e == 2)
        def _():
            ag_second(0, 0)
            rg_second(0)
            ag_second(0, 1)
            publish(0, 5, True)

        @pl.when(e == 3)
        def _():
            ag_second(0, 3)
            ag_second(0, 2)
            rg_forward(0)

        loop(4, lambda i: el_piece(4 * e + i))

    loop(4, lead)
    ag_second(0, 5)
    rg_start(1)
    rg_split(0)
    ag_second(0, 4)
    ag_forward(0, 0, 0)

    def step(m):
        par = lax.rem(m, 2)
        nxt = 1 - par
        more, first, later = m < LAST, m == 0, m > 0

        def finish(k):
            combine(m, k)
            publish(m, k, False)

        def halves(k):
            @pl.when(k == 1)
            def _():
                ag_forward(par, 1, m)

                @pl.when(later)
                def _():
                    ag_second(par, 3)
                    finish(5)

                red1_start()

                @pl.when(first)
                def _():
                    rg_start(2)
                    rg_second(1)

            @pl.when(k == 2)
            def _():
                pl.when(later)(lambda: ag_second(par, 4))
                ag_forward(par, 3, m)
                red_mid(0)
                pl.when(later)(lambda: ag_second(par, 5))

            @pl.when(k == 4)
            def _():
                red1_end(m)
                ag_forward(par, 5, m)
                pl.when(first)(lambda: rg_second(2))

            left_half(par, k)

            pl.when(k == 1)(lambda: ag_forward(par, 2, m))
            pl.when(k == 3)(lambda: ag_forward(par, 4, m))
            pl.when(lax.rem(k, 2) == 1)(lambda: mix_chunk(k // 2))

        loop(NCH, halves)
        pl.when(later)(lambda: export_send(m - 1))
        red_mid(1)

        def advance(k):
            combine(m + 1, k)
            pl.when(more)(lambda: publish(m + 1, k, False))

        def spread(k):
            pl.when(more)(lambda: ag_second(nxt, k))

        def outs(k):
            pl.when(first & (k == 1))(lambda: rg_forward(1))

            @pl.when(first & (k == 2))
            def _():
                rg_split(1)
                rg_forward(2)

            pl.when(first & (k == 4))(lambda: rg_split(2))
            right_half(k)
            pl.when(k == 3)(lambda: rs_second(par, 1))

            @pl.when(k == 5)
            def _():
                advance(1)
                rs_second(par, 3)

            send_out(m, k)

            @pl.when(k == 2)
            def _():
                red2_end(m, False)
                rs_second(par, 0)

            @pl.when(k == 4)
            def _():
                rs_second(par, 2)
                advance(0)

        loop(NCH, outs)

        @pl.when(first)
        def _():
            for c in TRIO:
                wait_bytes(rg_bytes(7), rr_send.at[c])
                wait_bytes(rbuf.at[0, 0], rf_send.at[c])

        spread(0)
        pl.when(later)(export_done)
        rs_second(par, 4)
        export_pack(vs.at[m], 0)
        export_pack(vs.at[m], 1)
        advance(2)
        spread(1)
        export_pack(vs.at[m], 2)
        advance(3)
        pl.when(more)(lambda: ag_forward(nxt, 0, 1))
        rs_second(par, 5)
        spread(2)
        advance(4)

    loop(STEPS, step)

    export_send(LAST)
    combine(STEPS, 5)
    red1_start()
    red_mid(0)
    red1_end(STEPS)
    export_done()
    for n in TRIO:
        export_pack(u1, n)
    export_send(STEPS)
    red_mid(1)
    red2_end(STEPS, True)
    for k in range(NCH):
        wait_bytes(parts(k, 14), ag_send.at[k])
        wait_bytes(parts(k, 14), rs_send.at[k])
        wait_bytes(gb.at[0, k, top(8)], fw_send.at[k])


def run_kernel(psi, wsm, el, rt):
    vmem = pl.BlockSpec(memory_space=pltpu.VMEM)
    hbm = pl.BlockSpec(memory_space=pl.ANY)
    dma = pltpu.SemaphoreType.DMA
    six, pair, three = dma((NCH,)), dma((2,)), dma((3,))
    both = dma((2, NCH))
    block = (HALF, WIDE)
    start = pltpu.VMEM((8, 96, 96), F32)
    return pl.pallas_call(
        kernel,
        out_shape=(jax.ShapeDtypeStruct((96, MROWS), F32), jax.ShapeDtypeStruct((8, LANE), F32)),
        in_specs=[hbm, vmem, hbm, hbm],
        out_specs=(vmem, vmem),
        scratch_shapes=[
            pltpu.VMEM((MROWS, 3 * D), BF16),
            pltpu.VMEM((3 * D, D), BF16),
            pltpu.VMEM((WIDE, MROWS), BF16),
            pltpu.VMEM((2, NCH, 16, *block), F32),
            pltpu.VMEM((3 * D, WIDE), BF16),
            pltpu.VMEM((MROWS, WIDE), F32),
            pltpu.VMEM((MROWS, MROWS), BF16),
            pltpu.VMEM((384, 3 * D), BF16),
            pltpu.VMEM((192, THIRD), F32),
            pltpu.VMEM((NCH, 4, 2, PART, WIDE), F32),
            pltpu.VMEM((NCH, 2, 4, PART, WIDE), F32),
            pltpu.VMEM((2, NCH, 14, PART, WIDE), F32),
            pltpu.VMEM((STEPS + 1, NCH, *block), F32),
            pltpu.VMEM((STEPS, NCH, *block), F32),
            pltpu.VMEM((NCH, *block), F32),
            pltpu.VMEM((2, HALF, D), F32),
            pltpu.VMEM((3, 2, 8, 96, THIRD), F32),
            start,
            pltpu.VMEM((8, 96, LANE), F32),
            start,
            pltpu.VMEM((96, MROWS), F32),
            pltpu.VMEM((2 * STEPS, 8, LANE), F32),
            pltpu.VMEM((2, 16, 16, LANE), F32),
            pltpu.VMEM((2, 8, 16, LANE), F32),
            pltpu.VMEM((8, LANE), F32),
            pltpu.VMEM((8, LANE), F32),
            pltpu.VMEM((STEPS, 8, LANE), F32),
            both, both, six, both, both, six, both, six, pair, pair, pair, pair,
            dma((4,)), six, three, three, three, three, three, three, three, dma, dma, dma, dma, six,
        ],
        compiler_params=pltpu.CompilerParams(collective_id=0, has_side_effects=True, vmem_limit_bytes=67043328),
        name="lanczos",
    )(psi, wsm, el, rt)


def solution(mesh):
    grid = Mesh(mesh.devices.reshape(4, 2, 2, 4, 2), AXES)
    psi_spec = P("core", None, None, ("z", "yb", "ya", "x"))

    def local_fn(psi_loc, env_left, env_right, mpo_pair):
        psi = jnp.transpose(psi_loc, (1, 2, 3, 0)).reshape(96, MROWS)
        wsm = jnp.transpose(mpo_pair.reshape(8, 8, 4, 4), (3, 1, 2, 0)).reshape(32, 32)
        vec, ab = run_kernel(psi, wsm, env_left.reshape(LANE, HALF, D), env_right)
        out = jnp.transpose(vec.reshape(2, 2, PART, MROWS), (3, 0, 1, 2))
        return ab[0, :STEPS], ab[1, :STEPS], out

    return jax.shard_map(
        local_fn,
        mesh=grid,
        in_specs=(psi_spec, P("core", None, None), P(("z", "yb", "ya", "x"), None, None), P()),
        out_specs=(P(), P(), psi_spec),
        check_vma=False,
    )
```

```python
import functools
import math

import jax
import jax.numpy as jnp
from jax import lax
from jax.experimental import pallas as pl
from jax.experimental.pallas import tpu as pltpu
from jax.sharding import Mesh
from jax.sharding import PartitionSpec as P

STEPS = 5
AXES = ("z", "yb", "ya", "x", "core")
F32, BF16 = jnp.float32, jnp.bfloat16
ROWSUM = dict(axis=0, keepdims=True)
MESH = pl.DeviceIdType.MESH
D = 1536
HALF = 48
NCH = 6
LANE = 128
WIDE = 256
MROWS = 768
PART = 24
THIRD = 512
LAST = STEPS - 1


def split3(val):
    hi = val.astype(BF16)
    rest = val - hi.astype(F32)
    mid = rest.astype(BF16)
    low = (rest - mid.astype(F32)).astype(BF16)
    return hi, mid, low


def swap(val):
    return pltpu.roll(val, 64, axis=val.ndim - 1)


def low_half(shape):
    return lax.broadcasted_iota(jnp.int32, shape, len(shape) - 1) < 64


def dot(a, b):
    return jnp.dot(a, b, preferred_element_type=F32)


def dot6(a, b, k):
    return dot(a[...], b[...]) + dot(a[:, : 2 * k], b[k:, :]) + dot(a[:, :k], b[2 * k :, :])


BOTH, TRIO, QUAD, EIGHT, SEVEN = range(2), range(3), range(4), range(8), range(1, 8)


def loop(n, body):
    def run(i, carry):
        body(i)
        return carry

    lax.fori_loop(0, n, run, 0)


def top(n):
    return pl.ds(0, n)


def mult(val, n):
    return pl.multiple_of(val, n)


def seg(i, size):
    return slice(i * size, (i + 1) * size)


def row1(i):
    return slice(i, i + 1)


def wide(val):
    return jnp.concatenate([val, val], axis=1)


def pair_halves(e, o):
    lo = low_half(e.shape)
    return jnp.where(lo, e, swap(o)), jnp.where(lo, swap(e), o)


def fold(val):
    return jnp.sum(val.reshape(-1, 8, LANE), axis=0)


def kernel(
    psi_ref, wsm_ref, el_ref, rt_ref, v_out, ab_out,
    l3, r3, w3, gb, v3, t1, tq, t2, o3, sz, sy, rsb, xs, vs, u1, stage, rbuf, pbuf, obuf, obr, pin, dots, ra, rb, cg, gam, gram,
    rs_first, rs_last, rs_send, ag_first, ag_last, ag_send, fw_recv, fw_send, ra_recv, ra_send, rb_recv, rb_send,
    st_sem, el_sem, rr_deep, rr_high, rr_low, rr_up, rr_send, rf_recv, rf_send, ps_recv, ps_send, in_sem, ex_send, ex_recv,
):
    z, yb, ya, x, core = (lax.axis_index(name) for name in AXES)
    row = lax.rem(ya + yb, 2)
    ia8 = row * 4 + x
    ia = core * 8 + ia8
    ib = z * 2 + yb
    mem = ya * 4 + x

    def a_peer(d, other=False):
        to_row = lax.rem(row + d // 4, 2)
        return {"z": z, "yb": yb, "ya": lax.rem(to_row + yb, 2), "x": lax.rem(x + d % 4, 4), "core": 1 - core if other else core}

    def b_peer(d):
        to_yb = lax.rem(yb + d // 4, 2)
        return {"z": lax.rem(z + d % 4, 4), "yb": to_yb, "ya": lax.rem(row + to_yb, 2), "x": x, "core": core}

    partner = a_peer(0, True)
    a_peers = [a_peer(d) for d in SEVEN] + [a_peer(d, True) for d in EIGHT]
    b_peers = [b_peer(d) for d in SEVEN]
    x_peers, ya_peer = [a_peers[1], a_peers[0], a_peers[2]], a_peers[3]
    z_peers, yb_peer = b_peers[:3], b_peers[3]

    def rt_copy(p):
        dst = stage.at[p // 2, pl.ds(PART * (p % 2), PART)]
        return pltpu.make_async_copy(rt_ref.at[:, core * 4 + p, :], dst, st_sem.at[p])

    psi_copy = pltpu.make_async_copy(psi_ref, pin, in_sem)
    psi_copy.start()
    for p in QUAD:
        rt_copy(p).start()
    for c in range(NCH):
        for h in BOTH:
            src = el_ref.at[pl.ds(h * 64 + ia8 * 8, 8), :, seg(c, WIDE)]
            pltpu.make_async_copy(src, gb.at[1, c, pl.ds(8 * h, 8)], el_sem.at[c]).start()

    barrier = pltpu.get_barrier_semaphore()
    for peer in a_peers + b_peers:
        pl.semaphore_signal(barrier, device_id=peer, device_id_type=MESH)

    def init(k):
        for i in range(STEPS):
            xs[i + 1, k] = jnp.zeros((HALF, WIDE), F32)
            vs[i, k] = jnp.zeros((HALF, WIDE), F32)

    loop(NCH, init)
    for ref in (dots, gram, gam, ab_out):
        ref[...] = jnp.zeros_like(ref)

    i0 = lax.broadcasted_iota(jnp.int32, (WIDE, WIDE), 0)
    i1 = lax.broadcasted_iota(jnp.int32, (WIDE, WIDE), 1)
    same = (i0 & 7) == ((i1 >> 3) & 7)
    left = ((i0 >> 3) == i1)[:, :32].astype(BF16)
    right = (((i1 >> 6) * 8 + (i1 & 7)) == i0)[:32].astype(BF16)
    for part, val in enumerate(split3(wsm_ref[...])):
        full = dot(dot(left, val).astype(BF16), right)
        w3[:, seg(part, WIDE)] = jnp.where(same, full, 0.0).astype(BF16)

    psi_copy.wait()
    for j in EIGHT:
        obr[j] = jnp.concatenate([pin[:, seg(8 * h + j, HALF)] for h in BOTH], axis=1)
    pl.semaphore_wait(barrier, len(a_peers) + len(b_peers))

    def remote(src, dst, send, recv, peer):
        pltpu.make_async_remote_copy(src_ref=src, dst_ref=dst, send_sem=send, recv_sem=recv, device_id=peer, device_id_type=MESH).start()

    def wait_bytes(ref, sem):
        pltpu.make_async_copy(ref, ref, sem).wait()

    def parts(k, n):
        return rsb.at[0, k, top(n)]

    upper, lower = top(PART), pl.ds(PART, PART)

    def publish(m, k, first):
        par = lax.rem(m, 2)
        if not first:
            wait_bytes(parts(k, 14), ag_send.at[k])
        gb[par, k, ia] = xs[m, k]
        low, up = gb.at[par, k, ia, lower], gb.at[par, k, ia, upper]
        for peer in x_peers:
            remote(low, low, ag_send.at[k], ag_first.at[par, k], peer)
        remote(up, up, ag_send.at[k], ag_first.at[par, k], ya_peer)
        for peer in x_peers:
            remote(up, up, ag_send.at[k], ag_last.at[par, k], peer)

    def ag_second(par, k):
        wait_bytes(parts(k, 4), ag_first.at[par, k])
        low = gb.at[par, k, pl.ds(core * 8 + row * 4, 4), lower]
        remote(low, low, ag_send.at[k], ag_last.at[par, k], ya_peer)
        up = gb.at[par, k, core * 8 + (1 - row) * 4 + x, upper]
        for peer in x_peers:
            remote(up, up, ag_send.at[k], ag_last.at[par, k], peer)

    def ag_forward(par, k, m):
        wait_bytes(parts(k, 10), ag_last.at[par, k])

        @pl.when(m > 0)
        def _():
            wait_bytes(gb.at[0, k, top(8)], fw_send.at[k])

        part = gb.at[par, k, pl.ds(core * 8, 8)]
        remote(part, part, fw_send.at[k], fw_recv.at[par, k], partner)
        split_blocks(par, k, core)

    def split_blocks(par, k, who):
        base = 3 * MROWS * lax.rem(k, 2) + who * 384

        def piece(i):
            for part, val in enumerate(reversed(split3(gb[par, k, who * 8 + i]))):
                v3[pl.ds(mult(base + part * MROWS + i * HALF, 16), HALF), :] = val

        loop(8, piece)

    def rs_start(par, k):
        remote(sy.at[k, 1 - yb], rsb.at[par, k, pl.ds(6, 4)], rs_send.at[k], rs_first.at[par, k], yb_peer)
        for d, peer in enumerate(z_peers):
            remote(sz.at[k, lax.rem(z + d + 1, 4)], rsb.at[par, k, pl.ds(2 * d, 2)], rs_send.at[k], rs_first.at[par, k], peer)

    def rs_second(par, k):
        wait_bytes(parts(k, 10), rs_first.at[par, k])
        for j in QUAD:
            sy[k, yb, j] = sy[k, yb, j] + rsb[par, k, 6 + j]
        for d, peer in enumerate(z_peers):
            remote(sy.at[k, yb, lax.rem(z + d + 1, 4)], rsb.at[par, k, 11 + d], rs_send.at[k], rs_last.at[par, k], peer)
        for j in BOTH:
            sz[k, z, j] = sz[k, z, j] + rsb[par, k, j] + rsb[par, k, 2 + j] + rsb[par, k, 4 + j]
        remote(sz.at[k, z, 1 - yb], rsb.at[par, k, 10], rs_send.at[k], rs_last.at[par, k], yb_peer)

    def combine(m, k):
        prev = lax.rem(m + 1, 2)
        wait_bytes(parts(k, 4), rs_last.at[prev, k])
        up = sz[k, z, yb] + rsb[prev, k, 10]
        low = sy[k, yb, z] + rsb[prev, k, 11] + rsb[prev, k, 12] + rsb[prev, k, 13]
        w = jnp.concatenate([up, low], axis=0)
        for i in range(STEPS):
            w = w - wide(gam[row1(i), :]) * xs[i + 1, k]
        w = w * wide(gam[row1(STEPS), :])
        xs[m, k] = w
        local_dots(m, k, w)

    def local_dots(m, k, cur):
        new = vs[jnp.maximum(m - 1, 0), k]
        for i in range(STEPS):
            vec = vs[i, k]
            dots[i] = dots[i] + fold(vec * cur)
            dots[STEPS + i] = dots[STEPS + i] + fold(vec * new)

    def red_rows(which, pairs):
        ra[which, ia] = jnp.zeros((16, LANE), F32)
        for src, dst in pairs:
            ra[which, ia, row1(dst), :] = jnp.sum(dots[src], **ROWSUM)
        mine = ra.at[which, ia]
        for peer in a_peers:
            remote(mine, mine, ra_send.at[which], ra_recv.at[which], peer)
        dots[...] = jnp.zeros_like(dots)

    def red_mid(which):
        wait_bytes(ra.at[which, top(15)], ra_recv.at[which])
        wait_bytes(ra.at[which, top(15)], ra_send.at[which])
        total = ra[which, 0]
        for i in range(1, 16):
            total = total + ra[which, i]
        rb[which, ib] = total
        mine = rb.at[which, ib]
        for peer in b_peers:
            remote(mine, mine, rb_send.at[which], rb_recv.at[which], peer)

    def red_end(which):
        wait_bytes(rb.at[which, top(7)], rb_recv.at[which])
        wait_bytes(rb.at[which, top(7)], rb_send.at[which])
        total = rb[which, 0]
        for i in SEVEN:
            total = total + rb[which, i]
        return jnp.broadcast_to(jnp.sum(total, axis=1, keepdims=True), (16, LANE))

    def record(line, m, val):
        here = lax.broadcasted_iota(jnp.int32, (1, LANE), 1) == m - 1
        ab_out[row1(line), :] = jnp.where(here, val, ab_out[row1(line), :])

    def red1_start():
        red_rows(0, [(i, i) for i in range(STEPS)] + [(STEPS + i, 8 + i) for i in range(STEPS)])

    def red1_end(m):
        total = red_end(0)
        c8 = total[:8]
        cg[...] = c8
        gram[jnp.maximum(m - 1, 0)] = total[8:]
        now = lax.broadcasted_iota(jnp.int32, c8.shape, 0) == m - 1
        record(0, m, jnp.sum(jnp.where(now, c8, 0.0), **ROWSUM))

        def piece(k):
            cur = xs[m, k]
            for i in range(STEPS):
                cur = cur - wide(cg[row1(i), :]) * vs[i, k]
            u1[k] = cur
            for i in range(STEPS):
                dots[i] = dots[i] + fold(vs[i, k] * cur)
            dots[STEPS] = dots[STEPS] + fold(cur * cur)

        loop(NCH, piece)
        red_rows(1, [(i, i) for i in range(STEPS)] + [(STEPS, 8)])

    def spare(i, slot):
        return rbuf.at[i // 2, lax.rem(i, 2), slot, :, top(LANE)]

    def export_pack(vec, n):
        for sp in BOTH:
            rows = [vec[2 * n + h, :, seg(sp, LANE)] for h in BOTH] + [jnp.zeros((32, LANE), F32)]
            tile = jnp.concatenate(rows, axis=0).T
            for s in BOTH:
                for g in EIGHT:
                    to, off = divmod(8 * n + g, 3)
                    obuf[to, seg(6 * sp + 3 * s + off, 8), :] = tile[seg(8 * s + g, 8), :]

    def export_send(i):
        for d, peer in enumerate(a_peers[:7]):
            to_row = lax.rem(row + (d + 1) // 4, 2)
            to = lax.rem(to_row + yb, 2) * 4 + lax.rem(x + (d + 1) % 4, 4)
            remote(obuf.at[to], spare(i, ia8), ex_send, ex_recv.at[i], peer)
        spare(i, ia8)[...] = obuf[mem]

    def export_done():
        wait_bytes(obuf.at[top(7)], ex_send)

    def red2_end(m, last):
        total = red_end(1)
        d8 = total[:8]
        sq = total[8:9]
        for i in range(STEPS):
            di = d8[row1(i)]
            inner = jnp.sum(d8 * gram[i], **ROWSUM)
            sq = sq - 2.0 * di * di + di * (2.0 * inner - di * gram[i, row1(i), :])
        beta = jnp.sqrt(sq)
        inv = 1.0 / beta
        record(1, m, beta)
        gam[...] = cg[...] + d8
        gam[row1(STEPS), :] = inv
        if last:
            scale = inv * math.sqrt(float(4 * D * D))
            for i in range(NCH):
                wait_bytes(obuf.at[top(7)], ex_recv.at[i])

            def final(j):
                cur = spare(STEPS, j)[...]
                for i in range(STEPS):
                    cur = cur - d8[row1(i)] * spare(i, j)[...]
                obuf[j] = cur * scale

            export_done()
            loop(8, final)
            for h in BOTH:
                v_out[:, seg(h, 384)] = jnp.concatenate([obuf[j, :, seg(h, HALF)] for j in EIGHT], axis=1)
        else:

            def piece(k):
                cur = u1[k]
                for i in range(STEPS):
                    cur = cur - wide(d8[row1(i)]) * vs[i, k]
                vs[m, k] = cur * wide(inv)

            loop(NCH, piece)

    def left_half(par, k):
        wait_bytes(gb.at[par, k, pl.ds((1 - core) * 8, 8)], fw_recv.at[par, k])
        split_blocks(par, k, 1 - core)
        h = lax.rem(k, 2)
        base = mult(3 * MROWS * h, 3 * MROWS)
        val = dot6(l3.at[:, pl.ds(base, 3 * MROWS)], v3.at[pl.ds(base, 3 * MROWS)], MROWS)
        t1[...] = jnp.where(h == 0, 0.0, t1[...]) + val

    def mix_chunk(n):
        for q in TRIO:
            xg = [t1[seg(4 * q + i, 64), :] for i in QUAD]
            for p in BOTH:
                for sp in BOTH:
                    e, o = (xg[2 * p + i][:, seg(sp, LANE)] for i in BOTH)
                    for s, val in enumerate(pair_halves(e, o)):
                        for part, piece in enumerate(reversed(split3(val))):
                            tq[seg(4 * part + 2 * sp + s, 64), seg(2 * q + p, LANE)] = piece
        out = dot6(w3, tq, WIDE)
        for pp in range(NCH):
            h, g3 = divmod(pp, 3)
            for t in QUAD:
                for rp in QUAD:
                    e, f = (out[seg(8 * t + 2 * rp + i, 8), seg(pp, LANE)] for i in BOTH)
                    g = jnp.concatenate(pair_halves(e, f), axis=0)
                    for part, val in enumerate(split3(g)):
                        t2[seg(12 * h + 3 * t + g3, 16), pl.ds(mult(part * D + n * THIRD + rp * LANE, LANE), LANE)] = val

    def right_half(k):
        n = k // 2
        rows = t2.at[pl.ds(mult((k - 2 * n) * 192, 192), 192)]
        o3[...] = dot6(rows, r3.at[:, pl.ds(mult(n * THIRD, THIRD), THIRD)], D)

    def send_out(m, k):
        @pl.when(m > 0)
        def _():
            wait_bytes(parts(k, 14), rs_send.at[k])

        for j in QUAD:
            y = [o3[seg(t, HALF), seg(j, LANE)] for t in QUAD]
            for sp in BOTH:
                for i, val in enumerate(pair_halves(y[2 * sp], y[2 * sp + 1])):
                    sz[k, j, i, :, seg(sp, LANE)] = val[:PART]
                    sy[k, i, j, :, seg(sp, LANE)] = val[PART:]
        rs_start(lax.rem(m, 2), k)

    high, deep = top(40), pl.ds(40, 56)

    def rg_send(c, who, rows, recv, peers):
        part = rbuf.at[c, core, who, rows]
        for peer in peers:
            remote(part, part, rr_send.at[c], recv.at[c], peer)

    def rg_wait(n, rows, sem):
        wait_bytes(rbuf.at[0, 0, top(n), top(rows)], sem)

    def rg_start(c):
        rg_send(c, mem, deep, rr_deep, x_peers)
        rg_send(c, mem, high, rr_high, [ya_peer])
        rg_send(c, mem, high, rr_up, x_peers)

    def rg_bytes(n):
        return rbuf.at[0, 0, top(n)]

    def rg_second(c):
        rg_wait(7, PART, rr_deep.at[c])
        rg_wait(1, 40, rr_high.at[c])
        rg_send(c, pl.ds(ya * 4, 4), deep, rr_low, [ya_peer])
        rg_send(c, (1 - ya) * 4 + x, high, rr_up, x_peers)

    def rg_split(c):
        def piece(i):
            turn = i // 4
            rr = i - 4 * turn
            half = lax.rem(core + turn, 2)

            @pl.when(i == 4)
            def _():
                wait_bytes(rbuf.at[c, half], rf_recv.at[c])

            for bg in range(12):
                dst = mult((bg // 4) * THIRD + (half * 4 + rr) * 64 + (bg % 4) * 16, 16)
                eights = []
                for e in BOTH:
                    who, off = divmod(2 * bg + e, 3)
                    eights.append(rbuf[c, half, who, pl.ds(mult(rr * PART + off * 8, 8), 8), :])
                for part, val in enumerate(reversed(split3(jnp.concatenate(eights, axis=0)))):
                    r3[pl.ds(part * D + dst, 16), pl.ds(mult(c * THIRD, THIRD), THIRD)] = val

        loop(8, piece)

    def rg_forward(c):
        rg_wait(7, 32, rr_low.at[c])
        rg_wait(5, HALF, rr_up.at[c])
        part = rbuf.at[c, core]
        remote(part, part, rf_send.at[c], rf_recv.at[c], partner)

    for d, peer in enumerate(a_peers[:7]):
        to = lax.rem(row + (d + 1) // 4, 2) * 4 + lax.rem(x + (d + 1) % 4, 4)
        remote(obr.at[to], pbuf.at[mem], ps_send, ps_recv, peer)
    pbuf[mem] = obr[ia8]

    for p in QUAD:
        rt_copy(p).wait()
    for i in BOTH:
        for j in QUAD:
            a, b, c = (stage[i, :, seg(3 * j + e, LANE)] for e in TRIO)
            lo = low_half(a.shape)
            for e, val in enumerate((jnp.where(lo, a, b), swap(jnp.where(lo, c, a)), jnp.where(lo, b, c))):
                rbuf[e, core, mem, seg(i, HALF), seg(j, LANE)] = val
    rg_start(0)

    wait_bytes(pbuf.at[top(7)], ps_recv)
    wait_bytes(pbuf.at[top(7)], ps_send)
    for i in EIGHT:
        for s in QUAD:
            t1[seg(8 * s + i, PART), :96] = pbuf[i, seg(s, PART), :]
    for n in TRIO:
        for sp in BOTH:
            tile = jnp.concatenate([t1[seg(6 * sp + 3 * i + n, 64), :LANE] for i in BOTH], axis=0).T
            for h in BOTH:
                xs[0, 2 * n + h, :, seg(sp, LANE)] = tile[seg(h, HALF), :]

    def first_dots(k):
        local_dots(0, k, xs[0, k])

    def el_piece(i):
        for t in range(12):
            c, h = divmod(t // 3, 2)
            for part, val in enumerate(split3(gb[1, t // 2, i, :, seg(t % 2, LANE)])):
                l3[pl.ds(mult(i * HALF, 16), HALF), seg(3 * (6 * h + 2 * part + c) + t % 3, LANE)] = val

    for c in range(NCH):
        wait_bytes(gb.at[1, c], el_sem.at[c])

    def lead(e):
        @pl.when(e == 0)
        def _():
            for k in TRIO:
                publish(0, k, True)

        @pl.when(e == 1)
        def _():
            publish(0, 3, True)
            publish(0, 4, True)
            loop(NCH, first_dots)

        @pl.when(e == 2)
        def _():
            ag_second(0, 0)
            rg_second(0)
            ag_second(0, 1)
            publish(0, 5, True)

        @pl.when(e == 3)
        def _():
            ag_second(0, 3)
            ag_second(0, 2)
            rg_forward(0)

        loop(4, lambda i: el_piece(4 * e + i))

    loop(4, lead)
    ag_second(0, 5)
    rg_start(1)
    rg_split(0)
    ag_second(0, 4)
    ag_forward(0, 0, 0)

    def step(m):
        par = lax.rem(m, 2)
        nxt = 1 - par
        more, first, later = m < LAST, m == 0, m > 0

        def finish(k):
            combine(m, k)
            publish(m, k, False)

        def halves(k):
            @pl.when(k == 1)
            def _():
                ag_forward(par, 1, m)

                @pl.when(later)
                def _():
                    ag_second(par, 3)
                    finish(5)

                red1_start()

                @pl.when(first)
                def _():
                    rg_start(2)
                    rg_second(1)

            @pl.when(k == 2)
            def _():
                pl.when(later)(lambda: ag_second(par, 4))
                ag_forward(par, 3, m)
                red_mid(0)
                pl.when(later)(lambda: ag_second(par, 5))

            @pl.when(k == 4)
            def _():
                red1_end(m)
                ag_forward(par, 5, m)
                pl.when(first)(lambda: rg_second(2))

            left_half(par, k)

            pl.when(k == 1)(lambda: ag_forward(par, 2, m))
            pl.when(k == 3)(lambda: ag_forward(par, 4, m))
            pl.when(lax.rem(k, 2) == 1)(lambda: mix_chunk(k // 2))

        loop(NCH, halves)
        pl.when(later)(lambda: export_send(m - 1))
        red_mid(1)

        def advance(k):
            combine(m + 1, k)
            pl.when(more)(lambda: publish(m + 1, k, False))

        def spread(k):
            pl.when(more)(lambda: ag_second(nxt, k))

        def outs(k):
            pl.when(first & (k == 1))(lambda: rg_forward(1))

            @pl.when(first & (k == 2))
            def _():
                rg_split(1)
                rg_forward(2)

            pl.when(first & (k == 4))(lambda: rg_split(2))
            right_half(k)
            pl.when(k == 3)(lambda: rs_second(par, 1))

            @pl.when(k == 5)
            def _():
                advance(1)
                rs_second(par, 3)

            send_out(m, k)

            @pl.when(k == 2)
            def _():
                red2_end(m, False)
                rs_second(par, 0)

            @pl.when(k == 4)
            def _():
                rs_second(par, 2)
                advance(0)

        loop(NCH, outs)

        @pl.when(first)
        def _():
            for c in TRIO:
                wait_bytes(rg_bytes(7), rr_send.at[c])
                wait_bytes(rbuf.at[0, 0], rf_send.at[c])

        spread(0)
        pl.when(later)(export_done)
        rs_second(par, 4)
        export_pack(vs.at[m], 0)
        export_pack(vs.at[m], 1)
        advance(2)
        spread(1)
        export_pack(vs.at[m], 2)
        advance(3)
        pl.when(more)(lambda: ag_forward(nxt, 0, 1))
        rs_second(par, 5)
        spread(2)
        advance(4)

    loop(STEPS, step)

    export_send(LAST)
    combine(STEPS, 5)
    red1_start()
    red_mid(0)
    red1_end(STEPS)
    export_done()
    for n in TRIO:
        export_pack(u1, n)
    export_send(STEPS)
    red_mid(1)
    red2_end(STEPS, True)
    for k in range(NCH):
        wait_bytes(parts(k, 14), ag_send.at[k])
        wait_bytes(parts(k, 14), rs_send.at[k])
        wait_bytes(gb.at[0, k, top(8)], fw_send.at[k])


def run_kernel(psi, wsm, el, rt):
    vmem = pl.BlockSpec(memory_space=pltpu.VMEM)
    hbm = pl.BlockSpec(memory_space=pl.ANY)
    dma = pltpu.SemaphoreType.DMA
    six, pair, three = dma((NCH,)), dma((2,)), dma((3,))
    both = dma((2, NCH))
    block = (HALF, WIDE)
    start = pltpu.VMEM((8, 96, 96), F32)
    return pl.pallas_call(
        kernel,
        out_shape=(jax.ShapeDtypeStruct((96, MROWS), F32), jax.ShapeDtypeStruct((8, LANE), F32)),
        in_specs=[hbm, vmem, hbm, hbm],
        out_specs=(vmem, vmem),
        scratch_shapes=[
            pltpu.VMEM((MROWS, 3 * D), BF16),
            pltpu.VMEM((3 * D, D), BF16),
            pltpu.VMEM((WIDE, MROWS), BF16),
            pltpu.VMEM((2, NCH, 16, *block), F32),
            pltpu.VMEM((3 * D, WIDE), BF16),
            pltpu.VMEM((MROWS, WIDE), F32),
            pltpu.VMEM((MROWS, MROWS), BF16),
            pltpu.VMEM((384, 3 * D), BF16),
            pltpu.VMEM((192, THIRD), F32),
            pltpu.VMEM((NCH, 4, 2, PART, WIDE), F32),
            pltpu.VMEM((NCH, 2, 4, PART, WIDE), F32),
            pltpu.VMEM((2, NCH, 14, PART, WIDE), F32),
            pltpu.VMEM((STEPS + 1, NCH, *block), F32),
            pltpu.VMEM((STEPS, NCH, *block), F32),
            pltpu.VMEM((NCH, *block), F32),
            pltpu.VMEM((2, HALF, D), F32),
            pltpu.VMEM((3, 2, 8, 96, THIRD), F32),
            start,
            pltpu.VMEM((8, 96, LANE), F32),
            start,
            pltpu.VMEM((96, MROWS), F32),
            pltpu.VMEM((2 * STEPS, 8, LANE), F32),
            pltpu.VMEM((2, 16, 16, LANE), F32),
            pltpu.VMEM((2, 8, 16, LANE), F32),
            pltpu.VMEM((8, LANE), F32),
            pltpu.VMEM((8, LANE), F32),
            pltpu.VMEM((STEPS, 8, LANE), F32),
            both, both, six, both, both, six, both, six, pair, pair, pair, pair,
            dma((4,)), six, three, three, three, three, three, three, three, dma, dma, dma, dma, six,
        ],
        compiler_params=pltpu.CompilerParams(collective_id=0, has_side_effects=True, vmem_limit_bytes=67043328),
        name="lanczos",
    )(psi, wsm, el, rt)


def solution(mesh):
    grid = Mesh(mesh.devices.reshape(4, 2, 2, 4, 2), AXES)
    psi_spec = P("core", None, None, ("z", "yb", "ya", "x"))

    def local_fn(psi_loc, env_left, env_right, mpo_pair):
        psi = jnp.transpose(psi_loc, (1, 2, 3, 0)).reshape(96, MROWS)
        wsm = jnp.transpose(mpo_pair.reshape(8, 8, 4, 4), (3, 1, 2, 0)).reshape(32, 32)
        vec, ab = run_kernel(psi, wsm, env_left.reshape(LANE, HALF, D), env_right)
        out = jnp.transpose(vec.reshape(2, 2, PART, MROWS), (3, 0, 1, 2))
        return ab[0, :STEPS], ab[1, :STEPS], out

    return jax.shard_map(
        local_fn,
        mesh=grid,
        in_specs=(psi_spec, P("core", None, None), P(("z", "yb", "ya", "x"), None, None), P()),
        out_specs=(P(), P(), psi_spec),
        check_vma=False,
    )
```

```python
import functools
import math

import jax
import jax.numpy as jnp
from jax import lax
from jax.experimental import pallas as pl
from jax.experimental.pallas import tpu as pltpu
from jax.sharding import Mesh
from jax.sharding import PartitionSpec as P

STEPS = 5
AXES = ("z", "yb", "ya", "x", "core")
F32, BF16 = jnp.float32, jnp.bfloat16
ROWSUM = dict(axis=0, keepdims=True)
MESH = pl.DeviceIdType.MESH
D = 1536
HALF = 48
NCH = 6
LANE = 128
WIDE = 256
MROWS = 768
PART = 24
THIRD = 512
LAST = STEPS - 1


def split3(val):
    hi = val.astype(BF16)
    rest = val - hi.astype(F32)
    mid = rest.astype(BF16)
    low = (rest - mid.astype(F32)).astype(BF16)
    return hi, mid, low


def swap(val):
    return pltpu.roll(val, 64, axis=val.ndim - 1)


def low_half(shape):
    return lax.broadcasted_iota(jnp.int32, shape, len(shape) - 1) < 64


def dot(a, b):
    return jnp.dot(a, b, preferred_element_type=F32)


def dot6(a, b, k):
    return dot(a[...], b[...]) + dot(a[:, : 2 * k], b[k:, :]) + dot(a[:, :k], b[2 * k :, :])


BOTH, TRIO, QUAD, EIGHT, SEVEN = range(2), range(3), range(4), range(8), range(1, 8)


def loop(n, body):
    def run(i, carry):
        body(i)
        return carry

    lax.fori_loop(0, n, run, 0)


def top(n):
    return pl.ds(0, n)


def mult(val, n):
    return pl.multiple_of(val, n)


def seg(i, size):
    return slice(i * size, (i + 1) * size)


def row1(i):
    return slice(i, i + 1)


def wide(val):
    return jnp.concatenate([val, val], axis=1)


def pair_halves(e, o):
    lo = low_half(e.shape)
    return jnp.where(lo, e, swap(o)), jnp.where(lo, swap(e), o)


def fold(val):
    return jnp.sum(val.reshape(-1, 8, LANE), axis=0)


def kernel(
    psi_ref, wsm_ref, el_ref, rt_ref, v_out, ab_out,
    l3, r3, w3, gb, v3, t1, tq, t2, o3, sz, sy, rsb, xs, vs, u1, stage, rbuf, pbuf, obuf, obr, pin, dots, ra, rb, cg, gam, gram,
    rs_first, rs_last, rs_send, ag_first, ag_last, ag_send, fw_recv, fw_send, ra_recv, ra_send, rb_recv, rb_send,
    st_sem, el_sem, rr_deep, rr_high, rr_low, rr_up, rr_send, rf_recv, rf_send, ps_recv, ps_send, in_sem, ex_send, ex_recv,
):
    z, yb, ya, x, core = (lax.axis_index(name) for name in AXES)
    row = lax.rem(ya + yb, 2)
    ia8 = row * 4 + x
    ia = core * 8 + ia8
    ib = z * 2 + yb
    mem = ya * 4 + x

    def a_peer(d, other=False):
        to_row = lax.rem(row + d // 4, 2)
        return {"z": z, "yb": yb, "ya": lax.rem(to_row + yb, 2), "x": lax.rem(x + d % 4, 4), "core": 1 - core if other else core}

    def b_peer(d):
        to_yb = lax.rem(yb + d // 4, 2)
        return {"z": lax.rem(z + d % 4, 4), "yb": to_yb, "ya": lax.rem(row + to_yb, 2), "x": x, "core": core}

    partner = a_peer(0, True)
    a_peers = [a_peer(d) for d in SEVEN] + [a_peer(d, True) for d in EIGHT]
    b_peers = [b_peer(d) for d in SEVEN]
    x_peers, ya_peer = [a_peers[1], a_peers[0], a_peers[2]], a_peers[3]
    z_peers, yb_peer = b_peers[:3], b_peers[3]

    def rt_copy(p):
        dst = stage.at[p // 2, pl.ds(PART * (p % 2), PART)]
        return pltpu.make_async_copy(rt_ref.at[:, core * 4 + p, :], dst, st_sem.at[p])

    psi_copy = pltpu.make_async_copy(psi_ref, pin, in_sem)
    psi_copy.start()
    for p in QUAD:
        rt_copy(p).start()
    for c in range(NCH):
        for h in BOTH:
            src = el_ref.at[pl.ds(h * 64 + ia8 * 8, 8), :, seg(c, WIDE)]
            pltpu.make_async_copy(src, gb.at[1, c, pl.ds(8 * h, 8)], el_sem.at[c]).start()

    barrier = pltpu.get_barrier_semaphore()
    for peer in a_peers + b_peers:
        pl.semaphore_signal(barrier, device_id=peer, device_id_type=MESH)

    def init(k):
        for i in range(STEPS):
            xs[i + 1, k] = jnp.zeros((HALF, WIDE), F32)
            vs[i, k] = jnp.zeros((HALF, WIDE), F32)

    loop(NCH, init)
    for ref in (dots, gram, gam, ab_out):
        ref[...] = jnp.zeros_like(ref)

    i0 = lax.broadcasted_iota(jnp.int32, (WIDE, WIDE), 0)
    i1 = lax.broadcasted_iota(jnp.int32, (WIDE, WIDE), 1)
    same = (i0 & 7) == ((i1 >> 3) & 7)
    left = ((i0 >> 3) == i1)[:, :32].astype(BF16)
    col = lax.broadcasted_iota(jnp.int32, (LANE, 4 * WIDE), 1)
    line = ((col & 7) << 4) + (((col >> 6) & 3) << 2) + (col >> 8)
    pick = (line == lax.broadcasted_iota(jnp.int32, (LANE, 4 * WIDE), 0)).astype(BF16)
    for part, val in enumerate(split3(wsm_ref[...].T)):
        rows = dot(val, pick)
        rows = jnp.concatenate([rows[:, seg(t, WIDE)] for t in QUAD], axis=0)
        full = dot(left, rows.astype(BF16))
        w3[:, seg(part, WIDE)] = jnp.where(same, full, 0.0).astype(BF16)

    psi_copy.wait()
    for j in EIGHT:
        obr[j] = jnp.concatenate([pin[:, seg(8 * h + j, HALF)] for h in BOTH], axis=1)
    pl.semaphore_wait(barrier, len(a_peers) + len(b_peers))

    def remote(src, dst, send, recv, peer):
        pltpu.make_async_remote_copy(src_ref=src, dst_ref=dst, send_sem=send, recv_sem=recv, device_id=peer, device_id_type=MESH).start()

    def wait_bytes(ref, sem):
        pltpu.make_async_copy(ref, ref, sem).wait()

    def parts(k, n):
        return rsb.at[0, k, top(n)]

    upper, lower = top(PART), pl.ds(PART, PART)

    def publish(m, k, first):
        par = lax.rem(m, 2)
        if not first:
            wait_bytes(parts(k, 14), ag_send.at[k])
        gb[par, k, ia] = xs[m, k]
        low, up = gb.at[par, k, ia, lower], gb.at[par, k, ia, upper]
        for peer in x_peers:
            remote(low, low, ag_send.at[k], ag_first.at[par, k], peer)
        remote(up, up, ag_send.at[k], ag_first.at[par, k], ya_peer)
        for peer in x_peers:
            remote(up, up, ag_send.at[k], ag_last.at[par, k], peer)

    def ag_second(par, k):
        wait_bytes(parts(k, 4), ag_first.at[par, k])
        low = gb.at[par, k, pl.ds(core * 8 + row * 4, 4), lower]
        remote(low, low, ag_send.at[k], ag_last.at[par, k], ya_peer)
        up = gb.at[par, k, core * 8 + (1 - row) * 4 + x, upper]
        for peer in x_peers:
            remote(up, up, ag_send.at[k], ag_last.at[par, k], peer)

    def ag_forward(par, k, m):
        wait_bytes(parts(k, 10), ag_last.at[par, k])

        @pl.when(m > 0)
        def _():
            wait_bytes(gb.at[0, k, top(8)], fw_send.at[k])

        part = gb.at[par, k, pl.ds(core * 8, 8)]
        remote(part, part, fw_send.at[k], fw_recv.at[par, k], partner)
        split_blocks(par, k, core)

    def split_blocks(par, k, who):
        base = 3 * MROWS * lax.rem(k, 2) + who * 384

        def piece(i):
            for part, val in enumerate(reversed(split3(gb[par, k, who * 8 + i]))):
                v3[pl.ds(mult(base + part * MROWS + i * HALF, 16), HALF), :] = val

        loop(8, piece)

    def rs_start(par, k):
        remote(sy.at[k, 1 - yb], rsb.at[par, k, pl.ds(6, 4)], rs_send.at[k], rs_first.at[par, k], yb_peer)
        for d, peer in enumerate(z_peers):
            remote(sz.at[k, lax.rem(z + d + 1, 4)], rsb.at[par, k, pl.ds(2 * d, 2)], rs_send.at[k], rs_first.at[par, k], peer)

    def rs_second(par, k):
        wait_bytes(parts(k, 10), rs_first.at[par, k])
        for j in QUAD:
            sy[k, yb, j] = sy[k, yb, j] + rsb[par, k, 6 + j]
        for d, peer in enumerate(z_peers):
            remote(sy.at[k, yb, lax.rem(z + d + 1, 4)], rsb.at[par, k, 11 + d], rs_send.at[k], rs_last.at[par, k], peer)
        for j in BOTH:
            sz[k, z, j] = sz[k, z, j] + rsb[par, k, j] + rsb[par, k, 2 + j] + rsb[par, k, 4 + j]
        remote(sz.at[k, z, 1 - yb], rsb.at[par, k, 10], rs_send.at[k], rs_last.at[par, k], yb_peer)

    def combine(m, k):
        prev = lax.rem(m + 1, 2)
        wait_bytes(parts(k, 4), rs_last.at[prev, k])
        up = sz[k, z, yb] + rsb[prev, k, 10]
        low = sy[k, yb, z] + rsb[prev, k, 11] + rsb[prev, k, 12] + rsb[prev, k, 13]
        w = jnp.concatenate([up, low], axis=0)
        for i in range(STEPS):
            w = w - wide(gam[row1(i), :]) * xs[i + 1, k]
        w = w * wide(gam[row1(STEPS), :])
        xs[m, k] = w
        local_dots(m, k, w)

    def local_dots(m, k, cur):
        new = vs[jnp.maximum(m - 1, 0), k]
        for i in range(STEPS):
            vec = vs[i, k]
            dots[i] = dots[i] + fold(vec * cur)
            dots[STEPS + i] = dots[STEPS + i] + fold(vec * new)

    def red_rows(which, pairs):
        ra[which, ia] = jnp.zeros((16, LANE), F32)
        for src, dst in pairs:
            ra[which, ia, row1(dst), :] = jnp.sum(dots[src], **ROWSUM)
        mine = ra.at[which, ia]
        for peer in a_peers:
            remote(mine, mine, ra_send.at[which], ra_recv.at[which], peer)
        dots[...] = jnp.zeros_like(dots)

    def red_mid(which):
        wait_bytes(ra.at[which, top(15)], ra_recv.at[which])
        wait_bytes(ra.at[which, top(15)], ra_send.at[which])
        total = ra[which, 0]
        for i in range(1, 16):
            total = total + ra[which, i]
        rb[which, ib] = total
        mine = rb.at[which, ib]
        for peer in b_peers:
            remote(mine, mine, rb_send.at[which], rb_recv.at[which], peer)

    def red_end(which):
        wait_bytes(rb.at[which, top(7)], rb_recv.at[which])
        wait_bytes(rb.at[which, top(7)], rb_send.at[which])
        total = rb[which, 0]
        for i in SEVEN:
            total = total + rb[which, i]
        return jnp.broadcast_to(jnp.sum(total, axis=1, keepdims=True), (16, LANE))

    def record(line, m, val):
        here = lax.broadcasted_iota(jnp.int32, (1, LANE), 1) == m - 1
        ab_out[row1(line), :] = jnp.where(here, val, ab_out[row1(line), :])

    def red1_start():
        red_rows(0, [(i, i) for i in range(STEPS)] + [(STEPS + i, 8 + i) for i in range(STEPS)])

    def red1_end(m):
        total = red_end(0)
        c8 = total[:8]
        cg[...] = c8
        gram[jnp.maximum(m - 1, 0)] = total[8:]
        now = lax.broadcasted_iota(jnp.int32, c8.shape, 0) == m - 1
        record(0, m, jnp.sum(jnp.where(now, c8, 0.0), **ROWSUM))

        def piece(k):
            cur = xs[m, k]
            for i in range(STEPS):
                cur = cur - wide(cg[row1(i), :]) * vs[i, k]
            u1[k] = cur
            for i in range(STEPS):
                dots[i] = dots[i] + fold(vs[i, k] * cur)
            dots[STEPS] = dots[STEPS] + fold(cur * cur)

        loop(NCH, piece)
        red_rows(1, [(i, i) for i in range(STEPS)] + [(STEPS, 8)])

    def spare(i, slot):
        return rbuf.at[i // 2, lax.rem(i, 2), slot, :, top(LANE)]

    def export_pack(vec, n):
        for sp in BOTH:
            rows = [vec[2 * n + h, :, seg(sp, LANE)] for h in BOTH] + [jnp.zeros((32, LANE), F32)]
            tile = jnp.concatenate(rows, axis=0).T
            for s in BOTH:
                for g in EIGHT:
                    to, off = divmod(8 * n + g, 3)
                    obuf[to, seg(6 * sp + 3 * s + off, 8), :] = tile[seg(8 * s + g, 8), :]

    def export_send(i):
        for d, peer in enumerate(a_peers[:7]):
            to_row = lax.rem(row + (d + 1) // 4, 2)
            to = lax.rem(to_row + yb, 2) * 4 + lax.rem(x + (d + 1) % 4, 4)
            remote(obuf.at[to], spare(i, ia8), ex_send, ex_recv.at[i], peer)
        spare(i, ia8)[...] = obuf[mem]

    def export_done():
        wait_bytes(obuf.at[top(7)], ex_send)

    def red2_end(m, last):
        total = red_end(1)
        d8 = total[:8]
        sq = total[8:9]
        for i in range(STEPS):
            di = d8[row1(i)]
            inner = jnp.sum(d8 * gram[i], **ROWSUM)
            sq = sq - 2.0 * di * di + di * (2.0 * inner - di * gram[i, row1(i), :])
        beta = jnp.sqrt(sq)
        inv = 1.0 / beta
        record(1, m, beta)
        gam[...] = cg[...] + d8
        gam[row1(STEPS), :] = inv
        if last:
            scale = inv * math.sqrt(float(4 * D * D))
            for i in range(NCH):
                wait_bytes(obuf.at[top(7)], ex_recv.at[i])

            def final(j):
                cur = spare(STEPS, j)[...]
                for i in range(STEPS):
                    cur = cur - d8[row1(i)] * spare(i, j)[...]
                obuf[j] = cur * scale

            export_done()
            loop(8, final)
            for h in BOTH:
                v_out[:, seg(h, 384)] = jnp.concatenate([obuf[j, :, seg(h, HALF)] for j in EIGHT], axis=1)
        else:

            def piece(k):
                cur = u1[k]
                for i in range(STEPS):
                    cur = cur - wide(d8[row1(i)]) * vs[i, k]
                vs[m, k] = cur * wide(inv)

            loop(NCH, piece)

    def left_half(par, k):
        wait_bytes(gb.at[par, k, pl.ds((1 - core) * 8, 8)], fw_recv.at[par, k])
        split_blocks(par, k, 1 - core)
        h = lax.rem(k, 2)
        base = mult(3 * MROWS * h, 3 * MROWS)
        val = dot6(l3.at[:, pl.ds(base, 3 * MROWS)], v3.at[pl.ds(base, 3 * MROWS)], MROWS)
        t1[...] = jnp.where(h == 0, 0.0, t1[...]) + val

    def mix_chunk(n):
        for q in TRIO:
            xg = [t1[seg(4 * q + i, 64), :] for i in QUAD]
            for p in BOTH:
                for sp in BOTH:
                    e, o = (xg[2 * p + i][:, seg(sp, LANE)] for i in BOTH)
                    for s, val in enumerate(pair_halves(e, o)):
                        for part, piece in enumerate(reversed(split3(val))):
                            tq[seg(4 * part + 2 * sp + s, 64), seg(2 * q + p, LANE)] = piece
        out = dot6(w3, tq, WIDE)
        for pp in range(NCH):
            h, g3 = divmod(pp, 3)
            for t in QUAD:
                for rp in QUAD:
                    e, f = (out[seg(8 * t + 2 * rp + i, 8), seg(pp, LANE)] for i in BOTH)
                    g = jnp.concatenate(pair_halves(e, f), axis=0)
                    for part, val in enumerate(split3(g)):
                        t2[seg(12 * h + 3 * t + g3, 16), pl.ds(mult(part * D + n * THIRD + rp * LANE, LANE), LANE)] = val

    def right_half(k):
        n = k // 2
        rows = t2.at[pl.ds(mult((k - 2 * n) * 192, 192), 192)]
        o3[...] = dot6(rows, r3.at[:, pl.ds(mult(n * THIRD, THIRD), THIRD)], D)

    def send_out(m, k):
        @pl.when(m > 0)
        def _():
            wait_bytes(parts(k, 14), rs_send.at[k])

        for j in QUAD:
            y = [o3[seg(t, HALF), seg(j, LANE)] for t in QUAD]
            for sp in BOTH:
                for i, val in enumerate(pair_halves(y[2 * sp], y[2 * sp + 1])):
                    sz[k, j, i, :, seg(sp, LANE)] = val[:PART]
                    sy[k, i, j, :, seg(sp, LANE)] = val[PART:]
        rs_start(lax.rem(m, 2), k)

    high, deep = top(40), pl.ds(40, 56)

    def rg_send(c, who, rows, recv, peers):
        part = rbuf.at[c, core, who, rows]
        for peer in peers:
            remote(part, part, rr_send.at[c], recv.at[c], peer)

    def rg_wait(n, rows, sem):
        wait_bytes(rbuf.at[0, 0, top(n), top(rows)], sem)

    def rg_start(c):
        rg_send(c, mem, deep, rr_deep, x_peers)
        rg_send(c, mem, high, rr_high, [ya_peer])
        rg_send(c, mem, high, rr_up, x_peers)

    def rg_bytes(n):
        return rbuf.at[0, 0, top(n)]

    def rg_second(c):
        rg_wait(7, PART, rr_deep.at[c])
        rg_wait(1, 40, rr_high.at[c])
        rg_send(c, pl.ds(ya * 4, 4), deep, rr_low, [ya_peer])
        rg_send(c, (1 - ya) * 4 + x, high, rr_up, x_peers)

    def rg_split(c):
        def piece(i):
            turn = i // 4
            rr = i - 4 * turn
            half = lax.rem(core + turn, 2)

            @pl.when(i == 4)
            def _():
                wait_bytes(rbuf.at[c, half], rf_recv.at[c])

            for bg in range(12):
                dst = mult((bg // 4) * THIRD + (half * 4 + rr) * 64 + (bg % 4) * 16, 16)
                eights = []
                for e in BOTH:
                    who, off = divmod(2 * bg + e, 3)
                    eights.append(rbuf[c, half, who, pl.ds(mult(rr * PART + off * 8, 8), 8), :])
                for part, val in enumerate(reversed(split3(jnp.concatenate(eights, axis=0)))):
                    r3[pl.ds(part * D + dst, 16), pl.ds(mult(c * THIRD, THIRD), THIRD)] = val

        loop(8, piece)

    def rg_forward(c):
        rg_wait(7, 32, rr_low.at[c])
        rg_wait(5, HALF, rr_up.at[c])
        part = rbuf.at[c, core]
        remote(part, part, rf_send.at[c], rf_recv.at[c], partner)

    for d, peer in enumerate(a_peers[:7]):
        to = lax.rem(row + (d + 1) // 4, 2) * 4 + lax.rem(x + (d + 1) % 4, 4)
        remote(obr.at[to], pbuf.at[mem], ps_send, ps_recv, peer)
    pbuf[mem] = obr[ia8]

    for p in QUAD:
        rt_copy(p).wait()
    for i in BOTH:
        for j in QUAD:
            a, b, c = (stage[i, :, seg(3 * j + e, LANE)] for e in TRIO)
            lo = low_half(a.shape)
            for e, val in enumerate((jnp.where(lo, a, b), swap(jnp.where(lo, c, a)), jnp.where(lo, b, c))):
                rbuf[e, core, mem, seg(i, HALF), seg(j, LANE)] = val
    rg_start(0)

    wait_bytes(pbuf.at[top(7)], ps_recv)
    wait_bytes(pbuf.at[top(7)], ps_send)
    for i in EIGHT:
        for s in QUAD:
            t1[seg(8 * s + i, PART), :96] = pbuf[i, seg(s, PART), :]
    for n in TRIO:
        for sp in BOTH:
            tile = jnp.concatenate([t1[seg(6 * sp + 3 * i + n, 64), :LANE] for i in BOTH], axis=0).T
            for h in BOTH:
                xs[0, 2 * n + h, :, seg(sp, LANE)] = tile[seg(h, HALF), :]

    def first_dots(k):
        local_dots(0, k, xs[0, k])

    def el_piece(i):
        for t in range(12):
            c, h = divmod(t // 3, 2)
            for part, val in enumerate(split3(gb[1, t // 2, i, :, seg(t % 2, LANE)])):
                l3[pl.ds(mult(i * HALF, 16), HALF), seg(3 * (6 * h + 2 * part + c) + t % 3, LANE)] = val

    for c in range(NCH):
        wait_bytes(gb.at[1, c], el_sem.at[c])

    def lead(e):
        @pl.when(e == 0)
        def _():
            for k in TRIO:
                publish(0, k, True)

        @pl.when(e == 1)
        def _():
            publish(0, 3, True)
            publish(0, 4, True)
            loop(NCH, first_dots)

        @pl.when(e == 2)
        def _():
            ag_second(0, 0)
            rg_second(0)
            ag_second(0, 1)
            publish(0, 5, True)

        @pl.when(e == 3)
        def _():
            ag_second(0, 3)
            ag_second(0, 2)
            rg_forward(0)

        loop(4, lambda i: el_piece(4 * e + i))

    loop(4, lead)
    ag_second(0, 5)
    rg_start(1)
    rg_split(0)
    ag_second(0, 4)
    ag_forward(0, 0, 0)

    def step(m):
        par = lax.rem(m, 2)
        nxt = 1 - par
        more, first, later = m < LAST, m == 0, m > 0

        def finish(k):
            combine(m, k)
            publish(m, k, False)

        def halves(k):
            @pl.when(k == 1)
            def _():
                ag_forward(par, 1, m)

                @pl.when(later)
                def _():
                    ag_second(par, 3)
                    finish(5)

                red1_start()

                @pl.when(first)
                def _():
                    rg_start(2)
                    rg_second(1)

            @pl.when(k == 2)
            def _():
                pl.when(later)(lambda: ag_second(par, 4))
                ag_forward(par, 3, m)
                red_mid(0)
                pl.when(later)(lambda: ag_second(par, 5))

            @pl.when(k == 4)
            def _():
                red1_end(m)
                ag_forward(par, 5, m)
                pl.when(first)(lambda: rg_second(2))

            left_half(par, k)

            pl.when(k == 1)(lambda: ag_forward(par, 2, m))
            pl.when(k == 3)(lambda: ag_forward(par, 4, m))
            pl.when(lax.rem(k, 2) == 1)(lambda: mix_chunk(k // 2))

        loop(NCH, halves)
        pl.when(later)(lambda: export_send(m - 1))
        red_mid(1)

        def advance(k):
            combine(m + 1, k)
            pl.when(more)(lambda: publish(m + 1, k, False))

        def spread(k):
            pl.when(more)(lambda: ag_second(nxt, k))

        def outs(k):
            pl.when(first & (k == 1))(lambda: rg_forward(1))

            @pl.when(first & (k == 2))
            def _():
                rg_split(1)
                rg_forward(2)

            pl.when(first & (k == 4))(lambda: rg_split(2))
            right_half(k)
            pl.when(k == 3)(lambda: rs_second(par, 1))

            @pl.when(k == 5)
            def _():
                advance(1)
                rs_second(par, 3)

            send_out(m, k)

            @pl.when(k == 2)
            def _():
                red2_end(m, False)
                rs_second(par, 0)

            @pl.when(k == 4)
            def _():
                rs_second(par, 2)
                advance(0)

        loop(NCH, outs)

        @pl.when(first)
        def _():
            for c in TRIO:
                wait_bytes(rg_bytes(7), rr_send.at[c])
                wait_bytes(rbuf.at[0, 0], rf_send.at[c])

        spread(0)
        pl.when(later)(export_done)
        rs_second(par, 4)
        export_pack(vs.at[m], 0)
        export_pack(vs.at[m], 1)
        advance(2)
        spread(1)
        export_pack(vs.at[m], 2)
        advance(3)
        pl.when(more)(lambda: ag_forward(nxt, 0, 1))
        rs_second(par, 5)
        spread(2)
        advance(4)

    loop(STEPS, step)

    export_send(LAST)
    combine(STEPS, 5)
    red1_start()
    red_mid(0)
    red1_end(STEPS)
    export_done()
    for n in TRIO:
        export_pack(u1, n)
    export_send(STEPS)
    red_mid(1)
    red2_end(STEPS, True)
    for k in range(NCH):
        wait_bytes(parts(k, 14), ag_send.at[k])
        wait_bytes(parts(k, 14), rs_send.at[k])
        wait_bytes(gb.at[0, k, top(8)], fw_send.at[k])


def run_kernel(psi, wsm, el, rt):
    vmem = pl.BlockSpec(memory_space=pltpu.VMEM)
    hbm = pl.BlockSpec(memory_space=pl.ANY)
    dma = pltpu.SemaphoreType.DMA
    six, pair, three = dma((NCH,)), dma((2,)), dma((3,))
    both = dma((2, NCH))
    block = (HALF, WIDE)
    start = pltpu.VMEM((8, 96, 96), F32)
    return pl.pallas_call(
        kernel,
        out_shape=(jax.ShapeDtypeStruct((96, MROWS), F32), jax.ShapeDtypeStruct((8, LANE), F32)),
        in_specs=[hbm, vmem, hbm, hbm],
        out_specs=(vmem, vmem),
        scratch_shapes=[
            pltpu.VMEM((MROWS, 3 * D), BF16),
            pltpu.VMEM((3 * D, D), BF16),
            pltpu.VMEM((WIDE, MROWS), BF16),
            pltpu.VMEM((2, NCH, 16, *block), F32),
            pltpu.VMEM((3 * D, WIDE), BF16),
            pltpu.VMEM((MROWS, WIDE), F32),
            pltpu.VMEM((MROWS, MROWS), BF16),
            pltpu.VMEM((384, 3 * D), BF16),
            pltpu.VMEM((192, THIRD), F32),
            pltpu.VMEM((NCH, 4, 2, PART, WIDE), F32),
            pltpu.VMEM((NCH, 2, 4, PART, WIDE), F32),
            pltpu.VMEM((2, NCH, 14, PART, WIDE), F32),
            pltpu.VMEM((STEPS + 1, NCH, *block), F32),
            pltpu.VMEM((STEPS, NCH, *block), F32),
            pltpu.VMEM((NCH, *block), F32),
            pltpu.VMEM((2, HALF, D), F32),
            pltpu.VMEM((3, 2, 8, 96, THIRD), F32),
            start,
            pltpu.VMEM((8, 96, LANE), F32),
            start,
            pltpu.VMEM((96, MROWS), F32),
            pltpu.VMEM((2 * STEPS, 8, LANE), F32),
            pltpu.VMEM((2, 16, 16, LANE), F32),
            pltpu.VMEM((2, 8, 16, LANE), F32),
            pltpu.VMEM((8, LANE), F32),
            pltpu.VMEM((8, LANE), F32),
            pltpu.VMEM((STEPS, 8, LANE), F32),
            both, both, six, both, both, six, both, six, pair, pair, pair, pair,
            dma((4,)), six, three, three, three, three, three, three, three, dma, dma, dma, dma, six,
        ],
        compiler_params=pltpu.CompilerParams(collective_id=0, has_side_effects=True, vmem_limit_bytes=67043328),
        name="lanczos",
    )(psi, wsm, el, rt)


def solution(mesh):
    grid = Mesh(mesh.devices.reshape(4, 2, 2, 4, 2), AXES)
    psi_spec = P("core", None, None, ("z", "yb", "ya", "x"))

    def local_fn(psi_loc, env_left, env_right, mpo_pair):
        psi = jnp.transpose(psi_loc, (1, 2, 3, 0)).reshape(96, MROWS)
        wsm = jnp.moveaxis(mpo_pair, 1, -1).reshape(LANE, 8)
        vec, ab = run_kernel(psi, wsm, env_left.reshape(LANE, HALF, D), env_right)
        out = jnp.transpose(vec.reshape(2, 2, PART, MROWS), (3, 0, 1, 2))
        return ab[0, :STEPS], ab[1, :STEPS], out

    return jax.shard_map(
        local_fn,
        mesh=grid,
        in_specs=(psi_spec, P("core", None, None), P(("z", "yb", "ya", "x"), None, None), P()),
        out_specs=(P(), P(), psi_spec),
        check_vma=False,
    )
```

```python
import functools
import math

import jax
import jax.numpy as jnp
from jax import lax
from jax.experimental import pallas as pl
from jax.experimental.pallas import tpu as pltpu
from jax.sharding import Mesh
from jax.sharding import PartitionSpec as P

STEPS = 5
AXES = ("z", "yb", "ya", "x", "core")
F32, BF16 = jnp.float32, jnp.bfloat16
ROWSUM = dict(axis=0, keepdims=True)
MESH = pl.DeviceIdType.MESH
D = 1536
HALF = 48
NCH = 6
LANE = 128
WIDE = 256
MROWS = 768
PART = 24
THIRD = 512
LAST = STEPS - 1


def split3(val):
    hi = val.astype(BF16)
    rest = val - hi.astype(F32)
    mid = rest.astype(BF16)
    low = (rest - mid.astype(F32)).astype(BF16)
    return hi, mid, low


def swap(val):
    return pltpu.roll(val, 64, axis=val.ndim - 1)


def low_half(shape):
    return lax.broadcasted_iota(jnp.int32, shape, len(shape) - 1) < 64


def dot(a, b):
    return jnp.dot(a, b, preferred_element_type=F32)


def dot6(a, b, k):
    return dot(a[...], b[...]) + dot(a[:, : 2 * k], b[k:, :]) + dot(a[:, :k], b[2 * k :, :])


BOTH, TRIO, QUAD, EIGHT, SEVEN = range(2), range(3), range(4), range(8), range(1, 8)


def loop(n, body):
    def run(i, carry):
        body(i)
        return carry

    lax.fori_loop(0, n, run, 0)


def top(n):
    return pl.ds(0, n)


def mult(val, n):
    return pl.multiple_of(val, n)


def seg(i, size):
    return slice(i * size, (i + 1) * size)


def row1(i):
    return slice(i, i + 1)


def wide(val):
    return jnp.concatenate([val, val], axis=1)


def pair_halves(e, o):
    lo = low_half(e.shape)
    return jnp.where(lo, e, swap(o)), jnp.where(lo, swap(e), o)


def fold(val):
    return jnp.sum(val.reshape(-1, 8, LANE), axis=0)


def kernel(
    psi_ref, wsm_ref, el_ref, rt_ref, v_out, ab_out,
    l3, r3, w3, gb, v3, t1, tq, t2, o3, sz, sy, rsb, xs, vs, u1, stage, rbuf, pbuf, obuf, obr, pin, dots, ra, rb, cg, gam, gram,
    rs_first, rs_last, rs_send, ag_first, ag_last, ag_send, fw_recv, fw_send, ra_recv, ra_send, rb_recv, rb_send,
    st_sem, el_sem, rr_deep, rr_high, rr_low, rr_up, rr_send, rf_recv, rf_send, ps_recv, ps_send, in_sem, ex_send, ex_recv,
):
    z, yb, ya, x, core = (lax.axis_index(name) for name in AXES)
    row = lax.rem(ya + yb, 2)
    ia8 = row * 4 + x
    ia = core * 8 + ia8
    ib = z * 2 + yb
    mem = ya * 4 + x

    def a_peer(d, other=False):
        to_row = lax.rem(row + d // 4, 2)
        return {"z": z, "yb": yb, "ya": lax.rem(to_row + yb, 2), "x": lax.rem(x + d % 4, 4), "core": 1 - core if other else core}

    def b_peer(d):
        to_yb = lax.rem(yb + d // 4, 2)
        return {"z": lax.rem(z + d % 4, 4), "yb": to_yb, "ya": lax.rem(row + to_yb, 2), "x": x, "core": core}

    partner = a_peer(0, True)
    a_peers = [a_peer(d) for d in SEVEN] + [a_peer(d, True) for d in EIGHT]
    b_peers = [b_peer(d) for d in SEVEN]
    x_peers, ya_peer = [a_peers[1], a_peers[0], a_peers[2]], a_peers[3]
    z_peers, yb_peer = b_peers[:3], b_peers[3]

    def rt_copy(p):
        dst = stage.at[p // 2, pl.ds(PART * (p % 2), PART)]
        return pltpu.make_async_copy(rt_ref.at[:, core * 4 + p, :], dst, st_sem.at[p])

    psi_copy = pltpu.make_async_copy(psi_ref, pin, in_sem)
    psi_copy.start()
    for p in QUAD:
        rt_copy(p).start()
    for c in range(NCH):
        for h in BOTH:
            src = el_ref.at[pl.ds(h * 64 + ia8 * 8, 8), :, seg(c, WIDE)]
            pltpu.make_async_copy(src, gb.at[1, c, pl.ds(8 * h, 8)], el_sem.at[c]).start()

    barrier = pltpu.get_barrier_semaphore()
    for peer in a_peers + b_peers:
        pl.semaphore_signal(barrier, device_id=peer, device_id_type=MESH)

    def init(k):
        for i in range(STEPS):
            xs[i + 1, k] = jnp.zeros((HALF, WIDE), F32)
            vs[i, k] = jnp.zeros((HALF, WIDE), F32)

    loop(NCH, init)
    for ref in (dots, gram, gam, ab_out):
        ref[...] = jnp.zeros_like(ref)

    i0 = lax.broadcasted_iota(jnp.int32, (WIDE, WIDE), 0)
    i1 = lax.broadcasted_iota(jnp.int32, (WIDE, WIDE), 1)
    same = (i0 & 7) == ((i1 >> 3) & 7)
    left = ((i0 >> 3) == i1)[:, :32].astype(BF16)
    col = lax.broadcasted_iota(jnp.int32, (LANE, 4 * WIDE), 1)
    line = ((col & 7) << 4) + (((col >> 6) & 3) << 2) + (col >> 8)
    pick = (line == lax.broadcasted_iota(jnp.int32, (LANE, 4 * WIDE), 0)).astype(BF16)
    for part, val in enumerate(split3(wsm_ref[...].T)):
        rows = dot(val, pick)
        rows = jnp.concatenate([rows[:, seg(t, WIDE)] for t in QUAD], axis=0)
        full = dot(left, rows.astype(BF16))
        w3[:, seg(part, WIDE)] = jnp.where(same, full, 0.0).astype(BF16)

    psi_copy.wait()
    for j in EIGHT:
        obr[j] = jnp.concatenate([pin[:, seg(8 * h + j, HALF)] for h in BOTH], axis=1)
    pl.semaphore_wait(barrier, len(a_peers) + len(b_peers))

    def remote(src, dst, send, recv, peer):
        pltpu.make_async_remote_copy(src_ref=src, dst_ref=dst, send_sem=send, recv_sem=recv, device_id=peer, device_id_type=MESH).start()

    def wait_bytes(ref, sem):
        pltpu.make_async_copy(ref, ref, sem).wait()

    def parts(k, n):
        return rsb.at[0, k, top(n)]

    upper, lower = top(PART), pl.ds(PART, PART)

    def publish(m, k, first):
        par = lax.rem(m, 2)
        if not first:
            wait_bytes(parts(k, 14), ag_send.at[k])
        gb[par, k, ia] = xs[m, k]
        low, up = gb.at[par, k, ia, lower], gb.at[par, k, ia, upper]
        for peer in x_peers:
            remote(low, low, ag_send.at[k], ag_first.at[par, k], peer)
        remote(up, up, ag_send.at[k], ag_first.at[par, k], ya_peer)
        for peer in x_peers:
            remote(up, up, ag_send.at[k], ag_last.at[par, k], peer)

    def ag_second(par, k):
        wait_bytes(parts(k, 4), ag_first.at[par, k])
        low = gb.at[par, k, pl.ds(core * 8 + row * 4, 4), lower]
        remote(low, low, ag_send.at[k], ag_last.at[par, k], ya_peer)
        up = gb.at[par, k, core * 8 + (1 - row) * 4 + x, upper]
        for peer in x_peers:
            remote(up, up, ag_send.at[k], ag_last.at[par, k], peer)

    def ag_forward(par, k, m):
        wait_bytes(parts(k, 10), ag_last.at[par, k])

        @pl.when(m > 0)
        def _():
            wait_bytes(gb.at[0, k, top(8)], fw_send.at[k])

        part = gb.at[par, k, pl.ds(core * 8, 8)]
        remote(part, part, fw_send.at[k], fw_recv.at[par, k], partner)
        split_blocks(par, k, core)

    def split_blocks(par, k, who):
        base = 3 * MROWS * lax.rem(k, 2) + who * 384

        def piece(i):
            for part, val in enumerate(reversed(split3(gb[par, k, who * 8 + i]))):
                v3[pl.ds(mult(base + part * MROWS + i * HALF, 16), HALF), :] = val

        loop(8, piece)

    def rs_start(par, k):
        remote(sy.at[k, 1 - yb], rsb.at[par, k, pl.ds(6, 4)], rs_send.at[k], rs_first.at[par, k], yb_peer)
        for d, peer in enumerate(z_peers):
            remote(sz.at[k, lax.rem(z + d + 1, 4)], rsb.at[par, k, pl.ds(2 * d, 2)], rs_send.at[k], rs_first.at[par, k], peer)

    def rs_second(par, k):
        wait_bytes(parts(k, 10), rs_first.at[par, k])
        for j in QUAD:
            sy[k, yb, j] = sy[k, yb, j] + rsb[par, k, 6 + j]
        for d, peer in enumerate(z_peers):
            remote(sy.at[k, yb, lax.rem(z + d + 1, 4)], rsb.at[par, k, 11 + d], rs_send.at[k], rs_last.at[par, k], peer)
        for j in BOTH:
            sz[k, z, j] = sz[k, z, j] + rsb[par, k, j] + rsb[par, k, 2 + j] + rsb[par, k, 4 + j]
        remote(sz.at[k, z, 1 - yb], rsb.at[par, k, 10], rs_send.at[k], rs_last.at[par, k], yb_peer)

    def combine(m, k):
        prev = lax.rem(m + 1, 2)
        wait_bytes(parts(k, 4), rs_last.at[prev, k])
        up = sz[k, z, yb] + rsb[prev, k, 10]
        low = sy[k, yb, z] + rsb[prev, k, 11] + rsb[prev, k, 12] + rsb[prev, k, 13]
        w = jnp.concatenate([up, low], axis=0)

        def take(i, w):
            return w - wide(gam[pl.ds(i, 1), :]) * xs[i + 1, k]

        w = lax.fori_loop(0, m - 1, take, w)
        w = w * wide(gam[row1(STEPS), :])
        xs[m, k] = w
        local_dots(m, k, w)

    def local_dots(m, k, cur):
        new = vs[jnp.maximum(m - 1, 0), k]

        def one(i):
            vec = vs[i, k]
            dots[i] = dots[i] + fold(vec * cur)
            dots[STEPS + i] = dots[STEPS + i] + fold(vec * new)

        loop(m, one)

    def red_rows(which, pairs):
        ra[which, ia] = jnp.zeros((16, LANE), F32)
        for src, dst in pairs:
            ra[which, ia, row1(dst), :] = jnp.sum(dots[src], **ROWSUM)
        mine = ra.at[which, ia]
        for peer in a_peers:
            remote(mine, mine, ra_send.at[which], ra_recv.at[which], peer)
        dots[...] = jnp.zeros_like(dots)

    def red_mid(which):
        wait_bytes(ra.at[which, top(15)], ra_recv.at[which])
        wait_bytes(ra.at[which, top(15)], ra_send.at[which])
        total = ra[which, 0]
        for i in range(1, 16):
            total = total + ra[which, i]
        rb[which, ib] = total
        mine = rb.at[which, ib]
        for peer in b_peers:
            remote(mine, mine, rb_send.at[which], rb_recv.at[which], peer)

    def red_end(which):
        wait_bytes(rb.at[which, top(7)], rb_recv.at[which])
        wait_bytes(rb.at[which, top(7)], rb_send.at[which])
        total = rb[which, 0]
        for i in SEVEN:
            total = total + rb[which, i]
        return jnp.broadcast_to(jnp.sum(total, axis=1, keepdims=True), (16, LANE))

    def record(line, m, val):
        here = lax.broadcasted_iota(jnp.int32, (1, LANE), 1) == m - 1
        ab_out[row1(line), :] = jnp.where(here, val, ab_out[row1(line), :])

    def red1_start():
        red_rows(0, [(i, i) for i in range(STEPS)] + [(STEPS + i, 8 + i) for i in range(STEPS)])

    def red1_end(m):
        total = red_end(0)
        c8 = total[:8]
        cg[...] = c8
        gram[jnp.maximum(m - 1, 0)] = total[8:]
        now = lax.broadcasted_iota(jnp.int32, c8.shape, 0) == m - 1
        record(0, m, jnp.sum(jnp.where(now, c8, 0.0), **ROWSUM))

        def piece(k):
            cur = xs[m, k]
            for i in range(STEPS):
                cur = cur - wide(cg[row1(i), :]) * vs[i, k]
            u1[k] = cur
            for i in range(STEPS):
                dots[i] = dots[i] + fold(vs[i, k] * cur)
            dots[STEPS] = dots[STEPS] + fold(cur * cur)

        loop(NCH, piece)
        red_rows(1, [(i, i) for i in range(STEPS)] + [(STEPS, 8)])

    def spare(i, slot):
        return rbuf.at[i // 2, lax.rem(i, 2), slot, :, top(LANE)]

    def export_pack(vec, n):
        for sp in BOTH:
            rows = [vec[2 * n + h, :, seg(sp, LANE)] for h in BOTH] + [jnp.zeros((32, LANE), F32)]
            tile = jnp.concatenate(rows, axis=0).T
            for s in BOTH:
                for g in EIGHT:
                    to, off = divmod(8 * n + g, 3)
                    obuf[to, seg(6 * sp + 3 * s + off, 8), :] = tile[seg(8 * s + g, 8), :]

    def export_send(i):
        for d, peer in enumerate(a_peers[:7]):
            to_row = lax.rem(row + (d + 1) // 4, 2)
            to = lax.rem(to_row + yb, 2) * 4 + lax.rem(x + (d + 1) % 4, 4)
            remote(obuf.at[to], spare(i, ia8), ex_send, ex_recv.at[i], peer)
        spare(i, ia8)[...] = obuf[mem]

    def export_done():
        wait_bytes(obuf.at[top(7)], ex_send)

    def red2_end(m, last):
        total = red_end(1)
        d8 = total[:8]
        sq = total[8:9]
        for i in range(STEPS):
            di = d8[row1(i)]
            inner = jnp.sum(d8 * gram[i], **ROWSUM)
            sq = sq - 2.0 * di * di + di * (2.0 * inner - di * gram[i, row1(i), :])
        beta = jnp.sqrt(sq)
        inv = 1.0 / beta
        record(1, m, beta)
        gam[...] = cg[...] + d8
        gam[row1(STEPS), :] = inv
        if last:
            scale = inv * math.sqrt(float(4 * D * D))
            for i in range(NCH):
                wait_bytes(obuf.at[top(7)], ex_recv.at[i])

            def final(j):
                cur = spare(STEPS, j)[...]
                for i in range(STEPS):
                    cur = cur - d8[row1(i)] * spare(i, j)[...]
                obuf[j] = cur * scale

            export_done()
            loop(8, final)
            for h in BOTH:
                v_out[:, seg(h, 384)] = jnp.concatenate([obuf[j, :, seg(h, HALF)] for j in EIGHT], axis=1)
        else:

            def piece(k):
                cur = u1[k]
                for i in range(STEPS):
                    cur = cur - wide(d8[row1(i)]) * vs[i, k]
                vs[m, k] = cur * wide(inv)

            loop(NCH, piece)

    def left_half(par, k):
        wait_bytes(gb.at[par, k, pl.ds((1 - core) * 8, 8)], fw_recv.at[par, k])
        split_blocks(par, k, 1 - core)
        h = lax.rem(k, 2)
        base = mult(3 * MROWS * h, 3 * MROWS)
        val = dot6(l3.at[:, pl.ds(base, 3 * MROWS)], v3.at[pl.ds(base, 3 * MROWS)], MROWS)
        t1[...] = jnp.where(h == 0, 0.0, t1[...]) + val

    def mix_chunk(n):
        for q in TRIO:
            xg = [t1[seg(4 * q + i, 64), :] for i in QUAD]
            for p in BOTH:
                for sp in BOTH:
                    e, o = (xg[2 * p + i][:, seg(sp, LANE)] for i in BOTH)
                    for s, val in enumerate(pair_halves(e, o)):
                        for part, piece in enumerate(reversed(split3(val))):
                            tq[seg(4 * part + 2 * sp + s, 64), seg(2 * q + p, LANE)] = piece
        out = dot6(w3, tq, WIDE)
        for pp in range(NCH):
            h, g3 = divmod(pp, 3)
            for t in QUAD:
                for rp in QUAD:
                    e, f = (out[seg(8 * t + 2 * rp + i, 8), seg(pp, LANE)] for i in BOTH)
                    g = jnp.concatenate(pair_halves(e, f), axis=0)
                    for part, val in enumerate(split3(g)):
                        t2[seg(12 * h + 3 * t + g3, 16), pl.ds(mult(part * D + n * THIRD + rp * LANE, LANE), LANE)] = val

    def right_half(k):
        n = k // 2
        rows = t2.at[pl.ds(mult((k - 2 * n) * 192, 192), 192)]
        o3[...] = dot6(rows, r3.at[:, pl.ds(mult(n * THIRD, THIRD), THIRD)], D)

    def send_out(m, k):
        @pl.when(m > 0)
        def _():
            wait_bytes(parts(k, 14), rs_send.at[k])

        for j in QUAD:
            y = [o3[seg(t, HALF), seg(j, LANE)] for t in QUAD]
            for sp in BOTH:
                for i, val in enumerate(pair_halves(y[2 * sp], y[2 * sp + 1])):
                    sz[k, j, i, :, seg(sp, LANE)] = val[:PART]
                    sy[k, i, j, :, seg(sp, LANE)] = val[PART:]
        rs_start(lax.rem(m, 2), k)

    high, deep = top(40), pl.ds(40, 56)

    def rg_send(c, who, rows, recv, peers):
        part = rbuf.at[c, core, who, rows]
        for peer in peers:
            remote(part, part, rr_send.at[c], recv.at[c], peer)

    def rg_wait(n, rows, sem):
        wait_bytes(rbuf.at[0, 0, top(n), top(rows)], sem)

    def rg_start(c):
        rg_send(c, mem, deep, rr_deep, x_peers)
        rg_send(c, mem, high, rr_high, [ya_peer])
        rg_send(c, mem, high, rr_up, x_peers)

    def rg_bytes(n):
        return rbuf.at[0, 0, top(n)]

    def rg_second(c):
        rg_wait(7, PART, rr_deep.at[c])
        rg_wait(1, 40, rr_high.at[c])
        rg_send(c, pl.ds(ya * 4, 4), deep, rr_low, [ya_peer])
        rg_send(c, (1 - ya) * 4 + x, high, rr_up, x_peers)

    def rg_split(c):
        def piece(i):
            turn = i // 4
            rr = i - 4 * turn
            half = lax.rem(core + turn, 2)

            @pl.when(i == 4)
            def _():
                wait_bytes(rbuf.at[c, half], rf_recv.at[c])

            for bg in range(12):
                dst = mult((bg // 4) * THIRD + (half * 4 + rr) * 64 + (bg % 4) * 16, 16)
                eights = []
                for e in BOTH:
                    who, off = divmod(2 * bg + e, 3)
                    eights.append(rbuf[c, half, who, pl.ds(mult(rr * PART + off * 8, 8), 8), :])
                for part, val in enumerate(reversed(split3(jnp.concatenate(eights, axis=0)))):
                    r3[pl.ds(part * D + dst, 16), pl.ds(mult(c * THIRD, THIRD), THIRD)] = val

        loop(8, piece)

    def rg_forward(c):
        rg_wait(7, 32, rr_low.at[c])
        rg_wait(5, HALF, rr_up.at[c])
        part = rbuf.at[c, core]
        remote(part, part, rf_send.at[c], rf_recv.at[c], partner)

    for d, peer in enumerate(a_peers[:7]):
        to = lax.rem(row + (d + 1) // 4, 2) * 4 + lax.rem(x + (d + 1) % 4, 4)
        remote(obr.at[to], pbuf.at[mem], ps_send, ps_recv, peer)
    pbuf[mem] = obr[ia8]

    for p in QUAD:
        rt_copy(p).wait()
    for i in BOTH:
        for j in QUAD:
            a, b, c = (stage[i, :, seg(3 * j + e, LANE)] for e in TRIO)
            lo = low_half(a.shape)
            for e, val in enumerate((jnp.where(lo, a, b), swap(jnp.where(lo, c, a)), jnp.where(lo, b, c))):
                rbuf[e, core, mem, seg(i, HALF), seg(j, LANE)] = val
    rg_start(0)

    wait_bytes(pbuf.at[top(7)], ps_recv)
    wait_bytes(pbuf.at[top(7)], ps_send)
    for i in EIGHT:
        for s in QUAD:
            t1[seg(8 * s + i, PART), :96] = pbuf[i, seg(s, PART), :]
    for n in TRIO:
        for sp in BOTH:
            tile = jnp.concatenate([t1[seg(6 * sp + 3 * i + n, 64), :LANE] for i in BOTH], axis=0).T
            for h in BOTH:
                xs[0, 2 * n + h, :, seg(sp, LANE)] = tile[seg(h, HALF), :]

    def first_dots(k):
        local_dots(0, k, xs[0, k])

    def el_piece(i):
        for t in range(12):
            c, h = divmod(t // 3, 2)
            for part, val in enumerate(split3(gb[1, t // 2, i, :, seg(t % 2, LANE)])):
                l3[pl.ds(mult(i * HALF, 16), HALF), seg(3 * (6 * h + 2 * part + c) + t % 3, LANE)] = val

    for c in range(NCH):
        wait_bytes(gb.at[1, c], el_sem.at[c])

    def lead(e):
        @pl.when(e == 0)
        def _():
            for k in TRIO:
                publish(0, k, True)

        @pl.when(e == 1)
        def _():
            publish(0, 3, True)
            publish(0, 4, True)
            loop(NCH, first_dots)

        @pl.when(e == 2)
        def _():
            ag_second(0, 0)
            rg_second(0)
            ag_second(0, 1)
            publish(0, 5, True)

        @pl.when(e == 3)
        def _():
            ag_second(0, 3)
            ag_second(0, 2)
            rg_forward(0)

        loop(4, lambda i: el_piece(4 * e + i))

    loop(4, lead)
    ag_second(0, 5)
    rg_start(1)
    rg_split(0)
    ag_second(0, 4)
    ag_forward(0, 0, 0)

    def step(m):
        par = lax.rem(m, 2)
        nxt = 1 - par
        more, first, later = m < LAST, m == 0, m > 0

        def finish(k):
            combine(m, k)
            publish(m, k, False)

        def halves(k):
            @pl.when(k == 1)
            def _():
                ag_forward(par, 1, m)

                @pl.when(later)
                def _():
                    ag_second(par, 3)
                    finish(5)

                red1_start()

                @pl.when(first)
                def _():
                    rg_start(2)
                    rg_second(1)

            @pl.when(k == 2)
            def _():
                pl.when(later)(lambda: ag_second(par, 4))
                ag_forward(par, 3, m)
                red_mid(0)
                pl.when(later)(lambda: ag_second(par, 5))

            @pl.when(k == 4)
            def _():
                red1_end(m)
                ag_forward(par, 5, m)
                pl.when(first)(lambda: rg_second(2))

            left_half(par, k)

            pl.when(k == 1)(lambda: ag_forward(par, 2, m))
            pl.when(k == 3)(lambda: ag_forward(par, 4, m))
            pl.when(lax.rem(k, 2) == 1)(lambda: mix_chunk(k // 2))

        loop(NCH, halves)
        pl.when(later)(lambda: export_send(m - 1))
        red_mid(1)

        def advance(k):
            combine(m + 1, k)
            pl.when(more)(lambda: publish(m + 1, k, False))

        def spread(k):
            pl.when(more)(lambda: ag_second(nxt, k))

        def outs(k):
            pl.when(first & (k == 1))(lambda: rg_forward(1))

            @pl.when(first & (k == 2))
            def _():
                rg_split(1)
                rg_forward(2)

            pl.when(first & (k == 4))(lambda: rg_split(2))
            right_half(k)
            pl.when(k == 3)(lambda: rs_second(par, 1))

            @pl.when(k == 5)
            def _():
                advance(1)
                rs_second(par, 3)

            send_out(m, k)

            @pl.when(k == 2)
            def _():
                red2_end(m, False)
                rs_second(par, 0)

            @pl.when(k == 4)
            def _():
                rs_second(par, 2)
                advance(0)

        loop(NCH, outs)

        @pl.when(first)
        def _():
            for c in TRIO:
                wait_bytes(rg_bytes(7), rr_send.at[c])
                wait_bytes(rbuf.at[0, 0], rf_send.at[c])

        spread(0)
        pl.when(later)(export_done)
        rs_second(par, 4)
        export_pack(vs.at[m], 0)
        export_pack(vs.at[m], 1)
        advance(2)
        spread(1)
        export_pack(vs.at[m], 2)
        advance(3)
        pl.when(more)(lambda: ag_forward(nxt, 0, 1))
        rs_second(par, 5)
        spread(2)
        advance(4)

    loop(STEPS, step)

    export_send(LAST)
    combine(STEPS, 5)
    red1_start()
    red_mid(0)
    red1_end(STEPS)
    export_done()
    for n in TRIO:
        export_pack(u1, n)
    export_send(STEPS)
    red_mid(1)
    red2_end(STEPS, True)
    for k in range(NCH):
        wait_bytes(parts(k, 14), ag_send.at[k])
        wait_bytes(parts(k, 14), rs_send.at[k])
        wait_bytes(gb.at[0, k, top(8)], fw_send.at[k])


def run_kernel(psi, wsm, el, rt):
    vmem = pl.BlockSpec(memory_space=pltpu.VMEM)
    hbm = pl.BlockSpec(memory_space=pl.ANY)
    dma = pltpu.SemaphoreType.DMA
    six, pair, three = dma((NCH,)), dma((2,)), dma((3,))
    both = dma((2, NCH))
    block = (HALF, WIDE)
    start = pltpu.VMEM((8, 96, 96), F32)
    return pl.pallas_call(
        kernel,
        out_shape=(jax.ShapeDtypeStruct((96, MROWS), F32), jax.ShapeDtypeStruct((8, LANE), F32)),
        in_specs=[hbm, vmem, hbm, hbm],
        out_specs=(vmem, vmem),
        scratch_shapes=[
            pltpu.VMEM((MROWS, 3 * D), BF16),
            pltpu.VMEM((3 * D, D), BF16),
            pltpu.VMEM((WIDE, MROWS), BF16),
            pltpu.VMEM((2, NCH, 16, *block), F32),
            pltpu.VMEM((3 * D, WIDE), BF16),
            pltpu.VMEM((MROWS, WIDE), F32),
            pltpu.VMEM((MROWS, MROWS), BF16),
            pltpu.VMEM((384, 3 * D), BF16),
            pltpu.VMEM((192, THIRD), F32),
            pltpu.VMEM((NCH, 4, 2, PART, WIDE), F32),
            pltpu.VMEM((NCH, 2, 4, PART, WIDE), F32),
            pltpu.VMEM((2, NCH, 14, PART, WIDE), F32),
            pltpu.VMEM((STEPS + 1, NCH, *block), F32),
            pltpu.VMEM((STEPS, NCH, *block), F32),
            pltpu.VMEM((NCH, *block), F32),
            pltpu.VMEM((2, HALF, D), F32),
            pltpu.VMEM((3, 2, 8, 96, THIRD), F32),
            start,
            pltpu.VMEM((8, 96, LANE), F32),
            start,
            pltpu.VMEM((96, MROWS), F32),
            pltpu.VMEM((2 * STEPS, 8, LANE), F32),
            pltpu.VMEM((2, 16, 16, LANE), F32),
            pltpu.VMEM((2, 8, 16, LANE), F32),
            pltpu.VMEM((8, LANE), F32),
            pltpu.VMEM((8, LANE), F32),
            pltpu.VMEM((STEPS, 8, LANE), F32),
            both, both, six, both, both, six, both, six, pair, pair, pair, pair,
            dma((4,)), six, three, three, three, three, three, three, three, dma, dma, dma, dma, six,
        ],
        compiler_params=pltpu.CompilerParams(collective_id=0, has_side_effects=True, vmem_limit_bytes=67043328),
        name="lanczos",
    )(psi, wsm, el, rt)


def solution(mesh):
    grid = Mesh(mesh.devices.reshape(4, 2, 2, 4, 2), AXES)
    psi_spec = P("core", None, None, ("z", "yb", "ya", "x"))

    def local_fn(psi_loc, env_left, env_right, mpo_pair):
        psi = jnp.transpose(psi_loc, (1, 2, 3, 0)).reshape(96, MROWS)
        wsm = jnp.moveaxis(mpo_pair, 1, -1).reshape(LANE, 8)
        vec, ab = run_kernel(psi, wsm, env_left.reshape(LANE, HALF, D), env_right)
        out = jnp.transpose(vec.reshape(2, 2, PART, MROWS), (3, 0, 1, 2))
        return ab[0, :STEPS], ab[1, :STEPS], out

    return jax.shard_map(
        local_fn,
        mesh=grid,
        in_specs=(psi_spec, P("core", None, None), P(("z", "yb", "ya", "x"), None, None), P()),
        out_specs=(P(), P(), psi_spec),
        check_vma=False,
    )
```
